8 devices in a mesh: emb: 2 (over z, y), col: 2 (over x), row: 2 (over core).
Axes of the slice: x: 2, y: 2, z: 1, core: 2. Of those that a mesh axis runs over, the one named last changes fastest.
Arguments:
- inter_mask: int32 [1024, 32768], P('row', 'col')
- emb_user: bfloat16 [1024, 64], P(('row', 'col'), 'emb')
- emb_item: bfloat16 [32768, 64], P(('col', 'row'), 'emb')
- triples: int32 [4096, 3], replicated
Outputs:
- output 1: bfloat16 [1024, 64], P(('row', 'col'), 'emb')
- output 2: bfloat16 [32768, 64], P(('col', 'row'), 'emb')
- output 3: float32 [4096], replicated
All inputs are finite; a program needn't handle non-finite values.
Results may differ from the reference program's by a relative error of at most 0.0178813.
Values are sent between devices in bfloat16 or wider.
A program may use at most 1 GiB of HBM per device.

```python
import jax
import jax.numpy as jnp
from jax import lax

NUM_USERS = 1024
NUM_ITEMS = 32768
EMB_DIM = 64
NUM_TRIPLES = 4096
NUM_LAYERS = 3
SPARSITY = 8
NUM_GROUPS = 4


def setup_inputs(seed: int = 0) -> dict:
    key = jax.random.key(seed)
    key_list = jax.random.split(key, 10)
    inter_mask = (jax.random.randint(key_list[0], (NUM_USERS, NUM_ITEMS), 0, SPARSITY) == 0).astype(jnp.int32)
    mean_user = jax.random.normal(key_list[1], (EMB_DIM,), jnp.float32)
    mean_item = jax.random.normal(key_list[2], (EMB_DIM,), jnp.float32)
    noise_user = jax.random.normal(key_list[3], (NUM_USERS, EMB_DIM), jnp.float32)
    noise_item = jax.random.normal(key_list[4], (NUM_ITEMS, EMB_DIM), jnp.float32)
    group_user = jax.random.normal(key_list[8], (NUM_GROUPS, EMB_DIM), jnp.float32)
    group_item = jax.random.normal(key_list[9], (NUM_GROUPS, EMB_DIM), jnp.float32)
    user_group = (jnp.arange(NUM_USERS) * NUM_GROUPS) // NUM_USERS
    item_group = (jnp.arange(NUM_ITEMS) * NUM_GROUPS) // NUM_ITEMS
    emb_user = (0.5 * (mean_user[None, :] + 1.5 * group_user[user_group] + noise_user)).astype(jnp.bfloat16)
    emb_item = (0.5 * (mean_item[None, :] + 1.5 * group_item[item_group] + noise_item)).astype(jnp.bfloat16)
    users = jax.random.randint(key_list[5], (NUM_TRIPLES,), 0, NUM_USERS).at[0].set(NUM_USERS - 1)
    pos_items = jax.random.randint(key_list[6], (NUM_TRIPLES,), 0, NUM_ITEMS).at[0].set(NUM_ITEMS - 1)
    neg_items = jax.random.randint(key_list[7], (NUM_TRIPLES,), 0, NUM_ITEMS).at[1].set(0)
    triples = jnp.stack([users, pos_items, neg_items], axis=1).astype(jnp.int32)
    return {"inter_mask": inter_mask, "emb_user": emb_user, "emb_item": emb_item, "triples": triples}


def reference(inter_mask, emb_user, emb_item, triples):
    deg_user = jnp.maximum(jnp.sum(inter_mask, axis=1), 1).astype(jnp.float32)
    deg_item = jnp.maximum(jnp.sum(inter_mask, axis=0), 1).astype(jnp.float32)
    adj_norm = ((lax.rsqrt(deg_user)[:, None] * inter_mask.astype(jnp.float32)) * lax.rsqrt(deg_item)[None, :]).astype(jnp.bfloat16)

    def layer_step(carry, unused):
        user_cur, item_cur, user_acc, item_acc = carry
        user_next = jnp.dot(adj_norm, item_cur, preferred_element_type=jnp.float32).astype(jnp.bfloat16)
        item_next = jnp.dot(adj_norm.T, user_cur, preferred_element_type=jnp.float32).astype(jnp.bfloat16)
        new_carry = (user_next, item_next, user_acc + user_next.astype(jnp.float32), item_acc + item_next.astype(jnp.float32))
        return new_carry, None

    init_state = (emb_user, emb_item, emb_user.astype(jnp.float32), emb_item.astype(jnp.float32))
    carry_out, scan_ys = lax.scan(layer_step, init_state, None, length=NUM_LAYERS)
    final_user = (carry_out[2] / (NUM_LAYERS + 1)).astype(jnp.bfloat16)
    final_item = (carry_out[3] / (NUM_LAYERS + 1)).astype(jnp.bfloat16)
    e_user = jnp.take(final_user, triples[:, 0], axis=0).astype(jnp.float32)
    e_pos = jnp.take(final_item, triples[:, 1], axis=0).astype(jnp.float32)
    e_neg = jnp.take(final_item, triples[:, 2], axis=0).astype(jnp.float32)
    score = jnp.sum(e_user * (e_pos - e_neg), axis=1)
    bpr_loss = jax.nn.softplus(-score)
    return final_user, final_item, bpr_loss
```

```python
import functools

import jax
import jax.numpy as jnp
from jax import lax
from jax.experimental import pallas as pl
from jax.experimental.pallas import tpu as pltpu
from jax.sharding import PartitionSpec as P

NUM_LAYERS = 3
CH = 1024
NSLOT = 5
MESH = pl.DeviceIdType.MESH
F32 = jnp.float32
BF16 = jnp.bfloat16


def remote(src, dst, ssem, rsem, dev):
    return pltpu.make_async_remote_copy(src_ref=src, dst_ref=dst, send_sem=ssem, recv_sem=rsem,
                                        device_id=dev, device_id_type=MESH)


def kernel(n_usr, n_itm, dim, n_trip,
           mask_ref, eu_ref, ei_ref, tri_ref, ou_ref, oi_ref, loss_ref,
           stage, adj, rowacc, degi, degi_r, degu, degu_r, invu, invi,
           it0, it1, it2, ut0, i1p, i1r, i2p, i2r, i3p, i3r,
           up, up_r, u3p, u3_r, ufin, ufin_r, ofin, oufin, table, utab,
           tri_v, idx_v, idx_s, dbuf, drecv, sbuf, srecv, lbuf,
           msem, lsem, ssem, rsem, cs1, cr1, cs2, cr2, cs3, cr3, ds, dr, bs, br):
    e = lax.axis_index("emb")
    c = lax.axis_index("col")
    r = lax.axis_index("row")
    sib = {"row": 1 - r}
    xpeer = {"col": 1 - c}
    nch = n_itm // CH
    half = n_itm // 2
    hch = nch // 2
    uh = n_usr // 2
    nhome = n_trip // 4
    hrow = nhome // 4

    def mask_copy(j):
        slot = lax.rem(j, NSLOT)
        return pltpu.make_async_copy(mask_ref.at[:, pl.ds(j * CH, CH)], stage.at[slot], msem.at[slot])

    for j in range(NSLOT):
        mask_copy(j).start()
    own_i = it0.at[:, pl.ds(pl.multiple_of(r * half, half), half)]
    own_u = ut0.at[:, pl.ds(pl.multiple_of(c * uh, uh), uh)]
    cp_i = pltpu.make_async_copy(ei_ref, own_i, lsem.at[0])
    cp_u = pltpu.make_async_copy(eu_ref, own_u, lsem.at[1])
    cp_t = pltpu.make_async_copy(tri_ref, tri_v, lsem.at[2])
    cp_i.start()
    cp_u.start()
    cp_t.start()

    barrier = pltpu.get_barrier_semaphore()
    for q in range(1, 8):
        dev = {"emb": lax.rem(e + q // 4, 2), "col": lax.rem(c + (q // 2) % 2, 2), "row": lax.rem(r + q % 2, 2)}
        pl.semaphore_signal(barrier, inc=1, device_id=dev, device_id_type=MESH)

    rowacc[...] = jnp.zeros_like(rowacc)

    def mask_step(j, _):
        slot = lax.rem(j, NSLOT)
        mask_copy(j).wait()
        cols = pl.ds(pl.multiple_of(j * CH, CH), CH)

        def rows_step(g, acc):
            rows = pl.ds(pl.multiple_of(g * 16, 16), 16)
            m = stage[slot, rows, :].astype(F32)
            adj[rows, cols] = m.astype(BF16)
            s = m[:, 0:128]
            for k in range(1, CH // 128):
                s = s + m[:, k * 128:(k + 1) * 128]
            rowacc[rows, :] += s
            return acc + (m[0:8] + m[8:16])

        acc = lax.fori_loop(0, n_usr // 16, rows_step, jnp.zeros((8, CH), F32), unroll=2)
        degi[pl.ds(j, 1), :] = jnp.sum(acc, axis=0, keepdims=True)

        @pl.when(j + NSLOT < nch)
        def _():
            mask_copy(j + NSLOT).start()
        return 0

    lax.fori_loop(0, 4, mask_step, 0)
    cp_i.wait()
    cp_u.wait()
    cp_t.wait()
    pl.semaphore_wait(barrier, 7)
    rc_i = remote(own_i, own_i, ssem.at[0], rsem.at[0], sib)
    rc_u = remote(own_u, own_u, ssem.at[1], rsem.at[1], xpeer)
    rc_i.start()
    rc_u.start()
    lax.fori_loop(4, nch, mask_step, 0)

    degu[...] = jnp.sum(rowacc[...].T, axis=0, keepdims=True)
    rc_du = remote(degu, degu_r, ssem.at[2], rsem.at[2], xpeer)
    rc_di = remote(degi, degi_r, ssem.at[3], rsem.at[3], sib)
    rc_du.start()
    rc_di.start()

    item_off = (c * 2 + r) * half
    for k in range(2):
        loc = tri_v[k + 1, :, :] - item_off
        idx_v[k, :, :] = jnp.where((loc >= 0) & (loc < half), loc, half)
    idx_v[2, :, :] = tri_v[0, :, :]
    cp_x = pltpu.make_async_copy(idx_v, idx_s, lsem.at[0])
    cp_x.start()
    table[pl.ds(half, 8), :] = jnp.zeros((8, 128), F32)

    rc_di.wait()
    invi[...] = lax.rsqrt(jnp.maximum(degi[...] + degi_r[...], 1.0))
    rc_i.wait()
    rc_u.wait()
    cp_x.wait()
    rc_du.wait()
    inv_row = lax.rsqrt(jnp.maximum(degu[...] + degu_r[...], 1.0))
    invu[...] = jnp.broadcast_to(inv_row, (128, n_usr)).T

    def chunk1(j):
        cols = pl.ds(pl.multiple_of(j * CH, CH), CH)
        return remote(i1p.at[:, cols], i1r.at[:, cols], cs1.at[j], cr1.at[j], sib)

    def build_step(j, _):
        cols = pl.ds(pl.multiple_of(j * CH, CH), CH)
        wi = jnp.broadcast_to(invi[pl.ds(j, 1), :], (16, CH))

        def rows_step(g, _):
            rows = pl.ds(pl.multiple_of(g * 16, 16), 16)
            wu = jnp.concatenate([invu[rows, :]] * (CH // 128), axis=1)
            adj[rows, cols] = (wu * wi).astype(BF16) * adj[rows, cols]
            return 0

        lax.fori_loop(0, n_usr // 16, rows_step, 0, unroll=4)
        i1p[:, cols] = jnp.dot(ut0[...], adj[:, cols], preferred_element_type=F32)
        chunk1(j).start()
        return 0

    lax.fori_loop(0, nch, build_step, 0)

    def dot_t(lhs, a):
        return lax.dot_general(lhs, a, (((1,), (1,)), ((), ())), preferred_element_type=F32)

    up[...] = jnp.zeros_like(up)

    def user_step(j, _):
        cols = pl.ds(pl.multiple_of(j * CH, CH), CH)
        chunk1(j).wait_recv()
        v1 = (i1p[:, cols] + i1r[:, cols]).astype(BF16)
        it1[:, cols] = v1
        lhs = jnp.concatenate([it0[:, cols], v1], axis=0)
        up[...] += dot_t(lhs, adj[:, cols])
        return 0

    lax.fori_loop(0, nch, user_step, 0)
    rc_up = remote(up, up_r, ssem.at[4], rsem.at[4], xpeer)
    rc_up.start()
    rc_up.wait()
    u12 = (up[...] + up_r[...]).astype(BF16)

    def chunk2(j):
        cols = pl.ds(pl.multiple_of(j * CH, CH), CH)
        return remote(i2p.at[:, cols], i2r.at[:, cols], cs2.at[j], cr2.at[j], sib)

    def chunk3(k, base):
        src = pl.ds(pl.multiple_of((base + k) * CH, CH), CH)
        dst = pl.ds(pl.multiple_of(k * CH, CH), CH)
        return remote(i3p.at[:, src], i3r.at[:, dst], cs3.at[k], cr3.at[k], sib)

    def item_step(k, base, send3):
        j = base + k
        cols = pl.ds(pl.multiple_of(j * CH, CH), CH)
        part = jnp.dot(u12, adj[:, cols], preferred_element_type=F32)
        i2p[:, cols] = part[0:dim]
        i3p[:, cols] = part[dim:2 * dim]
        chunk2(j).start()
        if send3:
            chunk3(k, base).start()
        return 0

    sbase = (1 - r) * hch
    obase = r * hch
    lax.fori_loop(0, hch, lambda k, _: item_step(k, sbase, True), 0)
    lax.fori_loop(0, hch, lambda k, _: item_step(k, obase, False), 0)

    u3p[...] = jnp.zeros_like(u3p)

    def user3_step(k, base):
        j = base + k
        cols = pl.ds(pl.multiple_of(j * CH, CH), CH)
        chunk2(j).wait_recv()
        v2 = (i2p[:, cols] + i2r[:, cols]).astype(BF16)
        it2[:, cols] = v2
        u3p[...] += dot_t(v2, adj[:, cols])
        return 0

    lax.fori_loop(0, hch, lambda k, _: user3_step(k, obase), 0)
    lax.fori_loop(0, hch, lambda k, _: user3_step(k, sbase), 0)
    rc_u3 = remote(u3p, u3_r, ssem.at[5], rsem.at[5], xpeer)
    rc_u3.start()

    def final_step(k, _):
        cols = pl.ds(pl.multiple_of((obase + k) * CH, CH), CH)
        loc = pl.ds(pl.multiple_of(k * CH, CH), CH)
        chunk3(k, sbase).wait_recv()
        v3 = (i3p[:, cols] + i3r[:, loc]).astype(BF16)
        acc = it0[:, cols].astype(F32) + it1[:, cols].astype(F32)
        acc = (acc + it2[:, cols].astype(F32)) + v3.astype(F32)
        fin = (acc * (1.0 / (NUM_LAYERS + 1))).astype(BF16)
        ofin[:, loc] = fin
        fin = fin.astype(F32)
        for b in range(CH // 128):
            blk = fin[:, b * 128:(b + 1) * 128]
            table[pl.ds(pl.multiple_of(k * CH + b * 128, 128), 128), :] = jnp.concatenate([blk] * 4, axis=0).T
        return 0

    lax.fori_loop(0, hch, final_step, 0)
    cp_oi = pltpu.make_async_copy(ofin, oi_ref, lsem.at[1])
    cp_oi.start()

    lane_blk = lax.broadcasted_iota(jnp.int32, (1, 128), 1) // dim

    def pack(rows4):
        d = rows4[0]
        for b in range(1, 4):
            d = jnp.where(lane_blk == b, rows4[b], d)
        return d

    def d_send(q, ah):
        hc, hr = lax.rem(c + q // 2, 2), lax.rem(r + q % 2, 2)
        rows = pl.ds(ah * 128, 128)
        return remote(dbuf.at[q, rows, :], drecv.at[q - 1, rows, :], ds.at[q - 1, ah], dr.at[q - 1, ah],
                      {"col": hc, "row": hr})

    def diff_rows(q, ah):
        home = lax.rem(c + q // 2, 2) * 2 + lax.rem(r + q % 2, 2)

        def body(al, _):
            out = []
            for b in range(4):
                row = home * (nhome // 128) + b * (hrow // 128) + ah
                p = idx_s[0, row, al]
                n = idx_s[1, row, al]
                out.append(table[pl.ds(p, 1), :] - table[pl.ds(n, 1), :])
            dbuf[q, pl.ds(ah * 128 + al, 1), :] = pack(out)
            return 0

        lax.fori_loop(0, 128, body, 0, unroll=8)

    for q in (3, 2, 1, 0):
        for ah in range(hrow // 128):
            diff_rows(q, ah)
            if q:
                d_send(q, ah).start()

    rc_u3.wait()
    u3 = (u3p[...] + u3_r[...]).astype(BF16).astype(F32)
    uacc = ut0[...].astype(F32) + u12[0:dim].astype(F32)
    uacc = (uacc + u12[dim:2 * dim].astype(F32)) + u3
    ufin[...] = (uacc * (1.0 / (NUM_LAYERS + 1))).astype(BF16)
    rc_uf = remote(ufin, ufin_r, ssem.at[6], rsem.at[6], sib)
    rc_uf.start()
    oufin[...] = ufin[:, pl.ds(pl.multiple_of(c * uh, uh), uh)]
    cp_ou = pltpu.make_async_copy(oufin, ou_ref, lsem.at[2])
    cp_ou.start()

    def user_table(src, base):
        for b in range(n_usr // 128):
            blk = src[:, b * 128:(b + 1) * 128].astype(F32)
            utab[pl.ds(pl.multiple_of(base + b * 128, 128), 128), :] = jnp.concatenate([blk] * 4, axis=0).T

    user_table(ufin, r * n_usr)
    rc_uf.wait()
    user_table(ufin_r, (1 - r) * n_usr)

    home = c * 2 + r
    for ah in range(hrow // 128):
        def ubody(al, _, ah=ah):
            out = []
            for b in range(4):
                row = home * (nhome // 128) + b * (hrow // 128) + ah
                out.append(utab[pl.ds(idx_s[2, row, al], 1), :])
            dbuf[4, pl.ds(ah * 128 + al, 1), :] = pack(out)
            return 0
        lax.fori_loop(0, 128, ubody, 0, unroll=8)

    for q in (3, 2, 1):
        for ah in range(hrow // 128):
            d_send(q, ah).wait()
    dsum = (dbuf[0] + drecv[0]) + (drecv[1] + drecv[2])
    prod = (dsum * dbuf[4]).T
    for b in range(4):
        s = jnp.sum(prod[b * dim:(b + 1) * dim, :], axis=0, keepdims=True)
        for h in range(hrow // 128):
            sbuf[pl.ds(b * (hrow // 128) + h, 1), :] = s[:, h * 128:(h + 1) * 128]

    def s_send(q):
        dev = {"emb": lax.rem(e + q // 4, 2), "col": lax.rem(c + (q // 2) % 2, 2), "row": lax.rem(r + q % 2, 2)}
        return remote(sbuf, srecv.at[q - 1], bs.at[q - 1], br.at[q - 1], dev)

    for q in range(7, 0, -1):
        s_send(q).start()
    for q in range(7, 0, -1):
        s_send(q).wait()
    for q in range(4):
        own = sbuf[...] if q == 0 else srecv[q - 1]
        x = own + srecv[q + 3]
        hq = lax.rem(c + q // 2, 2) * 2 + lax.rem(r + q % 2, 2)
        ls = jnp.maximum(-x, 0.0) + jnp.log1p(jnp.exp(-jnp.abs(x)))
        lbuf[pl.ds(pl.multiple_of(hq * (nhome // 128), 8), nhome // 128), :] = ls
    cp_l = pltpu.make_async_copy(lbuf, loss_ref, lsem.at[0])
    cp_l.start()

    def drain(j, _):
        chunk1(j).wait_send()
        chunk2(j).wait_send()
        return 0
    lax.fori_loop(0, nch, drain, 0)

    def drain3(k, _):
        chunk3(k, sbase).wait_send()
        return 0
    lax.fori_loop(0, hch, drain3, 0)
    cp_oi.wait()
    cp_ou.wait()
    cp_l.wait()


def solution(mesh):
    def local_fn(mask_blk, user_sh, item_sh, triples):
        n_usr, n_itm = mask_blk.shape
        dim = user_sh.shape[1]
        n_trip = triples.shape[0]
        nch = n_itm // CH
        half = n_itm // 2
        tri = triples.T.reshape(3, n_trip // 128, 128)
        vm = pltpu.VMEM
        dma = pltpu.SemaphoreType.DMA
        nhome = n_trip // 4
        hrow = nhome // 4
        scratch = [
            vm((NSLOT, n_usr, CH), jnp.int32), vm((n_usr, n_itm), BF16), vm((n_usr, 128), F32),
            vm((nch, CH), F32), vm((nch, CH), F32), vm((1, n_usr), F32), vm((1, n_usr), F32),
            vm((n_usr, 128), F32), vm((nch, CH), F32),
            vm((dim, n_itm), BF16), vm((dim, n_itm), BF16), vm((dim, n_itm), BF16), vm((dim, n_usr), BF16),
            vm((dim, n_itm), F32), vm((dim, n_itm), F32), vm((dim, n_itm), F32), vm((dim, n_itm), F32),
            vm((dim, n_itm), F32), vm((dim, half), F32),
            vm((2 * dim, n_usr), F32), vm((2 * dim, n_usr), F32), vm((dim, n_usr), F32), vm((dim, n_usr), F32),
            vm((dim, n_usr), BF16), vm((dim, n_usr), BF16), vm((dim, half), BF16), vm((dim, n_usr // 2), BF16),
            vm((half + 8, 128), F32), vm((2 * n_usr, 128), F32),
            vm((3, n_trip // 128, 128), jnp.int32), vm((3, n_trip // 128, 128), jnp.int32),
            pltpu.SMEM((3, n_trip // 128, 128), jnp.int32),
            vm((5, hrow, 128), F32), vm((3, hrow, 128), F32),
            vm((nhome // 128, 128), F32), vm((7, nhome // 128, 128), F32), vm((n_trip // 128, 128), F32),
            dma((NSLOT,)), dma((3,)), dma((7,)), dma((7,)),
            dma((nch,)), dma((nch,)), dma((nch,)), dma((nch,)), dma((nch // 2,)), dma((nch // 2,)),
            dma((3, hrow // 128)), dma((3, hrow // 128)), dma((7,)), dma((7,)),
        ]
        any_spec = pl.BlockSpec(memory_space=pl.ANY)
        ou, oi, loss = pl.pallas_call(
            functools.partial(kernel, n_usr, n_itm, dim, n_trip),
            out_shape=(jax.ShapeDtypeStruct((dim, n_usr // 2), BF16),
                       jax.ShapeDtypeStruct((dim, half), BF16),
                       jax.ShapeDtypeStruct((n_trip // 128, 128), F32)),
            in_specs=[any_spec] * 4,
            out_specs=(any_spec,) * 3,
            scratch_shapes=scratch,
            compiler_params=pltpu.CompilerParams(collective_id=0, has_side_effects=True,
                                                 vmem_limit_bytes=62 * 1024 * 1024),
            name="gcn",
        )(mask_blk, user_sh.T, item_sh.T, tri)
        return ou.T, oi.T, loss.reshape(n_trip)

    return jax.shard_map(
        local_fn, mesh=mesh,
        in_specs=(P("row", "col"), P(("row", "col"), "emb"), P(("col", "row"), "emb"), P()),
        out_specs=(P(("row", "col"), "emb"), P(("col", "row"), "emb"), P()),
        check_vma=False)
```

```python
import functools

import jax
import jax.numpy as jnp
from jax import lax
from jax.experimental import pallas as pl
from jax.experimental.pallas import tpu as pltpu
from jax.sharding import PartitionSpec as P

NUM_LAYERS = 3
CH = 1024
MC = 512
NSLOT = 6
WIDE = 4096
MESH = pl.DeviceIdType.MESH
F32 = jnp.float32
BF16 = jnp.bfloat16


def remote(src, dst, ssem, rsem, dev):
    return pltpu.make_async_remote_copy(src_ref=src, dst_ref=dst, send_sem=ssem, recv_sem=rsem,
                                        device_id=dev, device_id_type=MESH)


def kernel(n_usr, n_itm, dim, n_trip,
           mask_ref, eu_ref, ei_ref, tri_ref, ou_ref, oi_ref, loss_ref,
           stage, adj, rowacc, degi, degi_r, degu, degu_r, invu, invi,
           it0, it1, it2, ut0, i1p, i1r, i2p, i2r,
           up, up_r, u3p, u3_r, uall, sel, oufin, table,
           tri_v, idx_v, idx_t, idx_s, dbuf, drecv, sbuf, srecv, lbuf,
           msem, lsem, ssem, rsem, cs1, cr1, cs2, cr2, cs3, cr3, ds, dr, bs, br, free_sem):
    e = lax.axis_index("emb")
    c = lax.axis_index("col")
    r = lax.axis_index("row")
    sib = {"row": 1 - r}
    xpeer = {"col": 1 - c}
    nch = n_itm // CH
    half = n_itm // 2
    uh = n_usr // 2
    nhome = n_trip // 4
    hrow = nhome // 4

    def mask_copy(j):
        slot = lax.rem(j, NSLOT)
        return pltpu.make_async_copy(mask_ref.at[:, pl.ds(pl.multiple_of(j * MC, MC), MC)], stage.at[slot], msem.at[slot])

    for j in range(NSLOT):
        mask_copy(j).start()
    own_i = it0.at[:, pl.ds(pl.multiple_of(r * half, half), half)]
    own_u = ut0.at[:, pl.ds(pl.multiple_of(c * uh, uh), uh)]
    cp_i = pltpu.make_async_copy(ei_ref, own_i, lsem.at[0])
    cp_u = pltpu.make_async_copy(eu_ref, own_u, lsem.at[1])
    cp_t = pltpu.make_async_copy(tri_ref, tri_v, lsem.at[2])
    cp_i.start()
    cp_u.start()
    cp_t.start()

    barrier = pltpu.get_barrier_semaphore()
    for q in range(1, 8):
        dev = {"emb": lax.rem(e + q // 4, 2), "col": lax.rem(c + (q // 2) % 2, 2), "row": lax.rem(r + q % 2, 2)}
        pl.semaphore_signal(barrier, inc=1, device_id=dev, device_id_type=MESH)

    rowacc[...] = jnp.zeros_like(rowacc)

    def mask_step(j, _):
        slot = lax.rem(j, NSLOT)
        mask_copy(j).wait()
        cols = pl.ds(pl.multiple_of(j * MC, MC), MC)

        def rows_step(g, acc):
            rows = pl.ds(pl.multiple_of(g * 16, 16), 16)
            m = stage[slot, rows, :].astype(F32)
            adj[rows, cols] = m.astype(BF16)
            s = m[:, 0:128]
            for k in range(1, MC // 128):
                s = s + m[:, k * 128:(k + 1) * 128]
            rowacc[rows, :] += s
            return acc + (m[0:8] + m[8:16])

        acc = lax.fori_loop(0, n_usr // 16, rows_step, jnp.zeros((8, MC), F32), unroll=2)
        degi[pl.ds(j, 1), :] = jnp.sum(acc, axis=0, keepdims=True)

        @pl.when(j + NSLOT < n_itm // MC)
        def _():
            mask_copy(j + NSLOT).start()
        return 0

    with jax.named_scope("ph_mask0"):
        lax.fori_loop(0, 8, mask_step, 0)
    cp_i.wait()
    cp_u.wait()
    cp_t.wait()
    with jax.named_scope("ph_barrier"):
        pl.semaphore_wait(barrier, 7)
    rc_i = remote(own_i, own_i, ssem.at[0], rsem.at[0], sib)
    rc_u = remote(own_u, own_u, ssem.at[1], rsem.at[1], xpeer)
    rc_i.start()
    rc_u.start()
    with jax.named_scope("ph_mask1"):
        lax.fori_loop(8, n_itm // MC, mask_step, 0)

    degu[...] = jnp.sum(rowacc[...].T, axis=0, keepdims=True)
    rc_du = remote(degu, degu_r, ssem.at[2], rsem.at[2], xpeer)
    rc_di = remote(degi, degi_r, ssem.at[3], rsem.at[3], sib)
    rc_du.start()
    rc_di.start()

    nrow = n_trip // 128
    idx_v[...] = jnp.zeros_like(idx_v)
    for k in range(3):
        for i in range(nrow):
            idx_v[pl.ds(k * nrow + i, 1), :] = tri_v[pl.ds((k + 1) % 3, 1), i * 128:(i + 1) * 128]
    loc = idx_v[0:2 * nrow, :] - c * n_itm
    idx_v[0:2 * nrow, :] = jnp.where((loc >= 0) & (loc < n_itm), loc, n_itm)
    idx_t[...] = idx_v[...].T
    cp_x = pltpu.make_async_copy(idx_t, idx_s, lsem.at[0])
    cp_x.start()
    table[pl.ds(n_itm, 8), :] = jnp.zeros((8, 128), F32)

    with jax.named_scope("ph_di_wait"):
        rc_di.wait()
    invi[...] = lax.rsqrt(jnp.maximum(degi[...] + degi_r[...], 1.0))
    rc_i.wait()
    rc_u.wait()
    cp_x.wait()
    with jax.named_scope("ph_du_wait"):
        rc_du.wait()
    inv_row = lax.rsqrt(jnp.maximum(degu[...] + degu_r[...], 1.0))
    invu[...] = jnp.broadcast_to(inv_row, (128, n_usr)).T

    def chunk1(j):
        cols = pl.ds(pl.multiple_of(j * CH, CH), CH)
        return remote(i1p.at[:, cols], i1r.at[:, cols], cs1.at[j], cr1.at[j], sib)

    def build_step(i, _):
        for jj in range(2):
            j = i * 2 + jj
            for nt in range(CH // 256):
                cols = pl.ds(pl.multiple_of(j * CH + nt * 256, 256), 256)
                lane = nt * 256 % MC
                wi = jnp.broadcast_to(invi[pl.ds(j * (CH // MC) + nt * 256 // MC, 1), lane:lane + 256], (16, 256))
                part = None
                for kt in range(n_usr // 256):
                    tiles = []
                    for g in range(16):
                        rows = pl.ds(kt * 256 + g * 16, 16)
                        wu = jnp.concatenate([invu[rows, :]] * 2, axis=1)
                        a = (wu * wi).astype(BF16) * adj[rows, cols]
                        adj[rows, cols] = a
                        tiles.append(a)
                    p = jnp.dot(ut0[:, kt * 256:(kt + 1) * 256], jnp.concatenate(tiles, axis=0),
                                preferred_element_type=F32)
                    part = p if part is None else part + p
                i1p[:, cols] = part
        for jj in range(2):
            chunk1(i * 2 + jj).start()
        return 0

    with jax.named_scope("ph_build"):
        lax.fori_loop(0, nch // 2, build_step, 0)

    def dot_t(lhs, a):
        return lax.dot_general(lhs, a, (((1,), (1,)), ((), ())), preferred_element_type=F32)

    up[...] = jnp.zeros_like(up)

    def user_step(i, _):
        cols = pl.ds(pl.multiple_of(i * WIDE, WIDE), WIDE)
        for t in range(WIDE // CH):
            chunk1(i * (WIDE // CH) + t).wait_recv()
        v1 = (i1p[:, cols] + i1r[:, cols]).astype(BF16)
        it1[:, cols] = v1
        lhs = jnp.concatenate([it0[:, cols], v1], axis=0)
        up[...] += dot_t(lhs, adj[:, cols])
        return 0

    with jax.named_scope("ph_user"):
        lax.fori_loop(0, n_itm // WIDE, user_step, 0)
    rc_up = remote(up, up_r, ssem.at[4], rsem.at[4], xpeer)
    rc_up.start()
    pl.semaphore_signal(free_sem, inc=1, device_id=sib, device_id_type=MESH)

    def sent1(j, _):
        chunk1(j).wait_send()
        return 0
    lax.fori_loop(0, nch, sent1, 0)
    home = c * 2 + r

    def sel_step(g, _):
        users = lax.broadcasted_iota(jnp.int32, (16, 128), 0) + g * 16
        for t in range(nhome // 128):
            ids = idx_v[pl.ds(2 * nrow + home * (nhome // 128) + t, 1), :]
            hit = jnp.where(users == jnp.broadcast_to(ids, (16, 128)), 1.0, 0.0)
            sel[pl.ds(pl.multiple_of(g * 16, 16), 16), t * 128:(t + 1) * 128] = hit.astype(BF16)
        return 0

    with jax.named_scope("ph_sel"):
        lax.fori_loop(0, 2 * n_usr // 16, sel_step, 0, unroll=2)
    with jax.named_scope("ph_up_wait"):
        rc_up.wait()
    u12 = (up[...] + up_r[...]).astype(BF16)

    def chunk2(j):
        cols = pl.ds(pl.multiple_of(j * CH, CH), CH)
        return remote(i2p.at[:, cols], i2r.at[:, cols], cs2.at[j], cr2.at[j], sib)

    def chunk3(j):
        cols = pl.ds(pl.multiple_of(j * CH, CH), CH)
        return remote(i1p.at[:, cols], i1r.at[:, cols], cs3.at[j], cr3.at[j], sib)

    nw = WIDE // CH

    def item_step(i, _):
        cols = pl.ds(pl.multiple_of(i * WIDE, WIDE), WIDE)
        part = jnp.dot(u12, adj[:, cols], preferred_element_type=F32)
        i2p[:, cols] = part[0:dim]
        i1p[:, cols] = part[dim:2 * dim]
        for t in range(nw):
            chunk2(i * nw + t).start()
        return 0

    def send3(j, _):
        chunk3(j).start()
        return 0

    with jax.named_scope("ph_item"):
        lax.fori_loop(0, n_itm // WIDE, item_step, 0)
        pl.semaphore_wait(free_sem, 1)
        lax.fori_loop(0, nch, send3, 0)

    u3p[...] = jnp.zeros_like(u3p)

    def user3_step(i, _):
        cols = pl.ds(pl.multiple_of(i * WIDE, WIDE), WIDE)
        for t in range(nw):
            chunk2(i * nw + t).wait_recv()
        v2 = (i2p[:, cols] + i2r[:, cols]).astype(BF16)
        it2[:, cols] = v2
        u3p[...] += dot_t(v2, adj[:, cols])
        return 0

    with jax.named_scope("ph_user3"):
        lax.fori_loop(0, n_itm // WIDE, user3_step, 0)
    rc_u3 = remote(u3p, u3_r, ssem.at[5], rsem.at[5], xpeer)
    rc_u3.start()

    def final_step(k, _):
        cols = pl.ds(pl.multiple_of(k * CH, CH), CH)
        chunk3(k).wait_recv()
        v3 = (i1p[:, cols] + i1r[:, cols]).astype(BF16)
        acc = it0[:, cols].astype(F32) + it1[:, cols].astype(F32)
        acc = (acc + it2[:, cols].astype(F32)) + v3.astype(F32)
        fin = (acc * (1.0 / (NUM_LAYERS + 1))).astype(BF16)
        it1[:, cols] = fin
        fin = fin.astype(F32)
        for b in range(CH // 128):
            blk = fin[:, b * 128:(b + 1) * 128]
            table[pl.ds(pl.multiple_of(k * CH + b * 128, 128), 128), :] = jnp.concatenate([blk] * 4, axis=0).T
        return 0

    with jax.named_scope("ph_final"):
        lax.fori_loop(0, nch, final_step, 0)
    cp_oi = pltpu.make_async_copy(it1.at[:, pl.ds(pl.multiple_of(r * half, half), half)], oi_ref, lsem.at[1])
    cp_oi.start()

    lane_blk = lax.broadcasted_iota(jnp.int32, (1, 128), 1) // dim

    def pack(rows4):
        d = rows4[0]
        for b in range(1, 4):
            d = jnp.where(lane_blk == b, rows4[b], d)
        return d

    def d_send(ah):
        rows = pl.ds(pl.multiple_of(ah * 128, 128), 128)
        return remote(dbuf.at[1, rows, :], drecv.at[rows, :], ds.at[ah], dr.at[ah], xpeer)

    def diff_rows(q, ah):
        first = (lax.rem(c + q, 2) * 2 + r) * (nhome // 128) + ah

        def body(al, _):
            out = []
            for b in range(4):
                row = first + b * (hrow // 128)
                p = idx_s[al, row]
                n = idx_s[al, nrow + row]
                out.append(table[pl.ds(p, 1), :] - table[pl.ds(n, 1), :])
            dbuf[q, pl.ds(pl.multiple_of(ah * 128, 128) + al, 1), :] = pack(out)
            return 0

        lax.fori_loop(0, 128, body, 0, unroll=8)

    def diff_send(ah, _):
        diff_rows(1, ah)
        d_send(ah).start()
        return 0

    def diff_keep(ah, _):
        diff_rows(0, ah)
        return 0

    with jax.named_scope("ph_diff"):
        lax.fori_loop(0, hrow // 128, diff_send, 0)
    with jax.named_scope("ph_diff"):
        lax.fori_loop(0, hrow // 128, diff_keep, 0)

    with jax.named_scope("ph_u3_wait"):
        rc_u3.wait()
    u3 = (u3p[...] + u3_r[...]).astype(BF16).astype(F32)
    uacc = ut0[...].astype(F32) + u12[0:dim].astype(F32)
    uacc = (uacc + u12[dim:2 * dim].astype(F32)) + u3
    fin_u = (uacc * (1.0 / (NUM_LAYERS + 1))).astype(BF16)
    own_cols = pl.ds(pl.multiple_of(r * n_usr, n_usr), n_usr)
    uall[:, own_cols] = fin_u
    rc_uf = remote(uall.at[:, own_cols], uall.at[:, own_cols], ssem.at[6], rsem.at[6], sib)
    rc_uf.start()
    oufin[...] = uall[:, pl.ds(pl.multiple_of(r * n_usr + c * uh, uh), uh)]
    cp_ou = pltpu.make_async_copy(oufin, ou_ref, lsem.at[2])
    cp_ou.start()
    with jax.named_scope("ph_uf_wait"):
        rc_uf.wait()
    urow = jnp.dot(uall[...], sel[...], preferred_element_type=F32)

    with jax.named_scope("ph_d_wait"):
        for ah in range(hrow // 128):
            d_send(ah).wait()
    dsum = (dbuf[0] + drecv[...]).T
    for b in range(4):
        prod = dsum[b * dim:(b + 1) * dim, :] * urow[:, b * hrow:(b + 1) * hrow]
        s = jnp.sum(prod, axis=0, keepdims=True)
        for h in range(hrow // 128):
            sbuf[pl.ds(b * (hrow // 128) + h, 1), :] = s[:, h * 128:(h + 1) * 128]

    def s_send(q):
        dev = {"emb": lax.rem(e + q // 4, 2), "col": lax.rem(c + (q // 2) % 2, 2), "row": lax.rem(r + q % 2, 2)}
        return remote(sbuf, srecv.at[q - 1], bs.at[q - 1], br.at[q - 1], dev)

    for q in range(7, 0, -1):
        s_send(q).start()
    with jax.named_scope("ph_s_wait"):
        for q in range(7, 0, -1):
            s_send(q).wait()
    for q in range(4):
        own = sbuf[...] if q == 0 else srecv[q - 1]
        x = own + srecv[q + 3]
        hq = lax.rem(c + q // 2, 2) * 2 + lax.rem(r + q % 2, 2)
        ls = jnp.maximum(-x, 0.0) + jnp.log1p(jnp.exp(-jnp.abs(x)))
        lbuf[pl.ds(pl.multiple_of(hq * (nhome // 128), 8), nhome // 128), :] = ls
    cp_l = pltpu.make_async_copy(lbuf, loss_ref, lsem.at[0])
    cp_l.start()

    def drain(j, _):
        chunk2(j).wait_send()
        chunk3(j).wait_send()
        return 0
    with jax.named_scope("ph_drain"):
        lax.fori_loop(0, nch, drain, 0)

    cp_oi.wait()
    cp_ou.wait()
    cp_l.wait()


def solution(mesh):
    def local_fn(mask_blk, user_sh, item_sh, triples):
        n_usr, n_itm = mask_blk.shape
        dim = user_sh.shape[1]
        n_trip = triples.shape[0]
        nch = n_itm // CH
        half = n_itm // 2
        tri = triples.T
        vm = pltpu.VMEM
        dma = pltpu.SemaphoreType.DMA
        nhome = n_trip // 4
        hrow = nhome // 4
        scratch = [
            vm((NSLOT, n_usr, MC), jnp.int32), vm((n_usr, n_itm), BF16), vm((n_usr, 128), F32),
            vm((n_itm // MC, MC), F32), vm((n_itm // MC, MC), F32), vm((1, n_usr), F32), vm((1, n_usr), F32),
            vm((n_usr, 128), F32), vm((n_itm // MC, MC), F32),
            vm((dim, n_itm), BF16), vm((dim, n_itm), BF16), vm((dim, n_itm), BF16), vm((dim, n_usr), BF16),
            vm((dim, n_itm), F32), vm((dim, n_itm), F32), vm((dim, n_itm), F32), vm((dim, n_itm), F32),
            vm((2 * dim, n_usr), F32), vm((2 * dim, n_usr), F32), vm((dim, n_usr), F32), vm((dim, n_usr), F32),
            vm((dim, 2 * n_usr), BF16), vm((2 * n_usr, nhome), BF16), vm((dim, n_usr // 2), BF16),
            vm((n_itm + 8, 128), F32),
            vm((3, n_trip), jnp.int32), vm((128, 128), jnp.int32), vm((128, 128), jnp.int32),
            pltpu.SMEM((128, 128), jnp.int32),
            vm((2, hrow, 128), F32), vm((hrow, 128), F32),
            vm((nhome // 128, 128), F32), vm((7, nhome // 128, 128), F32), vm((n_trip // 128, 128), F32),
            dma((NSLOT,)), dma((3,)), dma((7,)), dma((7,)),
            dma((nch,)), dma((nch,)), dma((nch,)), dma((nch,)), dma((nch,)), dma((nch,)),
            dma((hrow // 128,)), dma((hrow // 128,)), dma((7,)), dma((7,)), pltpu.SemaphoreType.REGULAR,
        ]
        any_spec = pl.BlockSpec(memory_space=pl.ANY)
        ou, oi, loss = pl.pallas_call(
            functools.partial(kernel, n_usr, n_itm, dim, n_trip),
            out_shape=(jax.ShapeDtypeStruct((dim, n_usr // 2), BF16),
                       jax.ShapeDtypeStruct((dim, half), BF16),
                       jax.ShapeDtypeStruct((n_trip // 128, 128), F32)),
            in_specs=[any_spec] * 4,
            out_specs=(any_spec,) * 3,
            scratch_shapes=scratch,
            compiler_params=pltpu.CompilerParams(collective_id=0, has_side_effects=True,
                                                 vmem_limit_bytes=62 * 1024 * 1024),
            name="gcn",
        )(mask_blk, user_sh.T, item_sh.T, tri)
        return ou.T, oi.T, loss.reshape(n_trip)

    return jax.shard_map(
        local_fn, mesh=mesh,
        in_specs=(P("row", "col"), P(("row", "col"), "emb"), P(("col", "row"), "emb"), P()),
        out_specs=(P(("row", "col"), "emb"), P(("col", "row"), "emb"), P()),
        check_vma=False)
```

```python
import functools

import jax
import jax.numpy as jnp
from jax import lax
from jax.experimental import pallas as pl
from jax.experimental.pallas import tpu as pltpu
from jax.sharding import PartitionSpec as P

NUM_LAYERS = 3
CH = 1024
MC = 512
NSLOT = 6
WIDE = 4096
MESH = pl.DeviceIdType.MESH
F32 = jnp.float32
BF16 = jnp.bfloat16


def remote(src, dst, ssem, rsem, dev):
    return pltpu.make_async_remote_copy(src_ref=src, dst_ref=dst, send_sem=ssem, recv_sem=rsem,
                                        device_id=dev, device_id_type=MESH)


def kernel(n_usr, n_itm, dim, n_trip,
           mask_ref, eu_ref, ei_ref, tri_ref, ou_ref, oi_ref, loss_ref,
           stage, adj, rowacc, degi, degi_r, degu, degu_r, invu, invi,
           it0, it1, it2, ut0, i1p, i1r, i2p, i2r,
           up, up_r, u3p, u3_r, uall, sel, table,
           tri_v, idx_v, idx_t, idx_s, dbuf, drecv, sbuf, srecv,
           msem, lsem, ssem, rsem, cs1, cr1, cs2, cr2, cs3, cr3, ds, dr, bs, br, free_sem):
    e = lax.axis_index("emb")
    c = lax.axis_index("col")
    r = lax.axis_index("row")
    sib = {"row": 1 - r}
    xpeer = {"col": 1 - c}
    nch = n_itm // CH
    half = n_itm // 2
    uh = n_usr // 2
    nhome = n_trip // 4
    hrow = nhome // 4

    def mask_copy(j):
        slot = lax.rem(j, NSLOT)
        return pltpu.make_async_copy(mask_ref.at[:, pl.ds(pl.multiple_of(j * MC, MC), MC)], stage.at[slot], msem.at[slot])

    for j in range(NSLOT):
        mask_copy(j).start()
    own_i = it0.at[:, pl.ds(pl.multiple_of(r * half, half), half)]
    own_u = ut0.at[:, pl.ds(pl.multiple_of(c * uh, uh), uh)]
    cp_i = pltpu.make_async_copy(ei_ref, own_i, lsem.at[0])
    cp_u = pltpu.make_async_copy(eu_ref, own_u, lsem.at[1])
    cp_t = pltpu.make_async_copy(tri_ref, tri_v, lsem.at[2])
    cp_i.start()
    cp_u.start()
    cp_t.start()

    barrier = pltpu.get_barrier_semaphore()
    for q in range(1, 8):
        dev = {"emb": lax.rem(e + q // 4, 2), "col": lax.rem(c + (q // 2) % 2, 2), "row": lax.rem(r + q % 2, 2)}
        pl.semaphore_signal(barrier, inc=1, device_id=dev, device_id_type=MESH)

    rowacc[...] = jnp.zeros_like(rowacc)

    def mask_step(j, _):
        slot = lax.rem(j, NSLOT)
        mask_copy(j).wait()
        cols = pl.ds(pl.multiple_of(j * MC, MC), MC)

        def rows_step(g, acc):
            rows = pl.ds(pl.multiple_of(g * 16, 16), 16)
            m = stage[slot, rows, :].astype(F32)
            adj[rows, cols] = m.astype(BF16)
            s = m[:, 0:128]
            for k in range(1, MC // 128):
                s = s + m[:, k * 128:(k + 1) * 128]
            rowacc[rows, :] += s
            return acc + (m[0:8] + m[8:16])

        acc = lax.fori_loop(0, n_usr // 16, rows_step, jnp.zeros((8, MC), F32), unroll=2)
        degi[pl.ds(j, 1), :] = jnp.sum(acc, axis=0, keepdims=True)

        @pl.when(j + NSLOT < n_itm // MC)
        def _():
            mask_copy(j + NSLOT).start()
        return 0

    with jax.named_scope("ph_mask0"):
        lax.fori_loop(0, 8, mask_step, 0)
    cp_i.wait()
    cp_u.wait()
    cp_t.wait()
    with jax.named_scope("ph_barrier"):
        pl.semaphore_wait(barrier, 7)
    rc_i = remote(own_i, own_i, ssem.at[0], rsem.at[0], sib)
    rc_u = remote(own_u, own_u, ssem.at[1], rsem.at[1], xpeer)
    rc_i.start()
    rc_u.start()
    with jax.named_scope("ph_mask1"):
        lax.fori_loop(8, n_itm // MC, mask_step, 0)

    degu[...] = jnp.sum(rowacc[...].T, axis=0, keepdims=True)
    rc_du = remote(degu, degu_r, ssem.at[2], rsem.at[2], xpeer)
    rc_di = remote(degi, degi_r, ssem.at[3], rsem.at[3], sib)
    rc_du.start()
    rc_di.start()

    def tri_row(k, row):
        return tri_v[pl.ds(k, 1), pl.ds(pl.multiple_of(row * 128, 128), 128)]

    def home_row(q):
        return (lax.rem(c + q, 2) * 2 + r) * (nhome // 128)

    nah = hrow // 128
    ncol = 8 * nah
    idx_v[...] = jnp.zeros_like(idx_v)
    for k in range(2):
        for q in range(2):
            for ah in range(nah):
                for b in range(4):
                    col = k * ncol + (q * nah + ah) * 4 + b
                    idx_v[pl.ds(col, 1), :] = tri_row(k + 1, home_row(q) + b * nah + ah)
    loc = idx_v[0:2 * ncol, :] - c * n_itm
    idx_v[0:2 * ncol, :] = jnp.where((loc >= 0) & (loc < n_itm), loc, n_itm)
    idx_t[...] = idx_v[...].T
    cp_x = pltpu.make_async_copy(idx_t, idx_s, lsem.at[0])
    cp_x.start()
    table[pl.ds(n_itm, 8), :] = jnp.zeros((8, 128), F32)

    with jax.named_scope("ph_di_wait"):
        rc_di.wait()
    invi[...] = lax.rsqrt(jnp.maximum(degi[...] + degi_r[...], 1.0))
    rc_i.wait()
    rc_u.wait()
    cp_x.wait()
    with jax.named_scope("ph_du_wait"):
        rc_du.wait()
    inv_row = lax.rsqrt(jnp.maximum(degu[...] + degu_r[...], 1.0))
    invu[...] = jnp.broadcast_to(inv_row, (128, n_usr)).T

    def chunk1(j):
        cols = pl.ds(pl.multiple_of(j * CH, CH), CH)
        return remote(i1p.at[:, cols], i1r.at[:, cols], cs1.at[j], cr1.at[j], sib)

    def build_step(i, _):
        for jj in range(2):
            j = i * 2 + jj
            for nt in range(CH // 256):
                cols = pl.ds(pl.multiple_of(j * CH + nt * 256, 256), 256)
                lane = nt * 256 % MC
                wi = jnp.broadcast_to(invi[pl.ds(j * (CH // MC) + nt * 256 // MC, 1), lane:lane + 256], (16, 256))
                part = None
                for kt in range(n_usr // 256):
                    tiles = []
                    for g in range(16):
                        rows = pl.ds(kt * 256 + g * 16, 16)
                        wu = jnp.concatenate([invu[rows, :]] * 2, axis=1)
                        a = (wu * wi).astype(BF16) * adj[rows, cols]
                        adj[rows, cols] = a
                        tiles.append(a)
                    p = jnp.dot(ut0[:, kt * 256:(kt + 1) * 256], jnp.concatenate(tiles, axis=0),
                                preferred_element_type=F32)
                    part = p if part is None else part + p
                i1p[:, cols] = part
        for jj in range(2):
            chunk1(i * 2 + jj).start()
        return 0

    with jax.named_scope("ph_build"):
        lax.fori_loop(0, nch // 2, build_step, 0)

    def dot_t(lhs, a):
        return lax.dot_general(lhs, a, (((1,), (1,)), ((), ())), preferred_element_type=F32)

    up[...] = jnp.zeros_like(up)

    def user_step(i, _):
        cols = pl.ds(pl.multiple_of(i * WIDE, WIDE), WIDE)
        for t in range(WIDE // CH):
            chunk1(i * (WIDE // CH) + t).wait_recv()
        v1 = (i1p[:, cols] + i1r[:, cols]).astype(BF16)
        it1[:, cols] = v1
        lhs = jnp.concatenate([it0[:, cols], v1], axis=0)
        up[...] += dot_t(lhs, adj[:, cols])
        return 0

    with jax.named_scope("ph_user"):
        lax.fori_loop(0, n_itm // WIDE, user_step, 0)
    rc_up = remote(up, up_r, ssem.at[4], rsem.at[4], xpeer)
    rc_up.start()
    pl.semaphore_signal(free_sem, inc=1, device_id=sib, device_id_type=MESH)

    def sent1(j, _):
        chunk1(j).wait_send()
        return 0
    lax.fori_loop(0, nch, sent1, 0)
    def sel_step(g, _):
        users = lax.broadcasted_iota(jnp.int32, (16, 128), 0) + g * 16
        for t in range(nhome // 128):
            ids = tri_row(0, home_row(0) + t)
            hit = jnp.where(users == jnp.broadcast_to(ids, (16, 128)), 1.0, 0.0)
            sel[pl.ds(pl.multiple_of(g * 16, 16), 16), t * 128:(t + 1) * 128] = hit.astype(BF16)
        return 0

    with jax.named_scope("ph_sel"):
        lax.fori_loop(0, 2 * n_usr // 16, sel_step, 0, unroll=2)
    with jax.named_scope("ph_up_wait"):
        rc_up.wait()
    u12 = (up[...] + up_r[...]).astype(BF16)

    def chunk2(j):
        cols = pl.ds(pl.multiple_of(j * CH, CH), CH)
        return remote(i2p.at[:, cols], i2r.at[:, cols], cs2.at[j], cr2.at[j], sib)

    def chunk3(j):
        cols = pl.ds(pl.multiple_of(j * CH, CH), CH)
        return remote(i1p.at[:, cols], i1r.at[:, cols], cs3.at[j], cr3.at[j], sib)

    nw = WIDE // CH

    def item_step(i, _):
        cols = pl.ds(pl.multiple_of(i * WIDE, WIDE), WIDE)
        part = jnp.dot(u12, adj[:, cols], preferred_element_type=F32)
        i2p[:, cols] = part[0:dim]
        i1p[:, cols] = part[dim:2 * dim]
        for t in range(nw):
            chunk2(i * nw + t).start()
        return 0

    def send3(j, _):
        chunk3(j).start()
        return 0

    with jax.named_scope("ph_item"):
        lax.fori_loop(0, n_itm // WIDE, item_step, 0)
        pl.semaphore_wait(free_sem, 1)
        lax.fori_loop(0, nch, send3, 0)

    u3p[...] = jnp.zeros_like(u3p)

    def user3_step(i, _):
        cols = pl.ds(pl.multiple_of(i * WIDE, WIDE), WIDE)
        for t in range(nw):
            chunk2(i * nw + t).wait_recv()
        v2 = (i2p[:, cols] + i2r[:, cols]).astype(BF16)
        it2[:, cols] = v2
        u3p[...] += dot_t(v2, adj[:, cols])
        return 0

    with jax.named_scope("ph_user3"):
        lax.fori_loop(0, n_itm // WIDE, user3_step, 0)
    rc_u3 = remote(u3p, u3_r, ssem.at[5], rsem.at[5], xpeer)
    rc_u3.start()

    def final_step(k, _):
        cols = pl.ds(pl.multiple_of(k * CH, CH), CH)
        chunk3(k).wait_recv()
        v3 = (i1p[:, cols] + i1r[:, cols]).astype(BF16)
        acc = it0[:, cols].astype(F32) + it1[:, cols].astype(F32)
        acc = (acc + it2[:, cols].astype(F32)) + v3.astype(F32)
        fin = (acc * (1.0 / (NUM_LAYERS + 1))).astype(BF16)
        it1[:, cols] = fin
        fin = fin.astype(F32)
        for b in range(CH // 128):
            blk = fin[:, b * 128:(b + 1) * 128]
            table[pl.ds(pl.multiple_of(k * CH + b * 128, 128), 128), :] = jnp.concatenate([blk] * 4, axis=0).T
        return 0

    with jax.named_scope("ph_final"):
        lax.fori_loop(0, nch, final_step, 0)
    oi_ref[...] = it1[:, pl.ds(pl.multiple_of(r * half, half), half)]

    lane_blk = lax.broadcasted_iota(jnp.int32, (1, 128), 1) // dim

    def pack(rows4):
        d = rows4[0]
        for b in range(1, 4):
            d = jnp.where(lane_blk == b, rows4[b], d)
        return d

    def d_send(ah):
        rows = pl.ds(pl.multiple_of(ah * 128, 128), 128)
        return remote(dbuf.at[1, rows, :], drecv.at[rows, :], ds.at[ah], dr.at[ah], xpeer)

    def diff_rows(q, ah):
        def body(al, _):
            out = []
            for b in range(4):
                col = (q * nah + ah) * 4 + b
                p = idx_s[al, col]
                n = idx_s[al, ncol + col]
                out.append(table[pl.ds(p, 1), :] - table[pl.ds(n, 1), :])
            dbuf[q, pl.ds(ah * 128 + al, 1), :] = pack(out)
            return 0

        lax.fori_loop(0, 128, body, 0, unroll=8)

    with jax.named_scope("ph_diff"):
        for ah in range(nah):
            diff_rows(1, ah)
            d_send(ah).start()
    with jax.named_scope("ph_diff"):
        for ah in range(nah):
            diff_rows(0, ah)

    with jax.named_scope("ph_u3_wait"):
        rc_u3.wait()
    u3 = (u3p[...] + u3_r[...]).astype(BF16).astype(F32)
    uacc = ut0[...].astype(F32) + u12[0:dim].astype(F32)
    uacc = (uacc + u12[dim:2 * dim].astype(F32)) + u3
    fin_u = (uacc * (1.0 / (NUM_LAYERS + 1))).astype(BF16)
    own_cols = pl.ds(pl.multiple_of(r * n_usr, n_usr), n_usr)
    uall[:, own_cols] = fin_u
    rc_uf = remote(uall.at[:, own_cols], uall.at[:, own_cols], ssem.at[6], rsem.at[6], sib)
    rc_uf.start()
    ou_ref[...] = uall[:, pl.ds(pl.multiple_of(r * n_usr + c * uh, uh), uh)]
    with jax.named_scope("ph_uf_wait"):
        rc_uf.wait()
    urow = jnp.dot(uall[...], sel[...], preferred_element_type=F32)

    with jax.named_scope("ph_d_wait"):
        for ah in range(hrow // 128):
            d_send(ah).wait()
    dsum = (dbuf[0] + drecv[...]).T
    for b in range(4):
        prod = dsum[b * dim:(b + 1) * dim, :] * urow[:, b * hrow:(b + 1) * hrow]
        s = jnp.sum(prod, axis=0, keepdims=True)
        for h in range(hrow // 128):
            sbuf[pl.ds(b * (hrow // 128) + h, 1), :] = s[:, h * 128:(h + 1) * 128]

    def s_send(q):
        dev = {"emb": lax.rem(e + q // 4, 2), "col": lax.rem(c + (q // 2) % 2, 2), "row": lax.rem(r + q % 2, 2)}
        return remote(sbuf, srecv.at[q - 1], bs.at[q - 1], br.at[q - 1], dev)

    for q in range(7, 0, -1):
        s_send(q).start()
    with jax.named_scope("ph_s_wait"):
        for q in range(7, 0, -1):
            s_send(q).wait()
    for q in range(4):
        own = sbuf[...] if q == 0 else srecv[q - 1]
        x = own + srecv[q + 3]
        hq = lax.rem(c + q // 2, 2) * 2 + lax.rem(r + q % 2, 2)
        ls = jnp.maximum(-x, 0.0) + jnp.log1p(jnp.exp(-jnp.abs(x)))
        loss_ref[pl.ds(pl.multiple_of(hq * (nhome // 128), 8), nhome // 128), :] = ls

    def drain(j, _):
        chunk2(j).wait_send()
        chunk3(j).wait_send()
        return 0
    with jax.named_scope("ph_drain"):
        lax.fori_loop(0, nch, drain, 0)


def store_kernel(*refs):
    srcs, dsts, sem = refs[0:3], refs[3:6], refs[6]
    copies = [pltpu.make_async_copy(a, b, sem.at[k]) for k, (a, b) in enumerate(zip(srcs, dsts))]
    for copy in copies:
        copy.start()
    for copy in copies:
        copy.wait()


def solution(mesh):
    def local_fn(mask_blk, user_sh, item_sh, triples):
        n_usr, n_itm = mask_blk.shape
        dim = user_sh.shape[1]
        n_trip = triples.shape[0]
        nch = n_itm // CH
        half = n_itm // 2
        tri = triples.T
        vm = pltpu.VMEM
        dma = pltpu.SemaphoreType.DMA
        nhome = n_trip // 4
        hrow = nhome // 4
        scratch = [
            vm((NSLOT, n_usr, MC), jnp.int32), vm((n_usr, n_itm), BF16), vm((n_usr, 128), F32),
            vm((n_itm // MC, MC), F32), vm((n_itm // MC, MC), F32), vm((1, n_usr), F32), vm((1, n_usr), F32),
            vm((n_usr, 128), F32), vm((n_itm // MC, MC), F32),
            vm((dim, n_itm), BF16), vm((dim, n_itm), BF16), vm((dim, n_itm), BF16), vm((dim, n_usr), BF16),
            vm((dim, n_itm), F32), vm((dim, n_itm), F32), vm((dim, n_itm), F32), vm((dim, n_itm), F32),
            vm((2 * dim, n_usr), F32), vm((2 * dim, n_usr), F32), vm((dim, n_usr), F32), vm((dim, n_usr), F32),
            vm((dim, 2 * n_usr), BF16), vm((2 * n_usr, nhome), BF16),
            vm((n_itm + 8, 128), F32),
            vm((3, n_trip), jnp.int32), vm((128, 128), jnp.int32), vm((128, 128), jnp.int32),
            pltpu.SMEM((128, 128), jnp.int32),
            vm((2, hrow, 128), F32), vm((hrow, 128), F32),
            vm((nhome // 128, 128), F32), vm((7, nhome // 128, 128), F32),
            dma((NSLOT,)), dma((3,)), dma((7,)), dma((7,)),
            dma((nch,)), dma((nch,)), dma((nch,)), dma((nch,)), dma((nch,)), dma((nch,)),
            dma((hrow // 128,)), dma((hrow // 128,)), dma((7,)), dma((7,)), pltpu.SemaphoreType.REGULAR,
        ]
        hbm_spec = pl.BlockSpec(memory_space=pltpu.HBM)
        vmem_spec = pl.BlockSpec(memory_space=pltpu.VMEM)
        ou, oi, loss = pl.pallas_call(
            functools.partial(kernel, n_usr, n_itm, dim, n_trip),
            out_shape=(jax.ShapeDtypeStruct((dim, n_usr // 2), BF16),
                       jax.ShapeDtypeStruct((dim, half), BF16),
                       jax.ShapeDtypeStruct((n_trip // 128, 128), F32)),
            in_specs=[hbm_spec] * 4,
            out_specs=(vmem_spec,) * 3,
            scratch_shapes=scratch,
            compiler_params=pltpu.CompilerParams(collective_id=0, has_side_effects=True,
                                                 vmem_limit_bytes=50 * 1024 * 1024),
            name="gcn",
        )(mask_blk, *[pltpu.with_memory_space_constraint(v, pltpu.HBM) for v in (user_sh.T, item_sh.T, tri)])
        ou, oi, loss = pl.pallas_call(
            store_kernel,
            out_shape=tuple(jax.ShapeDtypeStruct(v.shape, v.dtype) for v in (ou, oi, loss)),
            in_specs=[vmem_spec] * 3,
            out_specs=(pl.BlockSpec(memory_space=pl.ANY),) * 3,
            scratch_shapes=[dma((3,))],
            compiler_params=pltpu.CompilerParams(vmem_limit_bytes=4 * 1024 * 1024),
            name="store",
        )(ou, oi, loss)
        return ou.T, oi.T, loss.reshape(n_trip)

    return jax.shard_map(
        local_fn, mesh=mesh,
        in_specs=(P("row", "col"), P(("row", "col"), "emb"), P(("col", "row"), "emb"), P()),
        out_specs=(P(("row", "col"), "emb"), P(("col", "row"), "emb"), P()),
        check_vma=False)
```

```python
import functools

import jax
import jax.numpy as jnp
from jax import lax
from jax.experimental import pallas as pl
from jax.experimental.pallas import tpu as pltpu
from jax.sharding import PartitionSpec as P

NUM_LAYERS = 3
CH = 2048
MC = 512
NSLOT = 6
FIN = 4096
WIDE = 8192
NARROW = 4096
MESH = pl.DeviceIdType.MESH
F32 = jnp.float32
BF16 = jnp.bfloat16


def remote(src, dst, ssem, rsem, dev):
    return pltpu.make_async_remote_copy(src_ref=src, dst_ref=dst, send_sem=ssem, recv_sem=rsem,
                                        device_id=dev, device_id_type=MESH)


def kernel(n_usr, n_itm, dim, n_trip,
           mask_ref, eu_ref, ei_ref, tri_ref, ou_ref, oi_ref, loss_ref,
           stage, adj, rowacc, degi, degi_r, degu, degu_r, invu, invi,
           it0, it1, it2, ut0, i1p, i1r, i2p, i2r,
           up, up_r, u3p, u3_r, uall, sel, table,
           tri_v, idx_v, idx_t, idx_s, dbuf, dt, drecv, sbuf, srecv,
           msem, lsem, ssem, rsem, cs1, cr1, cs2, cr2, ds, dr, bs, br, free_sem):
    e = lax.axis_index("emb")
    c = lax.axis_index("col")
    r = lax.axis_index("row")
    sib = {"row": 1 - r}
    xpeer = {"col": 1 - c}
    nch = n_itm // CH
    half = n_itm // 2
    uh = n_usr // 2
    nhome = n_trip // 4
    hrow = nhome // 4

    def mask_copy(j):
        slot = lax.rem(j, NSLOT)
        return pltpu.make_async_copy(mask_ref.at[:, pl.ds(pl.multiple_of(j * MC, MC), MC)], stage.at[slot], msem.at[slot])

    for j in range(NSLOT):
        mask_copy(j).start()
    own_i = it0.at[:, pl.ds(pl.multiple_of(r * half, half), half)]
    own_u = ut0.at[:, pl.ds(pl.multiple_of(c * uh, uh), uh)]
    cp_i = pltpu.make_async_copy(ei_ref, own_i, lsem.at[0])
    cp_u = pltpu.make_async_copy(eu_ref, own_u, lsem.at[1])
    cp_t = pltpu.make_async_copy(tri_ref, tri_v, lsem.at[2])
    cp_i.start()
    cp_u.start()
    cp_t.start()

    barrier = pltpu.get_barrier_semaphore()
    for q in range(1, 8):
        dev = {"emb": lax.rem(e + q // 4, 2), "col": lax.rem(c + (q // 2) % 2, 2), "row": lax.rem(r + q % 2, 2)}
        pl.semaphore_signal(barrier, inc=1, device_id=dev, device_id_type=MESH)

    rowacc[...] = jnp.zeros_like(rowacc)

    def mask_step(j, _):
        slot = lax.rem(j, NSLOT)
        mask_copy(j).wait()
        cols = pl.ds(pl.multiple_of(j * MC, MC), MC)

        def rows_step(g, acc):
            rows = pl.ds(pl.multiple_of(g * 16, 16), 16)
            m = stage[slot, rows, :].astype(F32)
            adj[rows, cols] = m.astype(BF16)
            s = m[:, 0:128]
            for k in range(1, MC // 128):
                s = s + m[:, k * 128:(k + 1) * 128]
            rowacc[rows, :] += s
            return acc + (m[0:8] + m[8:16])

        acc = lax.fori_loop(0, n_usr // 16, rows_step, jnp.zeros((8, MC), F32), unroll=2)
        degi[pl.ds(j, 1), :] = jnp.sum(acc, axis=0, keepdims=True)

        @pl.when(j + NSLOT < n_itm // MC)
        def _():
            mask_copy(j + NSLOT).start()
        return 0

    with jax.named_scope("ph_mask0"):
        lax.fori_loop(0, 8, mask_step, 0)
    cp_i.wait()
    cp_u.wait()
    cp_t.wait()
    with jax.named_scope("ph_barrier"):
        pl.semaphore_wait(barrier, 7)
    rc_i = remote(own_i, own_i, ssem.at[0], rsem.at[0], sib)
    rc_u = remote(own_u, own_u, ssem.at[1], rsem.at[1], xpeer)
    rc_i.start()
    rc_u.start()
    with jax.named_scope("ph_mask1"):
        lax.fori_loop(8, n_itm // MC, mask_step, 0)

    degu[...] = jnp.sum(rowacc[...].T, axis=0, keepdims=True)
    rc_du = remote(degu, degu_r, ssem.at[2], rsem.at[2], xpeer)
    rc_di = remote(degi, degi_r, ssem.at[3], rsem.at[3], sib)
    rc_du.start()
    rc_di.start()

    def tri_row(k, row):
        return tri_v[pl.ds(k, 1), pl.ds(pl.multiple_of(row * 128, 128), 128)]

    def home_row(q):
        return (lax.rem(c + q, 2) * 2 + r) * (nhome // 128)

    nrow = nhome // 128
    ncol = 2 * nrow
    idx_v[...] = jnp.zeros_like(idx_v)
    for k in range(2):
        for q in range(2):
            for row in range(nrow):
                idx_v[pl.ds(k * ncol + q * nrow + row, 1), :] = tri_row(k + 1, home_row(q) + row)
    loc = idx_v[0:2 * ncol, :] - c * n_itm
    idx_v[0:2 * ncol, :] = jnp.where((loc >= 0) & (loc < n_itm), loc, n_itm)
    idx_t[...] = idx_v[...].T
    cp_x = pltpu.make_async_copy(idx_t, idx_s, lsem.at[0])
    cp_x.start()
    table[pl.ds(n_itm, 8), :] = jnp.zeros((8, dim), F32)

    with jax.named_scope("ph_di_wait"):
        rc_di.wait()
    invi[...] = lax.rsqrt(jnp.maximum(degi[...] + degi_r[...], 1.0))
    rc_i.wait()
    rc_u.wait()
    cp_x.wait()
    with jax.named_scope("ph_du_wait"):
        rc_du.wait()
    inv_row = lax.rsqrt(jnp.maximum(degu[...] + degu_r[...], 1.0))
    invu[...] = jnp.broadcast_to(inv_row, (128, n_usr)).T

    nst = n_itm // WIDE

    def chunk1(j):
        cols = pl.ds(pl.multiple_of(j * CH, CH), CH)
        return remote(i1p.at[:, cols], i1r.at[:, cols], cs1, cr1.at[j // (WIDE // CH)], sib)

    def step1(i):
        cols = pl.ds(pl.multiple_of(i * WIDE, WIDE), WIDE)
        return remote(i1p.at[:, cols], i1r.at[:, cols], cs1, cr1.at[i], sib)

    def build_step(j, _):
        for nt in range(CH // 256):
            cols = pl.ds(pl.multiple_of(j * CH + nt * 256, 256), 256)
            lane = nt * 256 % MC
            wi = jnp.broadcast_to(invi[pl.ds(j * (CH // MC) + nt * 256 // MC, 1), lane:lane + 256], (16, 256))
            part = None
            for kt in range(n_usr // 256):
                tiles = []
                for g in range(16):
                    rows = pl.ds(kt * 256 + g * 16, 16)
                    wu = jnp.concatenate([invu[rows, :]] * 2, axis=1)
                    a = (wu * wi).astype(BF16) * adj[rows, cols]
                    adj[rows, cols] = a
                    tiles.append(a)
                p = jnp.dot(ut0[:, kt * 256:(kt + 1) * 256], jnp.concatenate(tiles, axis=0),
                            preferred_element_type=F32)
                part = p if part is None else part + p
            i1p[:, cols] = part
        chunk1(j).start()
        return 0

    with jax.named_scope("ph_build"):
        lax.fori_loop(0, nch, build_step, 0)

    def dot_t(a, b):
        return lax.dot_general(a, b, (((1,), (1,)), ((), ())), preferred_element_type=F32)

    up[...] = jnp.zeros_like(up)
    rc_up = []
    for h in range(2):
        rows = pl.ds(h * uh, uh)

        def user_step(i, _, h=h, rows=rows):
            cols = pl.ds(pl.multiple_of(i * WIDE, WIDE), WIDE)
            if h == 0:
                step1(i).wait_recv()
                it1[:, cols] = (i1p[:, cols] + i1r[:, cols]).astype(BF16)
            lhs = jnp.concatenate([it0[:, cols], it1[:, cols]], axis=0)
            up[:, rows] += dot_t(lhs, adj[rows, cols])
            return 0

        with jax.named_scope("ph_user"):
            lax.fori_loop(0, nst, user_step, 0)
        rc_up.append(remote(up.at[:, rows], up_r.at[:, rows], ssem.at[4 + h], rsem.at[4 + h], xpeer))
        rc_up[h].start()
    pl.semaphore_signal(free_sem, inc=1, device_id=sib, device_id_type=MESH)

    remote(i1p, i1r, cs1, cr1.at[0], sib).wait_send()

    def sel_step(g, _):
        users = lax.broadcasted_iota(jnp.int32, (16, 128), 0) + g * 16
        for t in range(nhome // 128):
            ids = tri_row(0, home_row(0) + t)
            hit = jnp.where(users == jnp.broadcast_to(ids, (16, 128)), 1.0, 0.0)
            sel[pl.ds(pl.multiple_of(g * 16, 16), 16), t * 128:(t + 1) * 128] = hit.astype(BF16)
        return 0

    with jax.named_scope("ph_sel"):
        lax.fori_loop(0, 2 * n_usr // 16, sel_step, 0, unroll=2)
    with jax.named_scope("ph_up_wait"):
        rc_up[0].wait()
        rc_up[1].wait()
    u12 = (up[...] + up_r[...]).astype(BF16)

    def part2(i, size, step):
        cols = pl.ds(pl.multiple_of(i * size, size), size)
        return remote(i2p.at[:, cols], i2r.at[:, cols], cs2, cr2.at[step], sib)

    def item_step(i, _):
        cols = pl.ds(pl.multiple_of(i * NARROW, NARROW), NARROW)
        part = jnp.dot(u12, adj[:, cols], preferred_element_type=F32)
        i2p[:, cols] = part[0:dim]
        i1p[:, cols] = part[dim:2 * dim]
        part2(i, NARROW, i // (WIDE // NARROW)).start()
        return 0

    with jax.named_scope("ph_item"):
        lax.fori_loop(0, n_itm // NARROW, item_step, 0)
        pl.semaphore_wait(free_sem, 1)
        for i in range(nst):
            step1(i).start()

    u3p[...] = jnp.zeros_like(u3p)

    def user3_step(i, _):
        cols = pl.ds(pl.multiple_of(i * WIDE, WIDE), WIDE)
        part2(i, WIDE, i).wait_recv()
        v2 = (i2p[:, cols] + i2r[:, cols]).astype(BF16)
        it2[:, cols] = v2
        u3p[...] += dot_t(adj[:, cols], v2).T
        return 0

    with jax.named_scope("ph_user3"):
        lax.fori_loop(0, nst, user3_step, 0)
    rc_u3 = remote(u3p, u3_r, ssem.at[6], rsem.at[6], xpeer)
    rc_u3.start()

    def final_step(k, _):
        cols = pl.ds(pl.multiple_of(k * FIN, FIN), FIN)
        v3 = (i1p[:, cols] + i1r[:, cols]).astype(BF16)
        acc = it0[:, cols].astype(F32) + it1[:, cols].astype(F32)
        acc = (acc + it2[:, cols].astype(F32)) + v3.astype(F32)
        fin = (acc * (1.0 / (NUM_LAYERS + 1))).astype(BF16)
        it1[:, cols] = fin
        fin = fin.astype(F32)
        for b in range(FIN // 128):
            table[pl.ds(pl.multiple_of(k * FIN + b * 128, 128), 128), :] = fin[:, b * 128:(b + 1) * 128].T
        return 0

    with jax.named_scope("ph_final"):
        for i in range(nst):
            step1(i).wait_recv()
        lax.fori_loop(0, n_itm // FIN, final_step, 0)
    oi_ref[...] = it1[:, pl.ds(pl.multiple_of(r * half, half), half)]

    def diff_rows(q, row0):
        def body(al, _):
            for row in (row0, row0 + 1):
                p = idx_s[al, q * nrow + row]
                n = idx_s[al, ncol + q * nrow + row]
                dbuf[pl.ds(row * 128 + al, 1), :] = table[pl.ds(p, 1), :] - table[pl.ds(n, 1), :]
            return 0

        lax.fori_loop(0, 128, body, 0, unroll=16)
        for row in (row0, row0 + 1):
            dt[q, :, row * 128:(row + 1) * 128] = dbuf[row * 128:(row + 1) * 128, :].T

    with jax.named_scope("ph_diff"):
        for row0 in range(0, nrow, 2):
            diff_rows(1, row0)
            cols = pl.ds(row0 * 128, 256)
            remote(dt.at[1, :, cols], drecv.at[:, cols], ds, dr, xpeer).start()

    with jax.named_scope("ph_u3_wait"):
        rc_u3.wait()
    u3 = (u3p[...] + u3_r[...]).astype(BF16).astype(F32)
    uacc = ut0[...].astype(F32) + u12[0:dim].astype(F32)
    uacc = (uacc + u12[dim:2 * dim].astype(F32)) + u3
    fin_u = (uacc * (1.0 / (NUM_LAYERS + 1))).astype(BF16)
    own_cols = pl.ds(pl.multiple_of(r * n_usr, n_usr), n_usr)
    uall[:, own_cols] = fin_u
    rc_uf = remote(uall.at[:, own_cols], uall.at[:, own_cols], ssem.at[7], rsem.at[7], sib)
    rc_uf.start()
    ou_ref[...] = uall[:, pl.ds(pl.multiple_of(r * n_usr + c * uh, uh), uh)]
    with jax.named_scope("ph_diff"):
        for row0 in range(0, nrow, 2):
            diff_rows(0, row0)
    with jax.named_scope("ph_uf_wait"):
        rc_uf.wait()
    urow = jnp.dot(uall[...], sel[...], preferred_element_type=F32)

    with jax.named_scope("ph_d_wait"):
        remote(dt.at[1], drecv, ds, dr, xpeer).wait()
    score = jnp.sum((dt[0] + drecv[...]) * urow, axis=0, keepdims=True)
    for row in range(nrow):
        sbuf[pl.ds(row, 1), :] = score[:, row * 128:(row + 1) * 128]

    def s_send(q):
        dev = {"emb": lax.rem(e + q // 4, 2), "col": lax.rem(c + (q // 2) % 2, 2), "row": lax.rem(r + q % 2, 2)}
        return remote(sbuf, srecv.at[q - 1], bs, br, dev)

    for q in range(7, 0, -1):
        s_send(q).start()
    with jax.named_scope("ph_s_wait"):
        remote(srecv, srecv, bs, br, sib).wait()
    for q in range(4):
        own = sbuf[...] if q == 0 else srecv[q - 1]
        x = own + srecv[q + 3]
        hq = lax.rem(c + q // 2, 2) * 2 + lax.rem(r + q % 2, 2)
        ls = jnp.maximum(-x, 0.0) + jnp.log1p(jnp.exp(-jnp.abs(x)))
        loss_ref[pl.ds(pl.multiple_of(hq * (nhome // 128), 8), nhome // 128), :] = ls

    with jax.named_scope("ph_drain"):
        remote(i2p, i2r, cs2, cr2.at[0], sib).wait_send()
        remote(i1p, i1r, cs1, cr1.at[0], sib).wait_send()


def store_kernel(*refs):
    srcs, dsts, sem = refs[0:3], refs[3:6], refs[6]
    copies = [pltpu.make_async_copy(a, b, sem.at[k]) for k, (a, b) in enumerate(zip(srcs, dsts))]
    for copy in copies:
        copy.start()
    for copy in copies:
        copy.wait()


def solution(mesh):
    def local_fn(mask_blk, user_sh, item_sh, triples):
        n_usr, n_itm = mask_blk.shape
        dim = user_sh.shape[1]
        n_trip = triples.shape[0]
        nch = n_itm // CH
        half = n_itm // 2
        tri = triples.T
        vm = pltpu.VMEM
        dma = pltpu.SemaphoreType.DMA
        nhome = n_trip // 4
        hrow = nhome // 4
        scratch = [
            vm((NSLOT, n_usr, MC), jnp.int32), vm((n_usr, n_itm + 128), BF16), vm((n_usr, 128), F32),
            vm((n_itm // MC, MC), F32), vm((n_itm // MC, MC), F32), vm((1, n_usr), F32), vm((1, n_usr), F32),
            vm((n_usr, 128), F32), vm((n_itm // MC, MC), F32),
            vm((dim, n_itm), BF16), vm((dim, n_itm), BF16), vm((dim, n_itm), BF16), vm((dim, n_usr), BF16),
            vm((dim, n_itm), F32), vm((dim, n_itm), F32), vm((dim, n_itm), F32), vm((dim, n_itm), F32),
            vm((2 * dim, n_usr), F32), vm((2 * dim, n_usr), F32), vm((dim, n_usr), F32), vm((dim, n_usr), F32),
            vm((dim, 2 * n_usr), BF16), vm((2 * n_usr, nhome), BF16),
            vm((n_itm + 8, dim), F32),
            vm((3, n_trip), jnp.int32), vm((128, 128), jnp.int32), vm((128, 128), jnp.int32),
            pltpu.SMEM((128, 128), jnp.int32),
            vm((nhome, dim), F32), vm((2, dim, nhome), F32), vm((dim, nhome), F32),
            vm((nhome // 128, 128), F32), vm((7, nhome // 128, 128), F32),
            dma((NSLOT,)), dma((3,)), dma((8,)), dma((8,)),
            dma(()), dma((n_itm // WIDE,)), dma(()), dma((n_itm // WIDE,)),
            dma(()), dma(()), dma(()), dma(()), pltpu.SemaphoreType.REGULAR,
        ]
        hbm_spec = pl.BlockSpec(memory_space=pltpu.HBM)
        vmem_spec = pl.BlockSpec(memory_space=pltpu.VMEM)
        ou, oi, loss = pl.pallas_call(
            functools.partial(kernel, n_usr, n_itm, dim, n_trip),
            out_shape=(jax.ShapeDtypeStruct((dim, n_usr // 2), BF16),
                       jax.ShapeDtypeStruct((dim, half), BF16),
                       jax.ShapeDtypeStruct((n_trip // 128, 128), F32)),
            in_specs=[hbm_spec] * 4,
            out_specs=(vmem_spec,) * 3,
            scratch_shapes=scratch,
            compiler_params=pltpu.CompilerParams(collective_id=0, has_side_effects=True,
                                                 vmem_limit_bytes=50 * 1024 * 1024),
            name="gcn",
        )(mask_blk, *[pltpu.with_memory_space_constraint(v, pltpu.HBM) for v in (user_sh.T, item_sh.T, tri)])
        ou, oi, loss = pl.pallas_call(
            store_kernel,
            out_shape=tuple(jax.ShapeDtypeStruct(v.shape, v.dtype) for v in (ou, oi, loss)),
            in_specs=[vmem_spec] * 3,
            out_specs=(pl.BlockSpec(memory_space=pl.ANY),) * 3,
            scratch_shapes=[dma((3,))],
            compiler_params=pltpu.CompilerParams(vmem_limit_bytes=4 * 1024 * 1024),
            name="store",
        )(ou, oi, loss)
        return ou.T, oi.T, loss.reshape(n_trip)

    return jax.shard_map(
        local_fn, mesh=mesh,
        in_specs=(P("row", "col"), P(("row", "col"), "emb"), P(("col", "row"), "emb"), P()),
        out_specs=(P(("row", "col"), "emb"), P(("col", "row"), "emb"), P()),
        check_vma=False)
```

```python
import functools

import jax
import jax.numpy as jnp
from jax import lax
from jax.experimental import pallas as pl
from jax.experimental.pallas import tpu as pltpu
from jax.sharding import PartitionSpec as P

NUM_LAYERS = 3
CH = 2048
MC = 512
NSLOT = 6
FIN = 4096
WIDE = 8192
NARROW = 4096
MESH = pl.DeviceIdType.MESH
F32 = jnp.float32
BF16 = jnp.bfloat16


def remote(src, dst, ssem, rsem, dev):
    return pltpu.make_async_remote_copy(src_ref=src, dst_ref=dst, send_sem=ssem, recv_sem=rsem,
                                        device_id=dev, device_id_type=MESH)


def kernel(n_usr, n_itm, dim, n_trip,
           mask_ref, eu_ref, ei_ref, tri_ref, ou_ref, oi_ref, loss_ref,
           stage, adj, rowacc, degi, degi_r, degu, degu_r, invu, invi,
           it0, it1, it2, ut0, i1p, i1r, i2p, i2r,
           up, up_r, u3p, u3_r, uall, sel, table,
           tri_v, idx_v, idx_t, idx_s, dbuf, dt, drecv, sbuf, srecv,
           msem, lsem, ssem, rsem, cs1, cr1, cs2, cr2, ds, dr, bs, br, free_sem):
    e = lax.axis_index("emb")
    c = lax.axis_index("col")
    r = lax.axis_index("row")
    sib = {"row": 1 - r}
    xpeer = {"col": 1 - c}
    nch = n_itm // CH
    half = n_itm // 2
    uh = n_usr // 2
    nhome = n_trip // 4
    hrow = nhome // 4

    def mask_copy(j):
        slot = lax.rem(j, NSLOT)
        return pltpu.make_async_copy(mask_ref.at[:, pl.ds(pl.multiple_of(j * MC, MC), MC)], stage.at[slot], msem.at[slot])

    for j in range(NSLOT):
        mask_copy(j).start()
    own_i = it0.at[:, pl.ds(pl.multiple_of(r * half, half), half)]
    own_u = ut0.at[:, pl.ds(pl.multiple_of(c * uh, uh), uh)]
    cp_i = pltpu.make_async_copy(ei_ref, own_i, lsem.at[0])
    cp_u = pltpu.make_async_copy(eu_ref, own_u, lsem.at[1])
    cp_t = pltpu.make_async_copy(tri_ref, tri_v, lsem.at[2])
    cp_i.start()
    cp_u.start()
    cp_t.start()

    barrier = pltpu.get_barrier_semaphore()
    for q in range(1, 8):
        dev = {"emb": lax.rem(e + q // 4, 2), "col": lax.rem(c + (q // 2) % 2, 2), "row": lax.rem(r + q % 2, 2)}
        pl.semaphore_signal(barrier, inc=1, device_id=dev, device_id_type=MESH)

    rowacc[...] = jnp.zeros_like(rowacc)

    def mask_step(j, _):
        slot = lax.rem(j, NSLOT)
        mask_copy(j).wait()
        cols = pl.ds(pl.multiple_of(j * MC, MC), MC)

        def rows_step(g, acc):
            rows = pl.ds(pl.multiple_of(g * 16, 16), 16)
            m = stage[slot, rows, :].astype(F32)
            adj[rows, cols] = m.astype(BF16)
            s = m[:, 0:128]
            for k in range(1, MC // 128):
                s = s + m[:, k * 128:(k + 1) * 128]
            rowacc[rows, :] += s
            return acc + (m[0:8] + m[8:16])

        acc = lax.fori_loop(0, n_usr // 16, rows_step, jnp.zeros((8, MC), F32), unroll=2)
        degi[pl.ds(j, 1), :] = jnp.sum(acc, axis=0, keepdims=True)

        @pl.when(j + NSLOT < n_itm // MC)
        def _():
            mask_copy(j + NSLOT).start()
        return 0

    with jax.named_scope("ph_mask0"):
        lax.fori_loop(0, 8, mask_step, 0)
    cp_i.wait()
    cp_u.wait()
    cp_t.wait()
    with jax.named_scope("ph_barrier"):
        pl.semaphore_wait(barrier, 7)
    rc_i = remote(own_i, own_i, ssem.at[0], rsem.at[0], sib)
    rc_u = remote(own_u, own_u, ssem.at[1], rsem.at[1], xpeer)
    rc_i.start()
    rc_u.start()
    with jax.named_scope("ph_mask1"):
        lax.fori_loop(8, n_itm // MC, mask_step, 0)

    degu[...] = jnp.sum(rowacc[...].T, axis=0, keepdims=True)
    rc_du = remote(degu, degu_r, ssem.at[2], rsem.at[2], xpeer)
    rc_di = remote(degi, degi_r, ssem.at[3], rsem.at[3], sib)
    rc_du.start()
    rc_di.start()

    def tri_row(k, row):
        return tri_v[pl.ds(k, 1), pl.ds(pl.multiple_of(row * 128, 128), 128)]

    def home_row(q):
        return (lax.rem(c + q, 2) * 2 + r) * (nhome // 128)

    nrow = nhome // 128
    ncol = 2 * nrow
    idx_v[...] = jnp.zeros_like(idx_v)
    for k in range(2):
        for q in range(2):
            for row in range(nrow):
                idx_v[pl.ds(k * ncol + q * nrow + row, 1), :] = tri_row(k + 1, home_row(q) + row)
    loc = idx_v[0:2 * ncol, :] - c * n_itm
    idx_v[0:2 * ncol, :] = jnp.where((loc >= 0) & (loc < n_itm), loc, n_itm)
    idx_t[...] = idx_v[...].T
    cp_x = pltpu.make_async_copy(idx_t, idx_s, lsem.at[0])
    cp_x.start()
    table[pl.ds(n_itm, 8), :] = jnp.zeros((8, dim), F32)

    with jax.named_scope("ph_di_wait"):
        rc_di.wait()
    invi[...] = lax.rsqrt(jnp.maximum(degi[...] + degi_r[...], 1.0))
    rc_i.wait()
    rc_u.wait()
    cp_x.wait()
    with jax.named_scope("ph_du_wait"):
        rc_du.wait()
    inv_row = lax.rsqrt(jnp.maximum(degu[...] + degu_r[...], 1.0))
    invu[...] = jnp.broadcast_to(inv_row, (128, n_usr)).T

    nst = n_itm // WIDE

    def chunk1(j):
        cols = pl.ds(pl.multiple_of(j * CH, CH), CH)
        return remote(i1p.at[:, cols], i1r.at[:, cols], cs1, cr1.at[j // (WIDE // CH)], sib)

    def step1(i):
        cols = pl.ds(pl.multiple_of(i * WIDE, WIDE), WIDE)
        return remote(i1p.at[:, cols], i1r.at[:, cols], cs1, cr1.at[i], sib)

    def build_step(j, _):
        for nt in range(CH // 256):
            cols = pl.ds(pl.multiple_of(j * CH + nt * 256, 256), 256)
            lane = nt * 256 % MC
            wi = jnp.broadcast_to(invi[pl.ds(j * (CH // MC) + nt * 256 // MC, 1), lane:lane + 256], (16, 256))
            part = None
            for kt in range(n_usr // 256):
                tiles = []
                for g in range(16):
                    rows = pl.ds(kt * 256 + g * 16, 16)
                    wu = jnp.concatenate([invu[rows, :]] * 2, axis=1)
                    a = (wu * wi).astype(BF16) * adj[rows, cols]
                    adj[rows, cols] = a
                    tiles.append(a)
                p = jnp.dot(ut0[:, kt * 256:(kt + 1) * 256], jnp.concatenate(tiles, axis=0),
                            preferred_element_type=F32)
                part = p if part is None else part + p
            i1p[:, cols] = part
        chunk1(j).start()
        return 0

    with jax.named_scope("ph_build"):
        lax.fori_loop(0, nch, build_step, 0)

    def dot_t(a, b):
        return lax.dot_general(a, b, (((1,), (1,)), ((), ())), preferred_element_type=F32)

    def mixed_t(vals, rows, i):
        acc1 = acc2 = None
        for lo in range(0, WIDE, 512):
            ca = pl.ds(pl.multiple_of(i * WIDE + lo, 256), 256)
            cb = pl.ds(pl.multiple_of(i * WIDE + lo + 256, 256), 256)
            p1 = dot_t(vals[:, lo:lo + 256], adj[rows, ca])
            p2 = dot_t(adj[rows, cb], vals[:, lo + 256:lo + 512])
            acc1 = p1 if acc1 is None else acc1 + p1
            acc2 = p2 if acc2 is None else acc2 + p2
        return acc1 + acc2.T

    up[...] = jnp.zeros_like(up)
    rc_up = []
    for h in range(1):
        rows = pl.ds(0, n_usr)

        def user_step(i, _, h=h, rows=rows):
            cols = pl.ds(pl.multiple_of(i * WIDE, WIDE), WIDE)
            if h == 0:
                step1(i).wait_recv()
                it1[:, cols] = (i1p[:, cols] + i1r[:, cols]).astype(BF16)
            lhs = jnp.concatenate([it0[:, cols], it1[:, cols]], axis=0)
            up[:, rows] += mixed_t(lhs, rows, i)
            return 0

        with jax.named_scope("ph_user"):
            lax.fori_loop(0, nst, user_step, 0)
        rc_up.append(remote(up.at[:, rows], up_r.at[:, rows], ssem.at[4 + h], rsem.at[4 + h], xpeer))
        rc_up[h].start()
    pl.semaphore_signal(free_sem, inc=1, device_id=sib, device_id_type=MESH)

    remote(i1p, i1r, cs1, cr1.at[0], sib).wait_send()

    def sel_step(g, _):
        users = lax.broadcasted_iota(jnp.int32, (16, 128), 0) + g * 16
        for t in range(nhome // 128):
            ids = tri_row(0, home_row(0) + t)
            hit = jnp.where(users == jnp.broadcast_to(ids, (16, 128)), 1.0, 0.0)
            sel[pl.ds(pl.multiple_of(g * 16, 16), 16), t * 128:(t + 1) * 128] = hit.astype(BF16)
        return 0

    with jax.named_scope("ph_sel"):
        lax.fori_loop(0, 2 * n_usr // 16, sel_step, 0, unroll=2)
    with jax.named_scope("ph_up_wait"):
        rc_up[0].wait()
    u12 = (up[...] + up_r[...]).astype(BF16)

    def part2(i, size, step):
        cols = pl.ds(pl.multiple_of(i * size, size), size)
        return remote(i2p.at[:, cols], i2r.at[:, cols], cs2, cr2.at[step], sib)

    def item_step(i, _):
        cols = pl.ds(pl.multiple_of(i * NARROW, NARROW), NARROW)
        part = jnp.dot(u12, adj[:, cols], preferred_element_type=F32)
        i2p[:, cols] = part[0:dim]
        i1p[:, cols] = part[dim:2 * dim]
        part2(i, NARROW, i // (WIDE // NARROW)).start()
        return 0

    with jax.named_scope("ph_item"):
        lax.fori_loop(0, n_itm // NARROW, item_step, 0)
        pl.semaphore_wait(free_sem, 1)
        for i in range(nst):
            step1(i).start()

    u3p[...] = jnp.zeros_like(u3p)

    def user3_step(i, _):
        cols = pl.ds(pl.multiple_of(i * WIDE, WIDE), WIDE)
        part2(i, WIDE, i).wait_recv()
        v2 = (i2p[:, cols] + i2r[:, cols]).astype(BF16)
        it2[:, cols] = v2
        u3p[...] += mixed_t(v2, slice(None), i)
        return 0

    with jax.named_scope("ph_user3"):
        lax.fori_loop(0, nst, user3_step, 0)
    rc_u3 = remote(u3p, u3_r, ssem.at[6], rsem.at[6], xpeer)
    rc_u3.start()

    def final_step(k, _):
        cols = pl.ds(pl.multiple_of(k * FIN, FIN), FIN)
        v3 = (i1p[:, cols] + i1r[:, cols]).astype(BF16)
        acc = it0[:, cols].astype(F32) + it1[:, cols].astype(F32)
        acc = (acc + it2[:, cols].astype(F32)) + v3.astype(F32)
        fin = (acc * (1.0 / (NUM_LAYERS + 1))).astype(BF16)
        it1[:, cols] = fin
        fin = fin.astype(F32)
        for b in range(FIN // 128):
            table[pl.ds(pl.multiple_of(k * FIN + b * 128, 128), 128), :] = fin[:, b * 128:(b + 1) * 128].T
        return 0

    with jax.named_scope("ph_final"):
        for i in range(nst):
            step1(i).wait_recv()
        lax.fori_loop(0, n_itm // FIN, final_step, 0)
    oi_ref[...] = it1[:, pl.ds(pl.multiple_of(r * half, half), half)]

    def diff_rows(q, row0):
        def body(al, _):
            for row in (row0, row0 + 1):
                p = idx_s[al, q * nrow + row]
                n = idx_s[al, ncol + q * nrow + row]
                dbuf[pl.ds(row * 128 + al, 1), :] = table[pl.ds(p, 1), :] - table[pl.ds(n, 1), :]
            return 0

        lax.fori_loop(0, 128, body, 0, unroll=16)
        for row in (row0, row0 + 1):
            dt[q, :, row * 128:(row + 1) * 128] = dbuf[row * 128:(row + 1) * 128, :].T

    with jax.named_scope("ph_diff"):
        for row0 in range(0, nrow, 2):
            diff_rows(1, row0)
            cols = pl.ds(row0 * 128, 256)
            remote(dt.at[1, :, cols], drecv.at[:, cols], ds, dr, xpeer).start()

    with jax.named_scope("ph_u3_wait"):
        rc_u3.wait()
    u3 = (u3p[...] + u3_r[...]).astype(BF16).astype(F32)
    uacc = ut0[...].astype(F32) + u12[0:dim].astype(F32)
    uacc = (uacc + u12[dim:2 * dim].astype(F32)) + u3
    fin_u = (uacc * (1.0 / (NUM_LAYERS + 1))).astype(BF16)
    own_cols = pl.ds(pl.multiple_of(r * n_usr, n_usr), n_usr)
    uall[:, own_cols] = fin_u
    rc_uf = remote(uall.at[:, own_cols], uall.at[:, own_cols], ssem.at[7], rsem.at[7], sib)
    rc_uf.start()
    ou_ref[...] = uall[:, pl.ds(pl.multiple_of(r * n_usr + c * uh, uh), uh)]
    with jax.named_scope("ph_diff"):
        for row0 in range(0, nrow, 2):
            diff_rows(0, row0)
    with jax.named_scope("ph_uf_wait"):
        rc_uf.wait()
    urow = jnp.dot(uall[...], sel[...], preferred_element_type=F32)

    with jax.named_scope("ph_d_wait"):
        remote(dt.at[1], drecv, ds, dr, xpeer).wait()
    score = jnp.sum((dt[0] + drecv[...]) * urow, axis=0, keepdims=True)
    for row in range(nrow):
        sbuf[pl.ds(row, 1), :] = score[:, row * 128:(row + 1) * 128]

    def s_send(q):
        dev = {"emb": lax.rem(e + q // 4, 2), "col": lax.rem(c + (q // 2) % 2, 2), "row": lax.rem(r + q % 2, 2)}
        return remote(sbuf, srecv.at[q - 1], bs, br, dev)

    for q in range(7, 0, -1):
        s_send(q).start()
    with jax.named_scope("ph_s_wait"):
        remote(srecv, srecv, bs, br, sib).wait()
    for q in range(4):
        own = sbuf[...] if q == 0 else srecv[q - 1]
        x = own + srecv[q + 3]
        hq = lax.rem(c + q // 2, 2) * 2 + lax.rem(r + q % 2, 2)
        ls = jnp.maximum(-x, 0.0) + jnp.log1p(jnp.exp(-jnp.abs(x)))
        loss_ref[pl.ds(pl.multiple_of(hq * (nhome // 128), 8), nhome // 128), :] = ls

    with jax.named_scope("ph_drain"):
        remote(i2p, i2r, cs2, cr2.at[0], sib).wait_send()
        remote(i1p, i1r, cs1, cr1.at[0], sib).wait_send()


def store_kernel(*refs):
    srcs, dsts, sem = refs[0:3], refs[3:6], refs[6]
    copies = [pltpu.make_async_copy(a, b, sem.at[k]) for k, (a, b) in enumerate(zip(srcs, dsts))]
    for copy in copies:
        copy.start()
    for copy in copies:
        copy.wait()


def solution(mesh):
    def local_fn(mask_blk, user_sh, item_sh, triples):
        n_usr, n_itm = mask_blk.shape
        dim = user_sh.shape[1]
        n_trip = triples.shape[0]
        nch = n_itm // CH
        half = n_itm // 2
        tri = triples.T
        vm = pltpu.VMEM
        dma = pltpu.SemaphoreType.DMA
        nhome = n_trip // 4
        hrow = nhome // 4
        scratch = [
            vm((NSLOT, n_usr, MC), jnp.int32), vm((n_usr, n_itm + 256), BF16), vm((n_usr, 128), F32),
            vm((n_itm // MC, MC), F32), vm((n_itm // MC, MC), F32), vm((1, n_usr), F32), vm((1, n_usr), F32),
            vm((n_usr, 128), F32), vm((n_itm // MC, MC), F32),
            vm((dim, n_itm), BF16), vm((dim, n_itm), BF16), vm((dim, n_itm), BF16), vm((dim, n_usr), BF16),
            vm((dim, n_itm), F32), vm((dim, n_itm), F32), vm((dim, n_itm), F32), vm((dim, n_itm), F32),
            vm((2 * dim, n_usr), F32), vm((2 * dim, n_usr), F32), vm((dim, n_usr), F32), vm((dim, n_usr), F32),
            vm((dim, 2 * n_usr), BF16), vm((2 * n_usr, nhome), BF16),
            vm((n_itm + 8, dim), F32),
            vm((3, n_trip), jnp.int32), vm((128, 128), jnp.int32), vm((128, 128), jnp.int32),
            pltpu.SMEM((128, 128), jnp.int32),
            vm((nhome, dim), F32), vm((2, dim, nhome), F32), vm((dim, nhome), F32),
            vm((nhome // 128, 128), F32), vm((7, nhome // 128, 128), F32),
            dma((NSLOT,)), dma((3,)), dma((8,)), dma((8,)),
            dma(()), dma((n_itm // WIDE,)), dma(()), dma((n_itm // WIDE,)),
            dma(()), dma(()), dma(()), dma(()), pltpu.SemaphoreType.REGULAR,
        ]
        hbm_spec = pl.BlockSpec(memory_space=pltpu.HBM)
        vmem_spec = pl.BlockSpec(memory_space=pltpu.VMEM)
        ou, oi, loss = pl.pallas_call(
            functools.partial(kernel, n_usr, n_itm, dim, n_trip),
            out_shape=(jax.ShapeDtypeStruct((dim, n_usr // 2), BF16),
                       jax.ShapeDtypeStruct((dim, half), BF16),
                       jax.ShapeDtypeStruct((n_trip // 128, 128), F32)),
            in_specs=[hbm_spec] * 4,
            out_specs=(vmem_spec,) * 3,
            scratch_shapes=scratch,
            compiler_params=pltpu.CompilerParams(collective_id=0, has_side_effects=True,
                                                 vmem_limit_bytes=50 * 1024 * 1024),
            name="gcn",
        )(mask_blk, *[pltpu.with_memory_space_constraint(v, pltpu.HBM) for v in (user_sh.T, item_sh.T, tri)])
        ou, oi, loss = pl.pallas_call(
            store_kernel,
            out_shape=tuple(jax.ShapeDtypeStruct(v.shape, v.dtype) for v in (ou, oi, loss)),
            in_specs=[vmem_spec] * 3,
            out_specs=(pl.BlockSpec(memory_space=pl.ANY),) * 3,
            scratch_shapes=[dma((3,))],
            compiler_params=pltpu.CompilerParams(vmem_limit_bytes=4 * 1024 * 1024),
            name="store",
        )(ou, oi, loss)
        return ou.T, oi.T, loss.reshape(n_trip)

    return jax.shard_map(
        local_fn, mesh=mesh,
        in_specs=(P("row", "col"), P(("row", "col"), "emb"), P(("col", "row"), "emb"), P()),
        out_specs=(P(("row", "col"), "emb"), P(("col", "row"), "emb"), P()),
        check_vma=False)
```

```python
import functools

import jax
import jax.numpy as jnp
from jax import lax
from jax.experimental import pallas as pl
from jax.experimental.pallas import tpu as pltpu
from jax.sharding import PartitionSpec as P

NUM_LAYERS = 3
BIG = 4096
CH = 2048
MC = 512
NSLOT = 8
FIN = 4096
WIDE = 8192
FIRST = 2048
NARROW = 4096
MESH = pl.DeviceIdType.MESH
F32 = jnp.float32
BF16 = jnp.bfloat16


def remote(src, dst, ssem, rsem, dev):
    return pltpu.make_async_remote_copy(src_ref=src, dst_ref=dst, send_sem=ssem, recv_sem=rsem,
                                        device_id=dev, device_id_type=MESH)


def kernel(n_usr, n_itm, dim, n_trip,
           mask_ref, eu_ref, ei_ref, tri_ref, ou_ref, oi_ref, loss_ref,
           stage, adj, rowacc, degi, degi_r, degu, degu_r, invu, invi,
           it0, it1, it2, ut0, i1p, i1r, i2p, i2r,
           up, up_r, u3p, u3_r, uall, sel, table,
           tri_v, idx_v, idx_t, idx_s, dbuf, dt, drecv, sbuf, srecv,
           msem, lsem, ssem, rsem, cs1, cr1, cs2, cr2, ds, dr, bs, br, free_sem):
    e = lax.axis_index("emb")
    c = lax.axis_index("col")
    r = lax.axis_index("row")
    sib = {"row": 1 - r}
    xpeer = {"col": 1 - c}
    nch = n_itm // CH
    half = n_itm // 2
    uh = n_usr // 2
    nhome = n_trip // 4
    hrow = nhome // 4

    def mask_copy(j):
        slot = lax.rem(j, NSLOT)
        return pltpu.make_async_copy(mask_ref.at[:, pl.ds(pl.multiple_of(j * MC, MC), MC)], stage.at[slot], msem.at[slot])

    for j in range(NSLOT):
        mask_copy(j).start()
    own_i = it0.at[:, pl.ds(pl.multiple_of(r * half, half), half)]
    own_u = ut0.at[:, pl.ds(pl.multiple_of(c * uh, uh), uh)]
    cp_i = pltpu.make_async_copy(ei_ref, own_i, lsem.at[0])
    cp_u = pltpu.make_async_copy(eu_ref, own_u, lsem.at[1])
    cp_t = pltpu.make_async_copy(tri_ref, tri_v, lsem.at[2])
    cp_i.start()
    cp_u.start()
    cp_t.start()

    barrier = pltpu.get_barrier_semaphore()
    for q in range(1, 8):
        dev = {"emb": lax.rem(e + q // 4, 2), "col": lax.rem(c + (q // 2) % 2, 2), "row": lax.rem(r + q % 2, 2)}
        pl.semaphore_signal(barrier, inc=1, device_id=dev, device_id_type=MESH)

    rowacc[...] = jnp.zeros_like(rowacc)

    def mask_step(j, _):
        slot = lax.rem(j, NSLOT)
        mask_copy(j).wait()
        cols = pl.ds(pl.multiple_of(j * MC, MC), MC)

        def rows_step(g, acc):
            rows = pl.ds(pl.multiple_of(g * 16, 16), 16)
            m = stage[slot, rows, :].astype(F32)
            adj[rows, cols] = m.astype(BF16)
            s = m[:, 0:128]
            for k in range(1, MC // 128):
                s = s + m[:, k * 128:(k + 1) * 128]
            rowacc[rows, :] += s
            return acc + (m[0:8] + m[8:16])

        acc = lax.fori_loop(0, n_usr // 16, rows_step, jnp.zeros((8, MC), F32), unroll=2)
        degi[pl.ds(j, 1), :] = jnp.sum(acc, axis=0, keepdims=True)

        @pl.when(j + NSLOT < n_itm // MC)
        def _():
            mask_copy(j + NSLOT).start()
        return 0

    with jax.named_scope("ph_mask0"):
        lax.fori_loop(0, 8, mask_step, 0)
    cp_i.wait()
    cp_u.wait()
    cp_t.wait()
    with jax.named_scope("ph_barrier"):
        pl.semaphore_wait(barrier, 7)
    rc_i = remote(own_i, own_i, ssem.at[0], rsem.at[0], sib)
    rc_u = remote(own_u, own_u, ssem.at[1], rsem.at[1], xpeer)
    rc_i.start()
    rc_u.start()
    with jax.named_scope("ph_mask1"):
        lax.fori_loop(8, n_itm // MC, mask_step, 0)

    degu[...] = jnp.sum(rowacc[...].T, axis=0, keepdims=True)
    rc_du = remote(degu, degu_r, ssem.at[2], rsem.at[2], xpeer)
    rc_di = remote(degi, degi_r, ssem.at[3], rsem.at[3], sib)
    rc_du.start()
    rc_di.start()

    def tri_row(k, row):
        return tri_v[pl.ds(k, 1), pl.ds(pl.multiple_of(row * 128, 128), 128)]

    def home_row(q):
        return (lax.rem(c + q, 2) * 2 + r) * (nhome // 128)

    nrow = nhome // 128
    ncol = 2 * nrow
    idx_v[...] = jnp.zeros_like(idx_v)
    for k in range(2):
        for q in range(2):
            for row in range(nrow):
                idx_v[pl.ds(k * ncol + q * nrow + row, 1), :] = tri_row(k + 1, home_row(q) + row)
    loc = idx_v[0:2 * ncol, :] - c * n_itm
    idx_v[0:2 * ncol, :] = jnp.where((loc >= 0) & (loc < n_itm), loc, n_itm)
    idx_t[...] = idx_v[...].T
    cp_x = pltpu.make_async_copy(idx_t, idx_s, lsem.at[0])
    cp_x.start()
    table[pl.ds(n_itm, 8), :] = jnp.zeros((8, dim), F32)

    with jax.named_scope("ph_di_wait"):
        rc_di.wait_recv()
    invi[...] = lax.rsqrt(jnp.maximum(degi[...] + degi_r[...], 1.0))
    rc_i.wait_recv()
    rc_u.wait_recv()
    cp_x.wait()
    with jax.named_scope("ph_du_wait"):
        rc_du.wait_recv()
    inv_row = lax.rsqrt(jnp.maximum(degu[...] + degu_r[...], 1.0))
    invu[...] = jnp.broadcast_to(inv_row, (128, n_usr)).T

    nst = n_itm // WIDE

    def chunk1(base, size):
        cols = pl.ds(pl.multiple_of(base, size), size)
        return remote(i1p.at[:, cols], i1r.at[:, cols], cs1, cr1.at[base // WIDE], sib)

    def step1(i):
        cols = pl.ds(pl.multiple_of(i * WIDE, WIDE), WIDE)
        return remote(i1p.at[:, cols], i1r.at[:, cols], cs1, cr1.at[i], sib)

    def build_step(base, size):
        for nt in range(size // 256):
            cols = pl.ds(pl.multiple_of(base + nt * 256, 256), 256)
            lane = nt * 256 % MC
            wi = jnp.broadcast_to(invi[pl.ds(base // MC + nt * 256 // MC, 1), lane:lane + 256], (16, 256))
            tiles = []
            for g in range(n_usr // 16):
                rows = pl.ds(g * 16, 16)
                wu = jnp.concatenate([invu[rows, :]] * 2, axis=1)
                a = (wu * wi).astype(BF16) * adj[rows, cols]
                adj[rows, cols] = a
                tiles.append(a)
            part = jnp.dot(ut0[...], jnp.concatenate(tiles, axis=0), preferred_element_type=F32)
            i1p[:, cols] = part
        chunk1(base, size).start()
        return 0

    with jax.named_scope("ph_build"):
        nbig = n_itm // BIG - 1
        lax.fori_loop(0, nbig, lambda i, _: build_step(i * BIG, BIG), 0)
        lax.fori_loop(0, BIG // CH, lambda i, _: build_step(nbig * BIG + i * CH, CH), 0)

    def dot_t(a, b):
        return lax.dot_general(a, b, (((1,), (1,)), ((), ())), preferred_element_type=F32)

    def mixed_t(vals, base):
        acc1 = acc2 = None
        for lo in range(0, WIDE, 512):
            ca = pl.ds(pl.multiple_of(base + lo, 256), 256)
            cb = pl.ds(pl.multiple_of(base + lo + 256, 256), 256)
            p1 = dot_t(vals[:, lo:lo + 256], adj[:, ca])
            p2 = dot_t(adj[:, cb], vals[:, lo + 256:lo + 512])
            acc1 = p1 if acc1 is None else acc1 + p1
            acc2 = p2 if acc2 is None else acc2 + p2
        return acc1 + acc2.T

    up[...] = jnp.zeros_like(up)

    def user_step(i, _):
        cols = pl.ds(pl.multiple_of(i * WIDE, WIDE), WIDE)
        step1(i).wait_recv()
        v1 = (i1p[:, cols] + i1r[:, cols]).astype(BF16)
        it1[:, cols] = v1
        up[...] += mixed_t(jnp.concatenate([it0[:, cols], v1], axis=0), i * WIDE)
        return 0

    with jax.named_scope("ph_user"):
        lax.fori_loop(0, nst, user_step, 0)
    rc_up = remote(up, up_r, ssem.at[4], rsem.at[4], xpeer)
    rc_up.start()
    pl.semaphore_signal(free_sem, inc=1, device_id=sib, device_id_type=MESH)

    remote(i1p, i1r, cs1, cr1.at[0], sib).wait_send()

    def sel_step(g, _):
        users = lax.broadcasted_iota(jnp.int32, (16, 128), 0) + g * 16
        for t in range(nhome // 128):
            ids = tri_row(0, home_row(0) + t)
            hit = jnp.where(users == jnp.broadcast_to(ids, (16, 128)), 1.0, 0.0)
            sel[pl.ds(pl.multiple_of(g * 16, 16), 16), t * 128:(t + 1) * 128] = hit.astype(BF16)
        return 0

    with jax.named_scope("ph_sel"):
        lax.fori_loop(0, 2 * n_usr // 16, sel_step, 0, unroll=2)
    with jax.named_scope("ph_up_wait"):
        rc_up.wait_recv()
    u12 = (up[...] + up_r[...]).astype(BF16)

    oo = r * half
    so = (1 - r) * half
    own = pl.ds(pl.multiple_of(oo, half), half)
    other = pl.ds(pl.multiple_of(so, half), half)

    def half2(k, size):
        src = pl.ds(pl.multiple_of(so + k * size, size), size)
        dst = pl.ds(pl.multiple_of(k * size, size), size)
        return remote(i2p.at[:, src], i2r.at[:, dst], cs2, cr2, sib)

    def half3(cols):
        return remote(i1p.at[:, cols], i1r.at[:, cols], cs1, cr1.at[0], sib)

    def rounded(ref, cols, k):
        return remote(ref.at[:, cols], ref.at[:, cols], ssem.at[k], rsem.at[k], sib)

    def item_step(k, base, size, send):
        cols = pl.ds(pl.multiple_of(base + k * size, size), size)
        part = jnp.dot(u12, adj[:, cols], preferred_element_type=F32)
        i2p[:, cols] = part[0:dim]
        i1p[:, cols] = part[dim:2 * dim]
        if send:
            half2(k, size).start()

    with jax.named_scope("ph_item"):
        for k in range(half // FIRST):
            item_step(k, so, FIRST, True)
        pl.semaphore_wait(free_sem, 1)
        half3(other).start()
        for k in range(half // NARROW):
            item_step(k, oo, NARROW, False)
    with jax.named_scope("ph_i2_wait"):
        half2(0, half).wait_recv()
    it2[:, own] = (i2p[:, own] + i2r[...]).astype(BF16)
    rounded(it2, own, 5).start()
    with jax.named_scope("ph_user3"):
        u3p[...] = mixed_t(it2[:, own], oo)

    def table_step(fin, base):
        fin = fin.astype(F32)
        for b in range(FIN // 128):
            table[pl.ds(pl.multiple_of(base + b * 128, 128), 128), :] = fin[:, b * 128:(b + 1) * 128].T

    def final_step(k, _):
        base = oo + k * FIN
        cols = pl.ds(pl.multiple_of(base, FIN), FIN)
        v3 = (i1p[:, cols] + i1r[:, cols]).astype(BF16)
        acc = it0[:, cols].astype(F32) + it1[:, cols].astype(F32)
        acc = (acc + it2[:, cols].astype(F32)) + v3.astype(F32)
        fin = (acc * (1.0 / (NUM_LAYERS + 1))).astype(BF16)
        it1[:, cols] = fin
        rounded(it1, cols, 8).start()
        table_step(fin, base)
        return 0

    with jax.named_scope("ph_i3_wait"):
        half3(own).wait_recv()
    with jax.named_scope("ph_final"):
        lax.fori_loop(0, half // FIN, final_step, 0)
    oi_ref[...] = it1[:, own]
    with jax.named_scope("ph_i2b_wait"):
        rounded(it2, other, 5).wait_recv()
    with jax.named_scope("ph_user3"):
        u3p[...] += mixed_t(it2[:, other], so)
    rc_u3 = remote(u3p, u3_r, ssem.at[6], rsem.at[6], xpeer)
    rc_u3.start()

    def other_step(k, _):
        base = so + k * FIN
        table_step(it1[:, pl.ds(pl.multiple_of(base, FIN), FIN)], base)
        return 0

    with jax.named_scope("ph_i3b_wait"):
        rounded(it1, other, 8).wait_recv()
    with jax.named_scope("ph_final"):
        lax.fori_loop(0, half // FIN, other_step, 0)

    def diff_rows(q, row0):
        def body(al, _):
            for row in (row0, row0 + 1):
                p = idx_s[al, q * nrow + row]
                n = idx_s[al, ncol + q * nrow + row]
                dbuf[pl.ds(row * 128 + al, 1), :] = table[pl.ds(p, 1), :] - table[pl.ds(n, 1), :]
            return 0

        lax.fori_loop(0, 128, body, 0, unroll=16)
        for row in (row0, row0 + 1):
            dt[q, :, row * 128:(row + 1) * 128] = dbuf[row * 128:(row + 1) * 128, :].T

    with jax.named_scope("ph_diff"):
        for row0 in range(0, nrow, 2):
            diff_rows(1, row0)
            cols = pl.ds(row0 * 128, 256)
            remote(dt.at[1, :, cols], drecv.at[:, cols], ds, dr, xpeer).start()

    with jax.named_scope("ph_diff"):
        for row0 in range(0, nrow // 2, 2):
            diff_rows(0, row0)

    with jax.named_scope("ph_u3_wait"):
        rc_u3.wait_recv()
    u3 = (u3p[...] + u3_r[...]).astype(BF16).astype(F32)
    uacc = ut0[...].astype(F32) + u12[0:dim].astype(F32)
    uacc = (uacc + u12[dim:2 * dim].astype(F32)) + u3
    fin_u = (uacc * (1.0 / (NUM_LAYERS + 1))).astype(BF16)
    own_cols = pl.ds(pl.multiple_of(r * n_usr, n_usr), n_usr)
    uall[:, own_cols] = fin_u
    rc_uf = remote(uall.at[:, own_cols], uall.at[:, own_cols], ssem.at[7], rsem.at[7], sib)
    rc_uf.start()
    ou_ref[...] = uall[:, pl.ds(pl.multiple_of(r * n_usr + c * uh, uh), uh)]
    with jax.named_scope("ph_diff"):
        for row0 in range(nrow // 2, nrow, 2):
            diff_rows(0, row0)
    with jax.named_scope("ph_uf_wait"):
        rc_uf.wait_recv()
    urow = jnp.dot(uall[...], sel[...], preferred_element_type=F32)

    with jax.named_scope("ph_d_wait"):
        remote(dt.at[1], drecv, ds, dr, xpeer).wait_recv()
    score = jnp.sum((dt[0] + drecv[...]) * urow, axis=0, keepdims=True)
    for row in range(nrow):
        sbuf[pl.ds(row, 1), :] = score[:, row * 128:(row + 1) * 128]

    def s_send(q):
        dev = {"emb": lax.rem(e + q // 4, 2), "col": lax.rem(c + (q // 2) % 2, 2), "row": lax.rem(r + q % 2, 2)}
        return remote(sbuf, srecv.at[q - 1], bs, br, dev)

    for q in range(7, 0, -1):
        s_send(q).start()
    with jax.named_scope("ph_s_wait"):
        remote(srecv, srecv, bs, br, sib).wait_recv()
    for q in range(4):
        mine = sbuf[...] if q == 0 else srecv[q - 1]
        x = mine + srecv[q + 3]
        hq = lax.rem(c + q // 2, 2) * 2 + lax.rem(r + q % 2, 2)
        ls = jnp.maximum(-x, 0.0) + jnp.log1p(jnp.exp(-jnp.abs(x)))
        loss_ref[pl.ds(pl.multiple_of(hq * (nhome // 128), 8), nhome // 128), :] = ls

    with jax.named_scope("ph_drain"):
        half2(0, half).wait_send()
        half3(other).wait_send()
        rounded(it2, own, 5).wait_send()
        rounded(it1, own, 8).wait_send()
        for copy in (rc_i, rc_u, rc_du, rc_di, rc_up, rc_u3, rc_uf, remote(dt.at[1], drecv, ds, dr, xpeer),
                     remote(srecv, srecv, bs, br, sib)):
            copy.wait_send()


def store_kernel(*refs):
    srcs, dsts, sem = refs[0:3], refs[3:6], refs[6]
    copies = [pltpu.make_async_copy(a, b, sem.at[k]) for k, (a, b) in enumerate(zip(srcs, dsts))]
    for copy in copies:
        copy.start()
    for copy in copies:
        copy.wait()


def solution(mesh):
    def local_fn(mask_blk, user_sh, item_sh, triples):
        n_usr, n_itm = mask_blk.shape
        dim = user_sh.shape[1]
        n_trip = triples.shape[0]
        nch = n_itm // CH
        half = n_itm // 2
        tri = triples.T
        vm = pltpu.VMEM
        dma = pltpu.SemaphoreType.DMA
        nhome = n_trip // 4
        hrow = nhome // 4
        scratch = [
            vm((NSLOT, n_usr, MC), jnp.int32), vm((n_usr, n_itm + 256), BF16), vm((n_usr, 128), F32),
            vm((n_itm // MC, MC), F32), vm((n_itm // MC, MC), F32), vm((1, n_usr), F32), vm((1, n_usr), F32),
            vm((n_usr, 128), F32), vm((n_itm // MC, MC), F32),
            vm((dim, n_itm), BF16), vm((dim, n_itm), BF16), vm((dim, n_itm), BF16), vm((dim, n_usr), BF16),
            vm((dim, n_itm), F32), vm((dim, n_itm), F32), vm((dim, n_itm), F32), vm((dim, half), F32),
            vm((2 * dim, n_usr), F32), vm((2 * dim, n_usr), F32), vm((dim, n_usr), F32), vm((dim, n_usr), F32),
            vm((dim, 2 * n_usr), BF16), vm((2 * n_usr, nhome), BF16),
            vm((n_itm + 8, dim), F32),
            vm((3, n_trip), jnp.int32), vm((128, 128), jnp.int32), vm((128, 128), jnp.int32),
            pltpu.SMEM((128, 128), jnp.int32),
            vm((nhome, dim), F32), vm((2, dim, nhome), F32), vm((dim, nhome), F32),
            vm((nhome // 128, 128), F32), vm((7, nhome // 128, 128), F32),
            dma((NSLOT,)), dma((3,)), dma((9,)), dma((9,)),
            dma(()), dma((n_itm // WIDE,)), dma(()), dma(()),
            dma(()), dma(()), dma(()), dma(()), pltpu.SemaphoreType.REGULAR,
        ]
        hbm_spec = pl.BlockSpec(memory_space=pltpu.HBM)
        vmem_spec = pl.BlockSpec(memory_space=pltpu.VMEM)
        ou, oi, loss = pl.pallas_call(
            functools.partial(kernel, n_usr, n_itm, dim, n_trip),
            out_shape=(jax.ShapeDtypeStruct((dim, n_usr // 2), BF16),
                       jax.ShapeDtypeStruct((dim, half), BF16),
                       jax.ShapeDtypeStruct((n_trip // 128, 128), F32)),
            in_specs=[hbm_spec] * 4,
            out_specs=(vmem_spec,) * 3,
            scratch_shapes=scratch,
            compiler_params=pltpu.CompilerParams(collective_id=0, has_side_effects=True,
                                                 vmem_limit_bytes=50 * 1024 * 1024),
            name="gcn",
        )(mask_blk, *[pltpu.with_memory_space_constraint(v, pltpu.HBM) for v in (user_sh.T, item_sh.T, tri)])
        ou, oi, loss = pl.pallas_call(
            store_kernel,
            out_shape=tuple(jax.ShapeDtypeStruct(v.shape, v.dtype) for v in (ou, oi, loss)),
            in_specs=[vmem_spec] * 3,
            out_specs=(pl.BlockSpec(memory_space=pl.ANY),) * 3,
            scratch_shapes=[dma((3,))],
            compiler_params=pltpu.CompilerParams(vmem_limit_bytes=4 * 1024 * 1024),
            name="store",
        )(ou, oi, loss)
        return ou.T, oi.T, loss.reshape(n_trip)

    return jax.shard_map(
        local_fn, mesh=mesh,
        in_specs=(P("row", "col"), P(("row", "col"), "emb"), P(("col", "row"), "emb"), P()),
        out_specs=(P(("row", "col"), "emb"), P(("col", "row"), "emb"), P()),
        check_vma=False)
```

```python
import functools

import jax
import jax.numpy as jnp
from jax import lax
from jax.experimental import pallas as pl
from jax.experimental.pallas import tpu as pltpu
from jax.sharding import PartitionSpec as P

NUM_LAYERS = 3
BIG = 4096
CH = 2048
MC = 512
NSLOT = 8
FIN = 4096
WIDE = 8192
FIRST = 2048
NARROW = 4096
MESH = pl.DeviceIdType.MESH
F32 = jnp.float32
BF16 = jnp.bfloat16


def remote(src, dst, ssem, rsem, dev):
    return pltpu.make_async_remote_copy(src_ref=src, dst_ref=dst, send_sem=ssem, recv_sem=rsem,
                                        device_id=dev, device_id_type=MESH)


def kernel(n_usr, n_itm, dim, n_trip,
           mask_ref, eu_ref, ei_ref, tri_ref, ou_ref, oi_ref, loss_ref,
           stage, adj, rowacc, degi, degi_r, degu, degu_r, invu, invi,
           it0, it1, it2, ut0, i1p, i1r, i2p, i2r,
           up, up_r, u3p, u3_r, uall, sel, table,
           tri_v, idx_v, s0, s1, s2, s3, s4, s5, s6, s7, dbuf, dt, drecv, sbuf, srecv,
           msem, lsem, ssem, rsem, cs1, cr1, cs2, cr2, ds, dr, bs, br, xsem, free_sem):
    idx_s = (s0, s1, s2, s3, s4, s5, s6, s7)
    e = lax.axis_index("emb")
    c = lax.axis_index("col")
    r = lax.axis_index("row")
    sib = {"row": 1 - r}
    xpeer = {"col": 1 - c}
    nch = n_itm // CH
    half = n_itm // 2
    uh = n_usr // 2
    nhome = n_trip // 4
    hrow = nhome // 4

    def mask_copy(j):
        slot = lax.rem(j, NSLOT)
        return pltpu.make_async_copy(mask_ref.at[:, pl.ds(pl.multiple_of(j * MC, MC), MC)], stage.at[slot], msem.at[slot])

    for j in range(NSLOT):
        mask_copy(j).start()
    own_i = it0.at[:, pl.ds(pl.multiple_of(r * half, half), half)]
    own_u = ut0.at[:, pl.ds(pl.multiple_of(c * uh, uh), uh)]
    cp_i = pltpu.make_async_copy(ei_ref, own_i, lsem.at[0])
    cp_u = pltpu.make_async_copy(eu_ref, own_u, lsem.at[1])
    cp_t = pltpu.make_async_copy(tri_ref, tri_v, lsem.at[2])
    cp_i.start()
    cp_u.start()
    cp_t.start()

    barrier = pltpu.get_barrier_semaphore()
    for q in range(1, 8):
        dev = {"emb": lax.rem(e + q // 4, 2), "col": lax.rem(c + (q // 2) % 2, 2), "row": lax.rem(r + q % 2, 2)}
        pl.semaphore_signal(barrier, inc=1, device_id=dev, device_id_type=MESH)

    rowacc[...] = jnp.zeros_like(rowacc)

    def mask_step(j, _):
        slot = lax.rem(j, NSLOT)
        mask_copy(j).wait()
        cols = pl.ds(pl.multiple_of(j * MC, MC), MC)

        def rows_step(g, acc):
            rows = pl.ds(pl.multiple_of(g * 16, 16), 16)
            m = stage[slot, rows, :].astype(F32)
            adj[rows, cols] = m.astype(BF16)
            s = m[:, 0:128]
            for k in range(1, MC // 128):
                s = s + m[:, k * 128:(k + 1) * 128]
            rowacc[rows, :] += s
            return acc + (m[0:8] + m[8:16])

        acc = lax.fori_loop(0, n_usr // 16, rows_step, jnp.zeros((8, MC), F32), unroll=2)
        degi[pl.ds(j, 1), :] = jnp.sum(acc, axis=0, keepdims=True)

        @pl.when(j + NSLOT < n_itm // MC)
        def _():
            mask_copy(j + NSLOT).start()
        return 0

    with jax.named_scope("ph_mask0"):
        lax.fori_loop(0, 8, mask_step, 0)
    cp_i.wait()
    cp_u.wait()
    cp_t.wait()
    with jax.named_scope("ph_barrier"):
        pl.semaphore_wait(barrier, 7)
    rc_i = remote(own_i, own_i, ssem.at[0], rsem.at[0], sib)
    rc_u = remote(own_u, own_u, ssem.at[1], rsem.at[1], xpeer)
    rc_i.start()
    rc_u.start()
    with jax.named_scope("ph_mask1"):
        lax.fori_loop(8, n_itm // MC, mask_step, 0)

    degu[...] = jnp.sum(rowacc[...].T, axis=0, keepdims=True)
    rc_du = remote(degu, degu_r, ssem.at[2], rsem.at[2], xpeer)
    rc_di = remote(degi, degi_r, ssem.at[3], rsem.at[3], sib)
    rc_du.start()
    rc_di.start()

    def tri_row(k, row):
        return tri_v[pl.ds(k, 1), pl.ds(pl.multiple_of(row * 128, 128), 128)]

    def home_row(q):
        return (lax.rem(c + q, 2) * 2 + r) * (nhome // 128)

    nrow = nhome // 128
    idx_v[...] = jnp.zeros_like(idx_v)
    for k in range(2):
        for q in range(2):
            for row in range(nrow):
                loc = tri_row(k + 1, home_row(q) + row) - c * n_itm
                loc = jnp.where((loc >= 0) & (loc < n_itm), loc, n_itm)
                for t in range(4):
                    idx_v[k * 4 + t, :, pl.ds((q * nrow + row) * 128, 32)] = loc[:, t * 32:(t + 1) * 32]
    cp_x = []
    for t in range(8):
        cp_x.append(pltpu.make_async_copy(idx_v.at[t], idx_s[t], xsem.at[t]))
        cp_x[t].start()
    table[pl.ds(n_itm, 8), :] = jnp.zeros((8, dim), F32)

    with jax.named_scope("ph_di_wait"):
        rc_di.wait_recv()
    invi[...] = lax.rsqrt(jnp.maximum(degi[...] + degi_r[...], 1.0))
    rc_i.wait_recv()
    rc_u.wait_recv()
    for t in range(8):
        cp_x[t].wait()
    with jax.named_scope("ph_du_wait"):
        rc_du.wait_recv()
    inv_row = lax.rsqrt(jnp.maximum(degu[...] + degu_r[...], 1.0))
    invu[...] = jnp.broadcast_to(inv_row, (128, n_usr)).T

    nst = n_itm // WIDE

    def chunk1(base, size):
        cols = pl.ds(pl.multiple_of(base, size), size)
        return remote(i1p.at[:, cols], i1r.at[:, cols], cs1, cr1.at[base // WIDE], sib)

    def step1(i):
        cols = pl.ds(pl.multiple_of(i * WIDE, WIDE), WIDE)
        return remote(i1p.at[:, cols], i1r.at[:, cols], cs1, cr1.at[i], sib)

    def build_step(base, size):
        for nt in range(size // 256):
            cols = pl.ds(pl.multiple_of(base + nt * 256, 256), 256)
            lane = nt * 256 % MC
            wi = jnp.broadcast_to(invi[pl.ds(base // MC + nt * 256 // MC, 1), lane:lane + 256], (16, 256))
            tiles = []
            for g in range(n_usr // 16):
                rows = pl.ds(g * 16, 16)
                wu = jnp.concatenate([invu[rows, :]] * 2, axis=1)
                a = (wu * wi).astype(BF16) * adj[rows, cols]
                adj[rows, cols] = a
                tiles.append(a)
            part = jnp.dot(ut0[...], jnp.concatenate(tiles, axis=0), preferred_element_type=F32)
            i1p[:, cols] = part
        chunk1(base, size).start()
        return 0

    with jax.named_scope("ph_build"):
        nbig = n_itm // BIG - 1
        lax.fori_loop(0, nbig, lambda i, _: build_step(i * BIG, BIG), 0)
        lax.fori_loop(0, BIG // CH, lambda i, _: build_step(nbig * BIG + i * CH, CH), 0)

    def dot_t(a, b):
        return lax.dot_general(a, b, (((1,), (1,)), ((), ())), preferred_element_type=F32)

    def mixed_t(vals, base, beside=None):
        acc1 = acc2 = None
        for lo in range(0, WIDE, 512):
            ca = pl.ds(pl.multiple_of(base + lo, 256), 256)
            cb = pl.ds(pl.multiple_of(base + lo + 256, 256), 256)
            p1 = dot_t(vals[:, lo:lo + 256], adj[:, ca])
            p2 = dot_t(adj[:, cb], vals[:, lo + 256:lo + 512])
            acc1 = p1 if acc1 is None else acc1 + p1
            acc2 = p2 if acc2 is None else acc2 + p2
            if beside:
                beside(lo)
        return acc1 + acc2.T

    up[...] = jnp.zeros_like(up)

    def user_step(i, _):
        cols = pl.ds(pl.multiple_of(i * WIDE, WIDE), WIDE)
        step1(i).wait_recv()
        v1 = (i1p[:, cols] + i1r[:, cols]).astype(BF16)
        it1[:, cols] = v1
        up[...] += mixed_t(jnp.concatenate([it0[:, cols], v1], axis=0), i * WIDE)
        return 0

    with jax.named_scope("ph_user"):
        lax.fori_loop(0, nst, user_step, 0)
    rc_up = remote(up, up_r, ssem.at[4], rsem.at[4], xpeer)
    rc_up.start()
    pl.semaphore_signal(free_sem, inc=1, device_id=sib, device_id_type=MESH)

    remote(i1p, i1r, cs1, cr1.at[0], sib).wait_send()

    def sel_step(g, _):
        users = lax.broadcasted_iota(jnp.int32, (16, 128), 0) + g * 16
        for t in range(nhome // 128):
            ids = tri_row(0, home_row(0) + t)
            hit = jnp.where(users == jnp.broadcast_to(ids, (16, 128)), 1.0, 0.0)
            sel[pl.ds(pl.multiple_of(g * 16, 16), 16), t * 128:(t + 1) * 128] = hit.astype(BF16)
        return 0

    with jax.named_scope("ph_sel"):
        lax.fori_loop(0, 2 * n_usr // 16, sel_step, 0, unroll=2)
    with jax.named_scope("ph_up_wait"):
        rc_up.wait_recv()
    u12 = (up[...] + up_r[...]).astype(BF16)

    oo = r * half
    so = (1 - r) * half
    own = pl.ds(pl.multiple_of(oo, half), half)
    other = pl.ds(pl.multiple_of(so, half), half)

    def half2(k, size):
        src = pl.ds(pl.multiple_of(so + k * size, size), size)
        dst = pl.ds(pl.multiple_of(k * size, size), size)
        return remote(i2p.at[:, src], i2r.at[:, dst], cs2, cr2, sib)

    def half3(cols):
        return remote(i1p.at[:, cols], i1r.at[:, cols], cs1, cr1.at[0], sib)

    def rounded(ref, cols, k):
        return remote(ref.at[:, cols], ref.at[:, cols], ssem.at[k], rsem.at[k], sib)

    def item_step(k, base, size, send):
        cols = pl.ds(pl.multiple_of(base + k * size, size), size)
        part = jnp.dot(u12, adj[:, cols], preferred_element_type=F32)
        i2p[:, cols] = part[0:dim]
        i1p[:, cols] = part[dim:2 * dim]
        if send:
            half2(k, size).start()

    with jax.named_scope("ph_item"):
        for k in range(half // FIRST):
            item_step(k, so, FIRST, True)
        pl.semaphore_wait(free_sem, 1)
        half3(other).start()
        for k in range(half // NARROW):
            item_step(k, oo, NARROW, False)
    with jax.named_scope("ph_i2_wait"):
        half2(0, half).wait_recv()
    it2[:, own] = (i2p[:, own] + i2r[...]).astype(BF16)
    rounded(it2, own, 5).start()
    with jax.named_scope("ph_user3"):
        u3p[...] = mixed_t(it2[:, own], oo)

    def table_step(fin, base):
        fin = fin.astype(F32)
        for b in range(FIN // 128):
            table[pl.ds(pl.multiple_of(base + b * 128, 128), 128), :] = fin[:, b * 128:(b + 1) * 128].T

    def final_step(k, _):
        base = oo + k * FIN
        cols = pl.ds(pl.multiple_of(base, FIN), FIN)
        v3 = (i1p[:, cols] + i1r[:, cols]).astype(BF16)
        acc = it0[:, cols].astype(F32) + it1[:, cols].astype(F32)
        acc = (acc + it2[:, cols].astype(F32)) + v3.astype(F32)
        fin = (acc * (1.0 / (NUM_LAYERS + 1))).astype(BF16)
        it1[:, cols] = fin
        rounded(it1, cols, 8).start()
        return 0

    with jax.named_scope("ph_i3_wait"):
        half3(own).wait_recv()
    with jax.named_scope("ph_final"):
        lax.fori_loop(0, half // FIN, final_step, 0)
    oi_ref[...] = it1[:, own]

    def own_rows(lo):
        for b in range(4):
            at = pl.ds(pl.multiple_of(oo + lo + b * 128, 128), 128)
            table[at, :] = it1[:, at].astype(F32).T

    with jax.named_scope("ph_i2b_wait"):
        rounded(it2, other, 5).wait_recv()
    with jax.named_scope("ph_user3"):
        u3p[...] += mixed_t(it2[:, other], so, own_rows)
    rc_u3 = remote(u3p, u3_r, ssem.at[6], rsem.at[6], xpeer)
    rc_u3.start()

    def rows_step(k, start):
        base = start + k * FIN
        table_step(it1[:, pl.ds(pl.multiple_of(base, FIN), FIN)], base)
        return 0


    with jax.named_scope("ph_i3b_wait"):
        rounded(it1, other, 8).wait_recv()
    with jax.named_scope("ph_final"):
        lax.fori_loop(0, half // FIN, lambda k, _: rows_step(k, so), 0)

    def diff_row(q, row):
        def body(i, _):
            for u in range(8):
                at = (q * nrow + row) * 128 + i * 8 + u
                for t in range(4):
                    p = idx_s[t][0, at]
                    n = idx_s[4 + t][0, at]
                    dbuf[pl.ds(t * 32 + i * 8 + u, 1), :] = table[pl.ds(p, 1), :] - table[pl.ds(n, 1), :]
            return 0

        lax.fori_loop(0, 4, body, 0)
        cols = pl.ds(pl.multiple_of(row * 128, 128), 128)
        dt[q, :, cols] = dbuf[...].T
        if q:
            remote(dt.at[1, :, cols], drecv.at[:, cols], ds, dr, xpeer).start()
        return 0

    with jax.named_scope("ph_diff"):
        lax.fori_loop(0, nrow, lambda row, _: diff_row(1, row), 0)

    with jax.named_scope("ph_diff"):
        lax.fori_loop(0, nrow // 2, lambda row, _: diff_row(0, row), 0)

    with jax.named_scope("ph_u3_wait"):
        rc_u3.wait_recv()
    u3 = (u3p[...] + u3_r[...]).astype(BF16).astype(F32)
    uacc = ut0[...].astype(F32) + u12[0:dim].astype(F32)
    uacc = (uacc + u12[dim:2 * dim].astype(F32)) + u3
    fin_u = (uacc * (1.0 / (NUM_LAYERS + 1))).astype(BF16)
    own_cols = pl.ds(pl.multiple_of(r * n_usr, n_usr), n_usr)
    uall[:, own_cols] = fin_u
    rc_uf = remote(uall.at[:, own_cols], uall.at[:, own_cols], ssem.at[7], rsem.at[7], sib)
    rc_uf.start()
    ou_ref[...] = uall[:, pl.ds(pl.multiple_of(r * n_usr + c * uh, uh), uh)]
    with jax.named_scope("ph_diff"):
        lax.fori_loop(nrow // 2, nrow, lambda row, _: diff_row(0, row), 0)
    with jax.named_scope("ph_uf_wait"):
        rc_uf.wait_recv()
    urow = jnp.dot(uall[...], sel[...], preferred_element_type=F32)

    with jax.named_scope("ph_d_wait"):
        remote(dt.at[1], drecv, ds, dr, xpeer).wait_recv()
    score = jnp.sum((dt[0] + drecv[...]) * urow, axis=0, keepdims=True)
    for row in range(nrow):
        sbuf[pl.ds(row, 1), :] = score[:, row * 128:(row + 1) * 128]

    def s_send(q):
        dev = {"emb": lax.rem(e + q // 4, 2), "col": lax.rem(c + (q // 2) % 2, 2), "row": lax.rem(r + q % 2, 2)}
        return remote(sbuf, srecv.at[q - 1], bs, br, dev)

    for q in range(7, 0, -1):
        s_send(q).start()
    with jax.named_scope("ph_s_wait"):
        remote(srecv, srecv, bs, br, sib).wait_recv()
    for q in range(4):
        mine = sbuf[...] if q == 0 else srecv[q - 1]
        x = mine + srecv[q + 3]
        hq = lax.rem(c + q // 2, 2) * 2 + lax.rem(r + q % 2, 2)
        ls = jnp.maximum(-x, 0.0) + jnp.log1p(jnp.exp(-jnp.abs(x)))
        loss_ref[pl.ds(pl.multiple_of(hq * (nhome // 128), 8), nhome // 128), :] = ls

    with jax.named_scope("ph_drain"):
        half2(0, half).wait_send()
        half3(other).wait_send()
        rounded(it2, own, 5).wait_send()
        rounded(it1, own, 8).wait_send()
        for copy in (rc_i, rc_u, rc_du, rc_di, rc_up, rc_u3, rc_uf, remote(dt.at[1], drecv, ds, dr, xpeer),
                     remote(srecv, srecv, bs, br, sib)):
            copy.wait_send()


def store_kernel(*refs):
    srcs, dsts, sem = refs[0:3], refs[3:6], refs[6]
    copies = [pltpu.make_async_copy(a, b, sem.at[k]) for k, (a, b) in enumerate(zip(srcs, dsts))]
    for copy in copies:
        copy.start()
    for copy in copies:
        copy.wait()


def solution(mesh):
    def local_fn(mask_blk, user_sh, item_sh, triples):
        n_usr, n_itm = mask_blk.shape
        dim = user_sh.shape[1]
        n_trip = triples.shape[0]
        nch = n_itm // CH
        half = n_itm // 2
        tri = triples.T
        vm = pltpu.VMEM
        dma = pltpu.SemaphoreType.DMA
        nhome = n_trip // 4
        hrow = nhome // 4
        scratch = [
            vm((NSLOT, n_usr, MC), jnp.int32), vm((n_usr, n_itm + 256), BF16), vm((n_usr, 128), F32),
            vm((n_itm // MC, MC), F32), vm((n_itm // MC, MC), F32), vm((1, n_usr), F32), vm((1, n_usr), F32),
            vm((n_usr, 128), F32), vm((n_itm // MC, MC), F32),
            vm((dim, n_itm), BF16), vm((dim, n_itm), BF16), vm((dim, n_itm), BF16), vm((dim, n_usr), BF16),
            vm((dim, n_itm), F32), vm((dim, n_itm), F32), vm((dim, n_itm), F32), vm((dim, half), F32),
            vm((2 * dim, n_usr), F32), vm((2 * dim, n_usr), F32), vm((dim, n_usr), F32), vm((dim, n_usr), F32),
            vm((dim, 2 * n_usr), BF16), vm((2 * n_usr, nhome), BF16),
            vm((n_itm + 8, dim), F32),
            vm((3, n_trip), jnp.int32), vm((8, 1, 2 * nhome), jnp.int32),
            *[pltpu.SMEM((1, 2 * nhome), jnp.int32)] * 8,
            vm((128, dim), F32), vm((2, dim, nhome), F32), vm((dim, nhome), F32),
            vm((nhome // 128, 128), F32), vm((7, nhome // 128, 128), F32),
            dma((NSLOT,)), dma((3,)), dma((9,)), dma((9,)),
            dma(()), dma((n_itm // WIDE,)), dma(()), dma(()),
            dma(()), dma(()), dma(()), dma(()), dma((8,)), pltpu.SemaphoreType.REGULAR,
        ]
        hbm_spec = pl.BlockSpec(memory_space=pltpu.HBM)
        vmem_spec = pl.BlockSpec(memory_space=pltpu.VMEM)
        ou, oi, loss = pl.pallas_call(
            functools.partial(kernel, n_usr, n_itm, dim, n_trip),
            out_shape=(jax.ShapeDtypeStruct((dim, n_usr // 2), BF16),
                       jax.ShapeDtypeStruct((dim, half), BF16),
                       jax.ShapeDtypeStruct((n_trip // 128, 128), F32)),
            in_specs=[hbm_spec] * 4,
            out_specs=(vmem_spec,) * 3,
            scratch_shapes=scratch,
            compiler_params=pltpu.CompilerParams(collective_id=0, has_side_effects=True,
                                                 vmem_limit_bytes=50 * 1024 * 1024),
            name="gcn",
        )(mask_blk, *[pltpu.with_memory_space_constraint(v, pltpu.HBM) for v in (user_sh.T, item_sh.T, tri)])
        ou, oi, loss = pl.pallas_call(
            store_kernel,
            out_shape=tuple(jax.ShapeDtypeStruct(v.shape, v.dtype) for v in (ou, oi, loss)),
            in_specs=[vmem_spec] * 3,
            out_specs=(pl.BlockSpec(memory_space=pl.ANY),) * 3,
            scratch_shapes=[dma((3,))],
            compiler_params=pltpu.CompilerParams(vmem_limit_bytes=4 * 1024 * 1024),
            name="store",
        )(ou, oi, loss)
        return ou.T, oi.T, loss.reshape(n_trip)

    return jax.shard_map(
        local_fn, mesh=mesh,
        in_specs=(P("row", "col"), P(("row", "col"), "emb"), P(("col", "row"), "emb"), P()),
        out_specs=(P(("row", "col"), "emb"), P(("col", "row"), "emb"), P()),
        check_vma=False)
```

```python
import functools

import jax
import jax.numpy as jnp
from jax import lax
from jax.experimental import pallas as pl
from jax.experimental.pallas import tpu as pltpu
from jax.sharding import PartitionSpec as P

NUM_LAYERS = 3
BIG = 4096
CH = 2048
MC = 512
NSLOT = 8
FIN = 4096
WIDE = 8192
FIRST = 2048
NARROW = 4096
MESH = pl.DeviceIdType.MESH
F32 = jnp.float32
BF16 = jnp.bfloat16


def remote(src, dst, ssem, rsem, dev):
    return pltpu.make_async_remote_copy(src_ref=src, dst_ref=dst, send_sem=ssem, recv_sem=rsem,
                                        device_id=dev, device_id_type=MESH)


def kernel(n_usr, n_itm, dim, n_trip,
           mask_ref, eu_ref, ei_ref, tri_ref, ou_ref, oi_ref, loss_ref,
           stage, adj, rowacc, degi, degi_r, degu, degu_r, invu, invi,
           it0, it1, it2, ut0, i1p, i1r, i2p, i2r,
           up, up_r, u3p, u3_r, uall, sel, table,
           tri_v, idx_v, s0, s1, s2, s3, s4, s5, s6, s7, dbuf, dt, drecv, sbuf, srecv,
           msem, lsem, ssem, rsem, cs1, cr1, cs2, cr2, ds, dr, bs, br, xsem, free_sem):
    idx_s = (s0, s1, s2, s3, s4, s5, s6, s7)
    e = lax.axis_index("emb")
    c = lax.axis_index("col")
    r = lax.axis_index("row")
    sib = {"row": 1 - r}
    xpeer = {"col": 1 - c}
    nch = n_itm // CH
    half = n_itm // 2
    uh = n_usr // 2
    nhome = n_trip // 4
    hrow = nhome // 4

    def mask_copy(j):
        slot = lax.rem(j, NSLOT)
        return pltpu.make_async_copy(mask_ref.at[:, pl.ds(pl.multiple_of(j * MC, MC), MC)], stage.at[slot], msem.at[slot])

    for j in range(NSLOT):
        mask_copy(j).start()
    own_i = it0.at[:, pl.ds(pl.multiple_of(r * half, half), half)]
    own_u = ut0.at[:, pl.ds(pl.multiple_of(c * uh, uh), uh)]
    cp_i = pltpu.make_async_copy(ei_ref, own_i, lsem.at[0])
    cp_u = pltpu.make_async_copy(eu_ref, own_u, lsem.at[1])
    cp_t = pltpu.make_async_copy(tri_ref, tri_v, lsem.at[2])
    cp_i.start()
    cp_u.start()
    cp_t.start()

    barrier = pltpu.get_barrier_semaphore()
    for q in range(1, 8):
        dev = {"emb": lax.rem(e + q // 4, 2), "col": lax.rem(c + (q // 2) % 2, 2), "row": lax.rem(r + q % 2, 2)}
        pl.semaphore_signal(barrier, inc=1, device_id=dev, device_id_type=MESH)

    rowacc[...] = jnp.zeros_like(rowacc)

    def mask_step(j, _):
        slot = lax.rem(j, NSLOT)
        mask_copy(j).wait()
        cols = pl.ds(pl.multiple_of(j * MC, MC), MC)

        def rows_step(g, acc):
            rows = pl.ds(pl.multiple_of(g * 16, 16), 16)
            m = stage[slot, rows, :].astype(F32)
            adj[rows, cols] = m.astype(BF16)
            s = m[:, 0:128]
            for k in range(1, MC // 128):
                s = s + m[:, k * 128:(k + 1) * 128]
            rowacc[rows, :] += s
            return acc + (m[0:8] + m[8:16])

        acc = lax.fori_loop(0, n_usr // 16, rows_step, jnp.zeros((8, MC), F32), unroll=2)
        degi[pl.ds(j, 1), :] = jnp.sum(acc, axis=0, keepdims=True)

        @pl.when(j + NSLOT < n_itm // MC)
        def _():
            mask_copy(j + NSLOT).start()
        return 0

    with jax.named_scope("ph_mask0"):
        lax.fori_loop(0, 8, mask_step, 0)
    cp_i.wait()
    cp_u.wait()
    cp_t.wait()
    with jax.named_scope("ph_barrier"):
        pl.semaphore_wait(barrier, 7)
    rc_i = remote(own_i, own_i, ssem.at[0], rsem.at[0], sib)
    rc_u = remote(own_u, own_u, ssem.at[1], rsem.at[1], xpeer)
    rc_i.start()
    rc_u.start()
    with jax.named_scope("ph_mask1"):
        lax.fori_loop(8, n_itm // MC, mask_step, 0)

    degu[...] = jnp.sum(rowacc[...].T, axis=0, keepdims=True)
    rc_du = remote(degu, degu_r, ssem.at[2], rsem.at[2], xpeer)
    rc_di = remote(degi, degi_r, ssem.at[3], rsem.at[3], sib)
    rc_du.start()
    rc_di.start()

    def tri_row(k, row):
        return tri_v[pl.ds(k, 1), pl.ds(pl.multiple_of(row * 128, 128), 128)]

    def home_row(q):
        return (lax.rem(c + q, 2) * 2 + r) * (nhome // 128)

    nrow = nhome // 128
    idx_v[...] = jnp.zeros_like(idx_v)
    for k in range(2):
        for q in range(2):
            for row in range(nrow):
                loc = tri_row(k + 1, home_row(q) + row) - c * n_itm
                loc = jnp.where((loc >= 0) & (loc < n_itm), loc, n_itm)
                for t in range(4):
                    idx_v[k * 4 + t, :, pl.ds((q * nrow + row) * 128, 32)] = loc[:, t * 32:(t + 1) * 32]
    cp_x = []
    for t in range(8):
        cp_x.append(pltpu.make_async_copy(idx_v.at[t], idx_s[t], xsem.at[t]))
        cp_x[t].start()
    table[pl.ds(n_itm, 8), :] = jnp.zeros((8, dim), F32)

    with jax.named_scope("ph_di_wait"):
        rc_di.wait_recv()
    invi[...] = lax.rsqrt(jnp.maximum(degi[...] + degi_r[...], 1.0))
    rc_i.wait_recv()
    rc_u.wait_recv()
    with jax.named_scope("ph_du_wait"):
        rc_du.wait_recv()
    inv_row = lax.rsqrt(jnp.maximum(degu[...] + degu_r[...], 1.0))
    invu[...] = jnp.broadcast_to(inv_row, (128, n_usr)).T

    nst = n_itm // WIDE

    def chunk1(base, size):
        cols = pl.ds(pl.multiple_of(base, size), size)
        return remote(i1p.at[:, cols], i1r.at[:, cols], cs1, cr1.at[base // WIDE], sib)

    def step1(i):
        cols = pl.ds(pl.multiple_of(i * WIDE, WIDE), WIDE)
        return remote(i1p.at[:, cols], i1r.at[:, cols], cs1, cr1.at[i], sib)

    def build_step(base, size):
        for nt in range(size // 256):
            cols = pl.ds(pl.multiple_of(base + nt * 256, 256), 256)
            lane = nt * 256 % MC
            wi = jnp.broadcast_to(invi[pl.ds(base // MC + nt * 256 // MC, 1), lane:lane + 256], (16, 256))
            tiles = []
            for g in range(n_usr // 16):
                rows = pl.ds(g * 16, 16)
                wu = jnp.concatenate([invu[rows, :]] * 2, axis=1)
                a = (wu * wi).astype(BF16) * adj[rows, cols]
                adj[rows, cols] = a
                tiles.append(a)
            part = jnp.dot(ut0[...], jnp.concatenate(tiles, axis=0), preferred_element_type=F32)
            i1p[:, cols] = part
        chunk1(base, size).start()
        return 0

    with jax.named_scope("ph_build"):
        nbig = n_itm // BIG - 1
        lax.fori_loop(0, nbig, lambda i, _: build_step(i * BIG, BIG), 0)
        lax.fori_loop(0, BIG // CH, lambda i, _: build_step(nbig * BIG + i * CH, CH), 0)

    def dot_t(a, b):
        return lax.dot_general(a, b, (((1,), (1,)), ((), ())), preferred_element_type=F32)

    def mixed_t(vals, base, beside=None):
        acc1 = acc2 = None
        for lo in range(0, WIDE, 512):
            ca = pl.ds(pl.multiple_of(base + lo, 256), 256)
            cb = pl.ds(pl.multiple_of(base + lo + 256, 256), 256)
            p1 = dot_t(vals[:, lo:lo + 256], adj[:, ca])
            p2 = dot_t(adj[:, cb], vals[:, lo + 256:lo + 512])
            acc1 = p1 if acc1 is None else acc1 + p1
            acc2 = p2 if acc2 is None else acc2 + p2
            if beside:
                beside(lo)
        return acc1 + acc2.T

    up[...] = jnp.zeros_like(up)

    def user_step(i, _):
        cols = pl.ds(pl.multiple_of(i * WIDE, WIDE), WIDE)
        step1(i).wait_recv()
        v1 = (i1p[:, cols] + i1r[:, cols]).astype(BF16)
        it1[:, cols] = v1
        up[...] += mixed_t(jnp.concatenate([it0[:, cols], v1], axis=0), i * WIDE)
        return 0

    with jax.named_scope("ph_user"):
        lax.fori_loop(0, nst, user_step, 0)
    rc_up = remote(up, up_r, ssem.at[4], rsem.at[4], xpeer)
    rc_up.start()
    pl.semaphore_signal(free_sem, inc=1, device_id=sib, device_id_type=MESH)

    remote(i1p, i1r, cs1, cr1.at[0], sib).wait_send()

    def sel_step(g, _):
        users = lax.broadcasted_iota(jnp.int32, (16, 128), 0) + g * 16
        for t in range(nhome // 128):
            ids = tri_row(0, home_row(0) + t)
            hit = jnp.where(users == jnp.broadcast_to(ids, (16, 128)), 1.0, 0.0)
            sel[pl.ds(pl.multiple_of(g * 16, 16), 16), t * 128:(t + 1) * 128] = hit.astype(BF16)
        return 0

    with jax.named_scope("ph_sel"):
        lax.fori_loop(0, 2 * n_usr // 16, sel_step, 0, unroll=2)
    with jax.named_scope("ph_up_wait"):
        rc_up.wait_recv()
    u12 = (up[...] + up_r[...]).astype(BF16)

    oo = r * half
    so = (1 - r) * half
    own = pl.ds(pl.multiple_of(oo, half), half)
    other = pl.ds(pl.multiple_of(so, half), half)

    def half2(k, size):
        src = pl.ds(pl.multiple_of(so + k * size, size), size)
        dst = pl.ds(pl.multiple_of(k * size, size), size)
        return remote(i2p.at[:, src], i2r.at[:, dst], cs2, cr2, sib)

    def half3(cols):
        return remote(i1p.at[:, cols], i1r.at[:, cols], cs1, cr1.at[0], sib)

    def rounded(ref, cols, k):
        return remote(ref.at[:, cols], ref.at[:, cols], ssem.at[k], rsem.at[k], sib)

    def item_step(k, base, size, send):
        cols = pl.ds(pl.multiple_of(base + k * size, size), size)
        part = jnp.dot(u12, adj[:, cols], preferred_element_type=F32)
        i2p[:, cols] = part[0:dim]
        i1p[:, cols] = part[dim:2 * dim]
        if send:
            half2(k, size).start()

    with jax.named_scope("ph_item"):
        for k in range(half // FIRST):
            item_step(k, so, FIRST, True)
        pl.semaphore_wait(free_sem, 1)
        half3(other).start()
        for k in range(half // NARROW):
            item_step(k, oo, NARROW, False)
    with jax.named_scope("ph_i2_wait"):
        half2(0, half).wait_recv()
    it2[:, own] = (i2p[:, own] + i2r[...]).astype(BF16)
    rounded(it2, own, 5).start()
    with jax.named_scope("ph_user3"):
        u3p[...] = mixed_t(it2[:, own], oo)

    def table_step(fin, base):
        fin = fin.astype(F32)
        for b in range(FIN // 128):
            table[pl.ds(pl.multiple_of(base + b * 128, 128), 128), :] = fin[:, b * 128:(b + 1) * 128].T

    def final_step(k, _):
        base = oo + k * FIN
        cols = pl.ds(pl.multiple_of(base, FIN), FIN)
        v3 = (i1p[:, cols] + i1r[:, cols]).astype(BF16)
        acc = it0[:, cols].astype(F32) + it1[:, cols].astype(F32)
        acc = (acc + it2[:, cols].astype(F32)) + v3.astype(F32)
        fin = (acc * (1.0 / (NUM_LAYERS + 1))).astype(BF16)
        it1[:, cols] = fin
        rounded(it1, cols, 8).start()
        return 0

    with jax.named_scope("ph_i3_wait"):
        half3(own).wait_recv()
    with jax.named_scope("ph_final"):
        lax.fori_loop(0, half // FIN, final_step, 0)
    oi_ref[...] = it1[:, own]

    def own_rows(lo):
        for b in range(4):
            at = pl.ds(pl.multiple_of(oo + lo + b * 128, 128), 128)
            table[at, :] = it1[:, at].astype(F32).T

    with jax.named_scope("ph_i2b_wait"):
        rounded(it2, other, 5).wait_recv()
    with jax.named_scope("ph_user3"):
        u3p[...] += mixed_t(it2[:, other], so, own_rows)
    rc_u3 = remote(u3p, u3_r, ssem.at[6], rsem.at[6], xpeer)
    rc_u3.start()

    def rows_step(k, start):
        base = start + k * FIN
        table_step(it1[:, pl.ds(pl.multiple_of(base, FIN), FIN)], base)
        return 0


    with jax.named_scope("ph_i3b_wait"):
        rounded(it1, other, 8).wait_recv()
    with jax.named_scope("ph_final"):
        lax.fori_loop(0, half // FIN, lambda k, _: rows_step(k, so), 0)

    def diff_row(q, row):
        def body(i, _):
            for u in range(8):
                at = (q * nrow + row) * 128 + i * 8 + u
                for t in range(4):
                    p = idx_s[t][0, at]
                    n = idx_s[4 + t][0, at]
                    dbuf[pl.ds(t * 32 + i * 8 + u, 1), :] = table[pl.ds(p, 1), :] - table[pl.ds(n, 1), :]
            return 0

        lax.fori_loop(0, 4, body, 0)
        cols = pl.ds(pl.multiple_of(row * 128, 128), 128)
        dt[q, :, cols] = dbuf[...].T
        if q:
            remote(dt.at[1, :, cols], drecv.at[:, cols], ds, dr, xpeer).start()
        return 0

    for t in range(8):
        cp_x[t].wait()
    with jax.named_scope("ph_diff"):
        lax.fori_loop(0, nrow, lambda row, _: diff_row(1, row), 0)

    with jax.named_scope("ph_diff"):
        lax.fori_loop(0, nrow // 2, lambda row, _: diff_row(0, row), 0)

    with jax.named_scope("ph_u3_wait"):
        rc_u3.wait_recv()
    u3 = (u3p[...] + u3_r[...]).astype(BF16).astype(F32)
    uacc = ut0[...].astype(F32) + u12[0:dim].astype(F32)
    uacc = (uacc + u12[dim:2 * dim].astype(F32)) + u3
    fin_u = (uacc * (1.0 / (NUM_LAYERS + 1))).astype(BF16)
    own_cols = pl.ds(pl.multiple_of(r * n_usr, n_usr), n_usr)
    uall[:, own_cols] = fin_u
    rc_uf = remote(uall.at[:, own_cols], uall.at[:, own_cols], ssem.at[7], rsem.at[7], sib)
    rc_uf.start()
    ou_ref[...] = uall[:, pl.ds(pl.multiple_of(r * n_usr + c * uh, uh), uh)]
    with jax.named_scope("ph_diff"):
        lax.fori_loop(nrow // 2, nrow, lambda row, _: diff_row(0, row), 0)
    with jax.named_scope("ph_uf_wait"):
        rc_uf.wait_recv()
    urow = jnp.dot(uall[...], sel[...], preferred_element_type=F32)

    with jax.named_scope("ph_d_wait"):
        remote(dt.at[1], drecv, ds, dr, xpeer).wait_recv()
    score = jnp.sum((dt[0] + drecv[...]) * urow, axis=0, keepdims=True)
    for row in range(nrow):
        sbuf[pl.ds(row, 1), :] = score[:, row * 128:(row + 1) * 128]

    def s_send(q):
        dev = {"emb": lax.rem(e + q // 4, 2), "col": lax.rem(c + (q // 2) % 2, 2), "row": lax.rem(r + q % 2, 2)}
        return remote(sbuf, srecv.at[q - 1], bs, br, dev)

    for q in range(7, 0, -1):
        s_send(q).start()
    with jax.named_scope("ph_s_wait"):
        remote(srecv, srecv, bs, br, sib).wait_recv()
    for q in range(4):
        mine = sbuf[...] if q == 0 else srecv[q - 1]
        x = mine + srecv[q + 3]
        hq = lax.rem(c + q // 2, 2) * 2 + lax.rem(r + q % 2, 2)
        ls = jnp.maximum(-x, 0.0) + jnp.log1p(jnp.exp(-jnp.abs(x)))
        loss_ref[pl.ds(pl.multiple_of(hq * (nhome // 128), 8), nhome // 128), :] = ls

    with jax.named_scope("ph_drain"):
        half2(0, half).wait_send()
        half3(other).wait_send()
        rounded(it2, own, 5).wait_send()
        rounded(it1, own, 8).wait_send()
        for copy in (rc_i, rc_u, rc_du, rc_di, rc_up, rc_u3, rc_uf, remote(dt.at[1], drecv, ds, dr, xpeer),
                     remote(srecv, srecv, bs, br, sib)):
            copy.wait_send()


def store_kernel(*refs):
    srcs, dsts, sem = refs[0:3], refs[3:6], refs[6]
    copies = [pltpu.make_async_copy(a, b, sem.at[k]) for k, (a, b) in enumerate(zip(srcs, dsts))]
    for copy in copies:
        copy.start()
    for copy in copies:
        copy.wait()


def solution(mesh):
    def local_fn(mask_blk, user_sh, item_sh, triples):
        n_usr, n_itm = mask_blk.shape
        dim = user_sh.shape[1]
        n_trip = triples.shape[0]
        nch = n_itm // CH
        half = n_itm // 2
        tri = triples.T
        vm = pltpu.VMEM
        dma = pltpu.SemaphoreType.DMA
        nhome = n_trip // 4
        hrow = nhome // 4
        scratch = [
            vm((NSLOT, n_usr, MC), jnp.int32), vm((n_usr, n_itm + 256), BF16), vm((n_usr, 128), F32),
            vm((n_itm // MC, MC), F32), vm((n_itm // MC, MC), F32), vm((1, n_usr), F32), vm((1, n_usr), F32),
            vm((n_usr, 128), F32), vm((n_itm // MC, MC), F32),
            vm((dim, n_itm), BF16), vm((dim, n_itm), BF16), vm((dim, n_itm), BF16), vm((dim, n_usr), BF16),
            vm((dim, n_itm), F32), vm((dim, n_itm), F32), vm((dim, n_itm), F32), vm((dim, half), F32),
            vm((2 * dim, n_usr), F32), vm((2 * dim, n_usr), F32), vm((dim, n_usr), F32), vm((dim, n_usr), F32),
            vm((dim, 2 * n_usr), BF16), vm((2 * n_usr, nhome), BF16),
            vm((n_itm + 8, dim), F32),
            vm((3, n_trip), jnp.int32), vm((8, 1, 2 * nhome), jnp.int32),
            *[pltpu.SMEM((1, 2 * nhome), jnp.int32)] * 8,
            vm((128, dim), F32), vm((2, dim, nhome), F32), vm((dim, nhome), F32),
            vm((nhome // 128, 128), F32), vm((7, nhome // 128, 128), F32),
            dma((NSLOT,)), dma((3,)), dma((9,)), dma((9,)),
            dma(()), dma((n_itm // WIDE,)), dma(()), dma(()),
            dma(()), dma(()), dma(()), dma(()), dma((8,)), pltpu.SemaphoreType.REGULAR,
        ]
        hbm_spec = pl.BlockSpec(memory_space=pltpu.HBM)
        vmem_spec = pl.BlockSpec(memory_space=pltpu.VMEM)
        ou, oi, loss = pl.pallas_call(
            functools.partial(kernel, n_usr, n_itm, dim, n_trip),
            out_shape=(jax.ShapeDtypeStruct((dim, n_usr // 2), BF16),
                       jax.ShapeDtypeStruct((dim, half), BF16),
                       jax.ShapeDtypeStruct((n_trip // 128, 128), F32)),
            in_specs=[hbm_spec] * 4,
            out_specs=(vmem_spec,) * 3,
            scratch_shapes=scratch,
            compiler_params=pltpu.CompilerParams(collective_id=0, has_side_effects=True,
                                                 vmem_limit_bytes=50 * 1024 * 1024),
            name="gcn",
        )(mask_blk, *[pltpu.with_memory_space_constraint(v, pltpu.HBM) for v in (user_sh.T, item_sh.T, tri)])
        ou, oi, loss = pl.pallas_call(
            store_kernel,
            out_shape=tuple(jax.ShapeDtypeStruct(v.shape, v.dtype) for v in (ou, oi, loss)),
            in_specs=[vmem_spec] * 3,
            out_specs=(pl.BlockSpec(memory_space=pl.ANY),) * 3,
            scratch_shapes=[dma((3,))],
            compiler_params=pltpu.CompilerParams(vmem_limit_bytes=4 * 1024 * 1024),
            name="store",
        )(ou, oi, loss)
        return ou.T, oi.T, loss.reshape(n_trip)

    return jax.shard_map(
        local_fn, mesh=mesh,
        in_specs=(P("row", "col"), P(("row", "col"), "emb"), P(("col", "row"), "emb"), P()),
        out_specs=(P(("row", "col"), "emb"), P(("col", "row"), "emb"), P()),
        check_vma=False)
```

```python
import functools

import jax
import jax.numpy as jnp
from jax import lax
from jax.experimental import pallas as pl
from jax.experimental.pallas import tpu as pltpu
from jax.sharding import PartitionSpec as P

NUM_LAYERS = 3
BIG = 4096
CH = 2048
MC = 512
NSLOT = 8
FIN = 4096
WIDE = 8192
FIRST = 2048
NARROW = 4096
MESH = pl.DeviceIdType.MESH
F32 = jnp.float32
BF16 = jnp.bfloat16


def remote(src, dst, ssem, rsem, dev):
    return pltpu.make_async_remote_copy(src_ref=src, dst_ref=dst, send_sem=ssem, recv_sem=rsem,
                                        device_id=dev, device_id_type=MESH)


def kernel(n_usr, n_itm, dim, n_trip,
           mask_ref, eu_ref, ei_ref, tri_ref, ou_ref, oi_ref, loss_ref,
           stage, adj, rowacc, degi, degi_r, degu, degu_r, invu, invi,
           it0, it1, it2, ut0, i1p, i1r, i2p, i2r,
           up, up_r, u3p, u3_r, uall, sel, table,
           tri_v, idx_v, s0, s1, s2, s3, s4, s5, s6, s7, dbuf, dt, drecv, sbuf, srecv,
           msem, lsem, ssem, rsem, cs1, cr1, cs2, cr2, ds, dr, bs, br, xsem, free_sem):
    idx_s = (s0, s1, s2, s3, s4, s5, s6, s7)
    e = lax.axis_index("emb")
    c = lax.axis_index("col")
    r = lax.axis_index("row")
    sib = {"row": 1 - r}
    xpeer = {"col": 1 - c}
    nch = n_itm // CH
    half = n_itm // 2
    uh = n_usr // 2
    nhome = n_trip // 4
    hrow = nhome // 4

    def mask_copy(j):
        slot = lax.rem(j, NSLOT)
        return pltpu.make_async_copy(mask_ref.at[:, pl.ds(pl.multiple_of(j * MC, MC), MC)], stage.at[slot], msem.at[slot])

    for j in range(NSLOT):
        mask_copy(j).start()
    own_i = it0.at[:, pl.ds(pl.multiple_of(r * half, half), half)]
    own_u = ut0.at[:, pl.ds(pl.multiple_of(c * uh, uh), uh)]
    cp_i = pltpu.make_async_copy(ei_ref, own_i, lsem.at[0])
    cp_u = pltpu.make_async_copy(eu_ref, own_u, lsem.at[1])
    cp_t = pltpu.make_async_copy(tri_ref, tri_v, lsem.at[2])
    cp_i.start()
    cp_u.start()
    cp_t.start()

    barrier = pltpu.get_barrier_semaphore()
    for q in range(1, 8):
        dev = {"emb": lax.rem(e + q // 4, 2), "col": lax.rem(c + (q // 2) % 2, 2), "row": lax.rem(r + q % 2, 2)}
        pl.semaphore_signal(barrier, inc=1, device_id=dev, device_id_type=MESH)

    rowacc[...] = jnp.zeros_like(rowacc)

    def mask_step(j, _):
        slot = lax.rem(j, NSLOT)
        mask_copy(j).wait()
        cols = pl.ds(pl.multiple_of(j * MC, MC), MC)

        def rows_step(g, acc):
            rows = pl.ds(pl.multiple_of(g * 16, 16), 16)
            m = stage[slot, rows, :].astype(F32)
            adj[rows, cols] = m.astype(BF16)
            s = m[:, 0:128]
            for k in range(1, MC // 128):
                s = s + m[:, k * 128:(k + 1) * 128]
            rowacc[rows, :] += s
            return acc + (m[0:8] + m[8:16])

        acc = lax.fori_loop(0, n_usr // 16, rows_step, jnp.zeros((8, MC), F32), unroll=8)
        degi[pl.ds(j, 1), :] = jnp.sum(acc, axis=0, keepdims=True)

        @pl.when(j + NSLOT < n_itm // MC)
        def _():
            mask_copy(j + NSLOT).start()
        return 0

    with jax.named_scope("ph_mask0"):
        lax.fori_loop(0, 8, mask_step, 0)
    cp_i.wait()
    cp_u.wait()
    cp_t.wait()
    with jax.named_scope("ph_barrier"):
        pl.semaphore_wait(barrier, 7)
    rc_i = remote(own_i, own_i, ssem.at[0], rsem.at[0], sib)
    rc_u = remote(own_u, own_u, ssem.at[1], rsem.at[1], xpeer)
    rc_i.start()
    rc_u.start()
    with jax.named_scope("ph_mask1"):
        lax.fori_loop(8, n_itm // MC, mask_step, 0)

    degu[...] = jnp.sum(rowacc[...].T, axis=0, keepdims=True)
    rc_du = remote(degu, degu_r, ssem.at[2], rsem.at[2], xpeer)
    rc_di = remote(degi, degi_r, ssem.at[3], rsem.at[3], sib)
    rc_du.start()
    rc_di.start()

    def tri_row(k, row):
        return tri_v[pl.ds(k, 1), pl.ds(pl.multiple_of(row * 128, 128), 128)]

    def home_row(q):
        return (lax.rem(c + q, 2) * 2 + r) * (nhome // 128)

    nrow = nhome // 128
    idx_v[...] = jnp.zeros_like(idx_v)
    for k in range(2):
        for q in range(2):
            for row in range(nrow):
                loc = tri_row(k + 1, home_row(q) + row) - c * n_itm
                loc = jnp.where((loc >= 0) & (loc < n_itm), loc, n_itm)
                for t in range(4):
                    idx_v[k * 4 + t, :, pl.ds((q * nrow + row) * 128, 32)] = loc[:, t * 32:(t + 1) * 32]
    cp_x = []
    for t in range(8):
        cp_x.append(pltpu.make_async_copy(idx_v.at[t], idx_s[t], xsem.at[t]))
        cp_x[t].start()
    table[pl.ds(n_itm, 8), :] = jnp.zeros((8, dim), F32)

    with jax.named_scope("ph_di_wait"):
        rc_di.wait_recv()
    invi[...] = lax.rsqrt(jnp.maximum(degi[...] + degi_r[...], 1.0))
    rc_i.wait_recv()
    rc_u.wait_recv()
    with jax.named_scope("ph_du_wait"):
        rc_du.wait_recv()
    inv_row = lax.rsqrt(jnp.maximum(degu[...] + degu_r[...], 1.0))
    invu[...] = jnp.broadcast_to(inv_row, (128, n_usr)).T

    nst = n_itm // WIDE

    def chunk1(base, size):
        cols = pl.ds(pl.multiple_of(base, size), size)
        return remote(i1p.at[:, cols], i1r.at[:, cols], cs1, cr1.at[base // WIDE], sib)

    def step1(i):
        cols = pl.ds(pl.multiple_of(i * WIDE, WIDE), WIDE)
        return remote(i1p.at[:, cols], i1r.at[:, cols], cs1, cr1.at[i], sib)

    def build_step(base, size):
        for nt in range(size // 256):
            cols = pl.ds(pl.multiple_of(base + nt * 256, 256), 256)
            lane = nt * 256 % MC
            wi = jnp.broadcast_to(invi[pl.ds(base // MC + nt * 256 // MC, 1), lane:lane + 256], (16, 256))
            tiles = []
            for g in range(n_usr // 16):
                rows = pl.ds(g * 16, 16)
                wu = jnp.concatenate([invu[rows, :]] * 2, axis=1)
                a = (wu * wi).astype(BF16) * adj[rows, cols]
                adj[rows, cols] = a
                tiles.append(a)
            part = jnp.dot(ut0[...], jnp.concatenate(tiles, axis=0), preferred_element_type=F32)
            i1p[:, cols] = part
        chunk1(base, size).start()
        return 0

    with jax.named_scope("ph_build"):
        nbig = n_itm // BIG - 1
        lax.fori_loop(0, nbig, lambda i, _: build_step(i * BIG, BIG), 0)
        lax.fori_loop(0, BIG // CH, lambda i, _: build_step(nbig * BIG + i * CH, CH), 0)

    def dot_t(a, b):
        return lax.dot_general(a, b, (((1,), (1,)), ((), ())), preferred_element_type=F32)

    def mixed_t(vals, base, beside=None):
        acc1 = acc2 = None
        for lo in range(0, WIDE, 512):
            ca = pl.ds(pl.multiple_of(base + lo, 256), 256)
            cb = pl.ds(pl.multiple_of(base + lo + 256, 256), 256)
            p1 = dot_t(vals[:, lo:lo + 256], adj[:, ca])
            p2 = dot_t(adj[:, cb], vals[:, lo + 256:lo + 512])
            acc1 = p1 if acc1 is None else acc1 + p1
            acc2 = p2 if acc2 is None else acc2 + p2
            if beside:
                beside(lo)
        return acc1 + acc2.T

    up[...] = jnp.zeros_like(up)

    def user_step(i, _):
        cols = pl.ds(pl.multiple_of(i * WIDE, WIDE), WIDE)
        step1(i).wait_recv()
        v1 = (i1p[:, cols] + i1r[:, cols]).astype(BF16)
        it1[:, cols] = v1
        up[...] += mixed_t(jnp.concatenate([it0[:, cols], v1], axis=0), i * WIDE)
        return 0

    with jax.named_scope("ph_user"):
        lax.fori_loop(0, nst, user_step, 0)
    rc_up = remote(up, up_r, ssem.at[4], rsem.at[4], xpeer)
    rc_up.start()
    pl.semaphore_signal(free_sem, inc=1, device_id=sib, device_id_type=MESH)

    remote(i1p, i1r, cs1, cr1.at[0], sib).wait_send()

    def sel_step(g, _):
        users = lax.broadcasted_iota(jnp.int32, (16, 128), 0) + g * 16
        for t in range(nhome // 128):
            ids = tri_row(0, home_row(0) + t)
            hit = jnp.where(users == jnp.broadcast_to(ids, (16, 128)), 1.0, 0.0)
            sel[pl.ds(pl.multiple_of(g * 16, 16), 16), t * 128:(t + 1) * 128] = hit.astype(BF16)
        return 0

    with jax.named_scope("ph_sel"):
        lax.fori_loop(0, 2 * n_usr // 16, sel_step, 0, unroll=2)
    with jax.named_scope("ph_up_wait"):
        rc_up.wait_recv()
    u12 = (up[...] + up_r[...]).astype(BF16)

    oo = r * half
    so = (1 - r) * half
    own = pl.ds(pl.multiple_of(oo, half), half)
    other = pl.ds(pl.multiple_of(so, half), half)

    def half2(k, size):
        src = pl.ds(pl.multiple_of(so + k * size, size), size)
        dst = pl.ds(pl.multiple_of(k * size, size), size)
        return remote(i2p.at[:, src], i2r.at[:, dst], cs2, cr2, sib)

    def half3(cols):
        return remote(i1p.at[:, cols], i1r.at[:, cols], cs1, cr1.at[0], sib)

    def rounded(ref, cols, k):
        return remote(ref.at[:, cols], ref.at[:, cols], ssem.at[k], rsem.at[k], sib)

    def item_step(k, base, size, send):
        cols = pl.ds(pl.multiple_of(base + k * size, size), size)
        part = jnp.dot(u12, adj[:, cols], preferred_element_type=F32)
        i2p[:, cols] = part[0:dim]
        i1p[:, cols] = part[dim:2 * dim]
        if send:
            half2(k, size).start()

    with jax.named_scope("ph_item"):
        for k in range(half // FIRST):
            item_step(k, so, FIRST, True)
        pl.semaphore_wait(free_sem, 1)
        half3(other).start()
        for k in range(half // NARROW):
            item_step(k, oo, NARROW, False)
    with jax.named_scope("ph_i2_wait"):
        half2(0, half).wait_recv()
    it2[:, own] = (i2p[:, own] + i2r[...]).astype(BF16)
    rounded(it2, own, 5).start()
    with jax.named_scope("ph_user3"):
        u3p[...] = mixed_t(it2[:, own], oo)

    def table_step(fin, base):
        fin = fin.astype(F32)
        for b in range(FIN // 128):
            table[pl.ds(pl.multiple_of(base + b * 128, 128), 128), :] = fin[:, b * 128:(b + 1) * 128].T

    def final_step(k, _):
        base = oo + k * FIN
        cols = pl.ds(pl.multiple_of(base, FIN), FIN)
        v3 = (i1p[:, cols] + i1r[:, cols]).astype(BF16)
        acc = it0[:, cols].astype(F32) + it1[:, cols].astype(F32)
        acc = (acc + it2[:, cols].astype(F32)) + v3.astype(F32)
        fin = (acc * (1.0 / (NUM_LAYERS + 1))).astype(BF16)
        it1[:, cols] = fin
        rounded(it1, cols, 8).start()
        return 0

    with jax.named_scope("ph_i3_wait"):
        half3(own).wait_recv()
    with jax.named_scope("ph_final"):
        lax.fori_loop(0, half // FIN, final_step, 0)
    oi_ref[...] = it1[:, own]

    def own_rows(lo):
        for b in range(4):
            at = pl.ds(pl.multiple_of(oo + lo + b * 128, 128), 128)
            table[at, :] = it1[:, at].astype(F32).T

    with jax.named_scope("ph_i2b_wait"):
        rounded(it2, other, 5).wait_recv()
    with jax.named_scope("ph_user3"):
        u3p[...] += mixed_t(it2[:, other], so, own_rows)
    rc_u3 = remote(u3p, u3_r, ssem.at[6], rsem.at[6], xpeer)
    rc_u3.start()

    def rows_step(k, start):
        base = start + k * FIN
        table_step(it1[:, pl.ds(pl.multiple_of(base, FIN), FIN)], base)
        return 0


    with jax.named_scope("ph_i3b_wait"):
        rounded(it1, other, 8).wait_recv()
    with jax.named_scope("ph_final"):
        lax.fori_loop(0, half // FIN, lambda k, _: rows_step(k, so), 0)

    def diff_row(q, row):
        def body(i, _):
            for u in range(8):
                at = (q * nrow + row) * 128 + i * 8 + u
                for t in range(4):
                    p = idx_s[t][0, at]
                    n = idx_s[4 + t][0, at]
                    dbuf[pl.ds(t * 32 + i * 8 + u, 1), :] = table[pl.ds(p, 1), :] - table[pl.ds(n, 1), :]
            return 0

        lax.fori_loop(0, 4, body, 0)
        cols = pl.ds(pl.multiple_of(row * 128, 128), 128)
        dt[q, :, cols] = dbuf[...].T
        if q:
            remote(dt.at[1, :, cols], drecv.at[:, cols], ds, dr, xpeer).start()
        return 0

    for t in range(8):
        cp_x[t].wait()
    with jax.named_scope("ph_diff"):
        lax.fori_loop(0, nrow, lambda row, _: diff_row(1, row), 0)

    with jax.named_scope("ph_diff"):
        lax.fori_loop(0, nrow // 2, lambda row, _: diff_row(0, row), 0)

    with jax.named_scope("ph_u3_wait"):
        rc_u3.wait_recv()
    u3 = (u3p[...] + u3_r[...]).astype(BF16).astype(F32)
    uacc = ut0[...].astype(F32) + u12[0:dim].astype(F32)
    uacc = (uacc + u12[dim:2 * dim].astype(F32)) + u3
    fin_u = (uacc * (1.0 / (NUM_LAYERS + 1))).astype(BF16)
    own_cols = pl.ds(pl.multiple_of(r * n_usr, n_usr), n_usr)
    uall[:, own_cols] = fin_u
    rc_uf = remote(uall.at[:, own_cols], uall.at[:, own_cols], ssem.at[7], rsem.at[7], sib)
    rc_uf.start()
    ou_ref[...] = uall[:, pl.ds(pl.multiple_of(r * n_usr + c * uh, uh), uh)]
    with jax.named_scope("ph_diff"):
        lax.fori_loop(nrow // 2, nrow, lambda row, _: diff_row(0, row), 0)
    with jax.named_scope("ph_uf_wait"):
        rc_uf.wait_recv()
    urow = jnp.dot(uall[...], sel[...], preferred_element_type=F32)

    with jax.named_scope("ph_d_wait"):
        remote(dt.at[1], drecv, ds, dr, xpeer).wait_recv()
    score = jnp.sum((dt[0] + drecv[...]) * urow, axis=0, keepdims=True)
    for row in range(nrow):
        sbuf[pl.ds(row, 1), :] = score[:, row * 128:(row + 1) * 128]

    def s_send(q):
        dev = {"emb": lax.rem(e + q // 4, 2), "col": lax.rem(c + (q // 2) % 2, 2), "row": lax.rem(r + q % 2, 2)}
        return remote(sbuf, srecv.at[q - 1], bs, br, dev)

    for q in range(7, 0, -1):
        s_send(q).start()
    with jax.named_scope("ph_s_wait"):
        remote(srecv, srecv, bs, br, sib).wait_recv()
    for q in range(4):
        mine = sbuf[...] if q == 0 else srecv[q - 1]
        x = mine + srecv[q + 3]
        hq = lax.rem(c + q // 2, 2) * 2 + lax.rem(r + q % 2, 2)
        ls = jnp.maximum(-x, 0.0) + jnp.log1p(jnp.exp(-jnp.abs(x)))
        loss_ref[pl.ds(pl.multiple_of(hq * (nhome // 128), 8), nhome // 128), :] = ls

    with jax.named_scope("ph_drain"):
        half2(0, half).wait_send()
        half3(other).wait_send()
        rounded(it2, own, 5).wait_send()
        rounded(it1, own, 8).wait_send()
        for copy in (rc_i, rc_u, rc_du, rc_di, rc_up, rc_u3, rc_uf, remote(dt.at[1], drecv, ds, dr, xpeer),
                     remote(srecv, srecv, bs, br, sib)):
            copy.wait_send()


def store_kernel(*refs):
    srcs, dsts, sem = refs[0:3], refs[3:6], refs[6]
    copies = [pltpu.make_async_copy(a, b, sem.at[k]) for k, (a, b) in enumerate(zip(srcs, dsts))]
    for copy in copies:
        copy.start()
    for copy in copies:
        copy.wait()


def solution(mesh):
    def local_fn(mask_blk, user_sh, item_sh, triples):
        n_usr, n_itm = mask_blk.shape
        dim = user_sh.shape[1]
        n_trip = triples.shape[0]
        nch = n_itm // CH
        half = n_itm // 2
        tri = triples.T
        vm = pltpu.VMEM
        dma = pltpu.SemaphoreType.DMA
        nhome = n_trip // 4
        hrow = nhome // 4
        scratch = [
            vm((NSLOT, n_usr, MC), jnp.int32), vm((n_usr, n_itm + 256), BF16), vm((n_usr, 128), F32),
            vm((n_itm // MC, MC), F32), vm((n_itm // MC, MC), F32), vm((1, n_usr), F32), vm((1, n_usr), F32),
            vm((n_usr, 128), F32), vm((n_itm // MC, MC), F32),
            vm((dim, n_itm), BF16), vm((dim, n_itm), BF16), vm((dim, n_itm), BF16), vm((dim, n_usr), BF16),
            vm((dim, n_itm), F32), vm((dim, n_itm), F32), vm((dim, n_itm), F32), vm((dim, half), F32),
            vm((2 * dim, n_usr), F32), vm((2 * dim, n_usr), F32), vm((dim, n_usr), F32), vm((dim, n_usr), F32),
            vm((dim, 2 * n_usr), BF16), vm((2 * n_usr, nhome), BF16),
            vm((n_itm + 8, dim), F32),
            vm((3, n_trip), jnp.int32), vm((8, 1, 2 * nhome), jnp.int32),
            *[pltpu.SMEM((1, 2 * nhome), jnp.int32)] * 8,
            vm((128, dim), F32), vm((2, dim, nhome), F32), vm((dim, nhome), F32),
            vm((nhome // 128, 128), F32), vm((7, nhome // 128, 128), F32),
            dma((NSLOT,)), dma((3,)), dma((9,)), dma((9,)),
            dma(()), dma((n_itm // WIDE,)), dma(()), dma(()),
            dma(()), dma(()), dma(()), dma(()), dma((8,)), pltpu.SemaphoreType.REGULAR,
        ]
        hbm_spec = pl.BlockSpec(memory_space=pltpu.HBM)
        vmem_spec = pl.BlockSpec(memory_space=pltpu.VMEM)
        ou, oi, loss = pl.pallas_call(
            functools.partial(kernel, n_usr, n_itm, dim, n_trip),
            out_shape=(jax.ShapeDtypeStruct((dim, n_usr // 2), BF16),
                       jax.ShapeDtypeStruct((dim, half), BF16),
                       jax.ShapeDtypeStruct((n_trip // 128, 128), F32)),
            in_specs=[hbm_spec] * 4,
            out_specs=(vmem_spec,) * 3,
            scratch_shapes=scratch,
            compiler_params=pltpu.CompilerParams(collective_id=0, has_side_effects=True,
                                                 vmem_limit_bytes=50 * 1024 * 1024),
            name="gcn",
        )(mask_blk, *[pltpu.with_memory_space_constraint(v, pltpu.HBM) for v in (user_sh.T, item_sh.T, tri)])
        ou, oi, loss = pl.pallas_call(
            store_kernel,
            out_shape=tuple(jax.ShapeDtypeStruct(v.shape, v.dtype) for v in (ou, oi, loss)),
            in_specs=[vmem_spec] * 3,
            out_specs=(pl.BlockSpec(memory_space=pl.ANY),) * 3,
            scratch_shapes=[dma((3,))],
            compiler_params=pltpu.CompilerParams(vmem_limit_bytes=4 * 1024 * 1024),
            name="store",
        )(ou, oi, loss)
        return ou.T, oi.T, loss.reshape(n_trip)

    return jax.shard_map(
        local_fn, mesh=mesh,
        in_specs=(P("row", "col"), P(("row", "col"), "emb"), P(("col", "row"), "emb"), P()),
        out_specs=(P(("row", "col"), "emb"), P(("col", "row"), "emb"), P()),
        check_vma=False)
```

```python
import functools

import jax
import jax.numpy as jnp
from jax import lax
from jax.experimental import pallas as pl
from jax.experimental.pallas import tpu as pltpu
from jax.sharding import PartitionSpec as P

NUM_LAYERS = 3
BIG = 4096
CH = 2048
MC = 512
NSLOT = 8
FIN = 4096
WIDE = 8192
FIRST = 2048
NARROW = 4096
MESH = pl.DeviceIdType.MESH
F32 = jnp.float32
BF16 = jnp.bfloat16


def remote(src, dst, ssem, rsem, dev):
    return pltpu.make_async_remote_copy(src_ref=src, dst_ref=dst, send_sem=ssem, recv_sem=rsem,
                                        device_id=dev, device_id_type=MESH)


def kernel(n_usr, n_itm, dim, n_trip,
           mask_ref, eu_ref, ei_ref, tri_ref, ou_ref, oi_ref, loss_ref,
           stage, adj, rowacc, degi, degi_r, degu, degu_r, invu, invi,
           it0, it1, it2, ut0, i1p, i1r, i2p, i2r,
           up, up_r, u3p, u3_r, uall, sel, table,
           tri_v, idx_v, s0, s1, s2, s3, s4, s5, s6, s7, dbuf, dt, drecv, sbuf, srecv,
           msem, lsem, ssem, rsem, cs1, cr1, cs2, cr2, ds, dr, bs, br, free_sem):
    idx_s = (s0, s1, s2, s3, s4, s5, s6, s7)
    e = lax.axis_index("emb")
    c = lax.axis_index("col")
    r = lax.axis_index("row")
    sib = {"row": 1 - r}
    xpeer = {"col": 1 - c}
    nch = n_itm // CH
    half = n_itm // 2
    uh = n_usr // 2
    nhome = n_trip // 4
    hrow = nhome // 4

    def mask_copy(j):
        slot = lax.rem(j, NSLOT)
        return pltpu.make_async_copy(mask_ref.at[:, pl.ds(pl.multiple_of(j * MC, MC), MC)], stage.at[slot], msem.at[slot])

    for j in range(NSLOT):
        mask_copy(j).start()
    own_i = it0.at[:, pl.ds(pl.multiple_of(r * half, half), half)]
    own_u = ut0.at[:, pl.ds(pl.multiple_of(c * uh, uh), uh)]
    cp_i = pltpu.make_async_copy(ei_ref, own_i, lsem.at[0])
    cp_u = pltpu.make_async_copy(eu_ref, own_u, lsem.at[1])
    cp_t = pltpu.make_async_copy(tri_ref, tri_v, lsem.at[2])
    cp_i.start()
    cp_u.start()
    cp_t.start()

    barrier = pltpu.get_barrier_semaphore()
    for q in range(1, 8):
        dev = {"emb": lax.rem(e + q // 4, 2), "col": lax.rem(c + (q // 2) % 2, 2), "row": lax.rem(r + q % 2, 2)}
        pl.semaphore_signal(barrier, inc=1, device_id=dev, device_id_type=MESH)

    rowacc[...] = jnp.zeros_like(rowacc)

    def mask_step(j, _):
        slot = lax.rem(j, NSLOT)
        mask_copy(j).wait()
        cols = pl.ds(pl.multiple_of(j * MC, MC), MC)

        def rows_step(g, acc):
            rows = pl.ds(pl.multiple_of(g * 16, 16), 16)
            m = stage[slot, rows, :].astype(F32)
            adj[rows, cols] = m.astype(BF16)
            s = m[:, 0:128]
            for k in range(1, MC // 128):
                s = s + m[:, k * 128:(k + 1) * 128]
            rowacc[rows, :] += s
            return acc + (m[0:8] + m[8:16])

        acc = lax.fori_loop(0, n_usr // 16, rows_step, jnp.zeros((8, MC), F32), unroll=8)
        degi[pl.ds(j, 1), :] = jnp.sum(acc, axis=0, keepdims=True)

        @pl.when(j + NSLOT < n_itm // MC)
        def _():
            mask_copy(j + NSLOT).start()
        return 0

    with jax.named_scope("ph_mask0"):
        lax.fori_loop(0, 8, mask_step, 0)
    cp_i.wait()
    cp_u.wait()
    cp_t.wait()
    with jax.named_scope("ph_barrier"):
        pl.semaphore_wait(barrier, 7)
    rc_i = remote(own_i, own_i, ssem.at[0], rsem.at[0], sib)
    rc_u = remote(own_u, own_u, ssem.at[1], rsem.at[1], xpeer)
    rc_i.start()
    rc_u.start()
    with jax.named_scope("ph_mask1"):
        lax.fori_loop(8, n_itm // MC, mask_step, 0)

    degu[...] = jnp.sum(rowacc[...].T, axis=0, keepdims=True)
    rc_du = remote(degu, degu_r, ssem.at[2], rsem.at[2], xpeer)
    rc_di = remote(degi, degi_r, ssem.at[3], rsem.at[3], sib)
    rc_du.start()
    rc_di.start()

    def tri_row(k, row):
        return tri_v[pl.ds(k, 1), pl.ds(pl.multiple_of(row * 128, 128), 128)]

    def home_row(q):
        return (lax.rem(c + q, 2) * 2 + r) * (nhome // 128)

    nrow = nhome // 128
    idx_v[...] = jnp.zeros_like(idx_v)
    for k in range(2):
        for q in range(2):
            for row in range(nrow):
                loc = tri_row(k + 1, home_row(q) + row) - c * n_itm
                loc = jnp.where((loc >= 0) & (loc < n_itm), loc, n_itm)
                for t in range(4):
                    idx_v[k * 4 + t, :, pl.ds((q * nrow + row) * 128, 32)] = loc[:, t * 32:(t + 1) * 32]
    cp_x = []
    for t in range(8):
        cp_x.append(pltpu.make_async_copy(idx_v.at[t], idx_s[t], msem.at[t]))
        cp_x[t].start()
    table[pl.ds(n_itm, 8), :] = jnp.zeros((8, dim), F32)

    with jax.named_scope("ph_di_wait"):
        rc_di.wait_recv()
    invi[...] = lax.rsqrt(jnp.maximum(degi[...] + degi_r[...], 1.0))
    rc_i.wait_recv()
    rc_u.wait_recv()
    with jax.named_scope("ph_du_wait"):
        rc_du.wait_recv()
    inv_row = lax.rsqrt(jnp.maximum(degu[...] + degu_r[...], 1.0))
    invu[...] = jnp.broadcast_to(inv_row, (128, n_usr)).T

    nst = n_itm // WIDE

    def chunk1(base, size):
        cols = pl.ds(pl.multiple_of(base, size), size)
        return remote(i1p.at[:, cols], i1r.at[:, cols], cs1, cr1.at[base // WIDE], sib)

    def step1(i):
        cols = pl.ds(pl.multiple_of(i * WIDE, WIDE), WIDE)
        return remote(i1p.at[:, cols], i1r.at[:, cols], cs1, cr1.at[i], sib)

    def build_step(base, size):
        for nt in range(size // 256):
            cols = pl.ds(pl.multiple_of(base + nt * 256, 256), 256)
            lane = nt * 256 % MC
            wi = jnp.broadcast_to(invi[pl.ds(base // MC + nt * 256 // MC, 1), lane:lane + 256], (16, 256))
            tiles = []
            for g in range(n_usr // 16):
                rows = pl.ds(g * 16, 16)
                wu = jnp.concatenate([invu[rows, :]] * 2, axis=1)
                a = (wu * wi).astype(BF16) * adj[rows, cols]
                adj[rows, cols] = a
                tiles.append(a)
            part = jnp.dot(ut0[...], jnp.concatenate(tiles, axis=0), preferred_element_type=F32)
            i1p[:, cols] = part
        chunk1(base, size).start()
        return 0

    with jax.named_scope("ph_build"):
        nbig = n_itm // BIG - 1
        lax.fori_loop(0, nbig, lambda i, _: build_step(i * BIG, BIG), 0)
        lax.fori_loop(0, BIG // CH, lambda i, _: build_step(nbig * BIG + i * CH, CH), 0)

    def dot_t(a, b):
        return lax.dot_general(a, b, (((1,), (1,)), ((), ())), preferred_element_type=F32)

    def mixed_t(vals, base, beside=None):
        acc1 = acc2 = None
        for lo in range(0, WIDE, 512):
            ca = pl.ds(pl.multiple_of(base + lo, 256), 256)
            cb = pl.ds(pl.multiple_of(base + lo + 256, 256), 256)
            p1 = dot_t(vals[:, lo:lo + 256], adj[:, ca])
            p2 = dot_t(adj[:, cb], vals[:, lo + 256:lo + 512])
            acc1 = p1 if acc1 is None else acc1 + p1
            acc2 = p2 if acc2 is None else acc2 + p2
            if beside:
                beside(lo)
        return acc1 + acc2.T

    up[...] = jnp.zeros_like(up)

    def user_step(i, _):
        cols = pl.ds(pl.multiple_of(i * WIDE, WIDE), WIDE)
        step1(i).wait_recv()
        v1 = (i1p[:, cols] + i1r[:, cols]).astype(BF16)
        it1[:, cols] = v1
        up[...] += mixed_t(jnp.concatenate([it0[:, cols], v1], axis=0), i * WIDE)
        return 0

    with jax.named_scope("ph_user"):
        lax.fori_loop(0, nst, user_step, 0)
    rc_up = remote(up, up_r, ssem.at[4], rsem.at[4], xpeer)
    rc_up.start()
    pl.semaphore_signal(free_sem, inc=1, device_id=sib, device_id_type=MESH)

    remote(i1p, i1r, cs1, cr1.at[0], sib).wait_send()

    def sel_step(g, _):
        users = lax.broadcasted_iota(jnp.int32, (16, 128), 0) + g * 16
        for t in range(nhome // 128):
            ids = tri_row(0, home_row(0) + t)
            hit = jnp.where(users == jnp.broadcast_to(ids, (16, 128)), 1.0, 0.0)
            sel[pl.ds(pl.multiple_of(g * 16, 16), 16), t * 128:(t + 1) * 128] = hit.astype(BF16)
        return 0

    with jax.named_scope("ph_sel"):
        lax.fori_loop(0, 2 * n_usr // 16, sel_step, 0, unroll=2)
    with jax.named_scope("ph_up_wait"):
        rc_up.wait_recv()
    u12 = (up[...] + up_r[...]).astype(BF16)

    oo = r * half
    so = (1 - r) * half
    own = pl.ds(pl.multiple_of(oo, half), half)
    other = pl.ds(pl.multiple_of(so, half), half)

    def half2(k, size):
        src = pl.ds(pl.multiple_of(so + k * size, size), size)
        dst = pl.ds(pl.multiple_of(k * size, size), size)
        return remote(i2p.at[:, src], i2r.at[:, dst], cs2, cr2, sib)

    def half3(cols):
        return remote(i1p.at[:, cols], i1r.at[:, cols], cs1, cr1.at[0], sib)

    def rounded(ref, cols, k):
        return remote(ref.at[:, cols], ref.at[:, cols], ssem.at[k], rsem.at[k], sib)

    def item_step(k, base, size, send):
        cols = pl.ds(pl.multiple_of(base + k * size, size), size)
        part = jnp.dot(u12, adj[:, cols], preferred_element_type=F32)
        i2p[:, cols] = part[0:dim]
        i1p[:, cols] = part[dim:2 * dim]
        if send:
            half2(k, size).start()

    with jax.named_scope("ph_item"):
        for k in range(half // FIRST):
            item_step(k, so, FIRST, True)
        pl.semaphore_wait(free_sem, 1)
        half3(other).start()
        for k in range(half // NARROW):
            item_step(k, oo, NARROW, False)
    with jax.named_scope("ph_i2_wait"):
        half2(0, half).wait_recv()
    it2[:, own] = (i2p[:, own] + i2r[...]).astype(BF16)
    rounded(it2, own, 5).start()
    with jax.named_scope("ph_user3"):
        u3p[...] = mixed_t(it2[:, own], oo)

    def table_step(fin, base):
        fin = fin.astype(F32)
        for b in range(FIN // 128):
            table[pl.ds(pl.multiple_of(base + b * 128, 128), 128), :] = fin[:, b * 128:(b + 1) * 128].T

    def final_step(k, _):
        base = oo + k * FIN
        cols = pl.ds(pl.multiple_of(base, FIN), FIN)
        v3 = (i1p[:, cols] + i1r[:, cols]).astype(BF16)
        acc = it0[:, cols].astype(F32) + it1[:, cols].astype(F32)
        acc = (acc + it2[:, cols].astype(F32)) + v3.astype(F32)
        fin = (acc * (1.0 / (NUM_LAYERS + 1))).astype(BF16)
        it1[:, cols] = fin
        rounded(it1, cols, 8).start()
        return 0

    with jax.named_scope("ph_i3_wait"):
        half3(own).wait_recv()
    with jax.named_scope("ph_final"):
        lax.fori_loop(0, half // FIN, final_step, 0)
    oi_ref[...] = it1[:, own]

    def own_rows(lo):
        for b in range(4):
            at = pl.ds(pl.multiple_of(oo + lo + b * 128, 128), 128)
            table[at, :] = it1[:, at].astype(F32).T

    with jax.named_scope("ph_i2b_wait"):
        rounded(it2, other, 5).wait_recv()
    with jax.named_scope("ph_user3"):
        u3p[...] += mixed_t(it2[:, other], so, own_rows)
    rc_u3 = remote(u3p, u3_r, ssem.at[6], rsem.at[6], xpeer)
    rc_u3.start()

    def rows_step(k, start):
        base = start + k * FIN
        table_step(it1[:, pl.ds(pl.multiple_of(base, FIN), FIN)], base)
        return 0


    with jax.named_scope("ph_i3b_wait"):
        rounded(it1, other, 8).wait_recv()
    with jax.named_scope("ph_final"):
        lax.fori_loop(0, half // FIN, lambda k, _: rows_step(k, so), 0)

    def diff_row(q, row):
        def body(i, _):
            for u in range(8):
                at = (q * nrow + row) * 128 + i * 8 + u
                for t in range(4):
                    p = idx_s[t][0, at]
                    n = idx_s[4 + t][0, at]
                    dbuf[pl.ds(t * 32 + i * 8 + u, 1), :] = table[pl.ds(p, 1), :] - table[pl.ds(n, 1), :]
            return 0

        lax.fori_loop(0, 4, body, 0)
        cols = pl.ds(pl.multiple_of(row * 128, 128), 128)
        dt[q, :, cols] = dbuf[...].T
        if q:
            remote(dt.at[1, :, cols], drecv.at[:, cols], ds, dr, xpeer).start()
        return 0

    for t in range(8):
        cp_x[t].wait()
    with jax.named_scope("ph_diff"):
        lax.fori_loop(0, nrow, lambda row, _: diff_row(1, row), 0)

    with jax.named_scope("ph_diff"):
        lax.fori_loop(0, nrow // 2, lambda row, _: diff_row(0, row), 0)

    with jax.named_scope("ph_u3_wait"):
        rc_u3.wait_recv()
    u3 = (u3p[...] + u3_r[...]).astype(BF16).astype(F32)
    uacc = ut0[...].astype(F32) + u12[0:dim].astype(F32)
    uacc = (uacc + u12[dim:2 * dim].astype(F32)) + u3
    fin_u = (uacc * (1.0 / (NUM_LAYERS + 1))).astype(BF16)
    own_cols = pl.ds(pl.multiple_of(r * n_usr, n_usr), n_usr)
    uall[:, own_cols] = fin_u
    rc_uf = remote(uall.at[:, own_cols], uall.at[:, own_cols], ssem.at[7], rsem.at[7], sib)
    rc_uf.start()
    ou_ref[...] = uall[:, pl.ds(pl.multiple_of(r * n_usr + c * uh, uh), uh)]
    with jax.named_scope("ph_diff"):
        lax.fori_loop(nrow // 2, nrow, lambda row, _: diff_row(0, row), 0)
    with jax.named_scope("ph_uf_wait"):
        rc_uf.wait_recv()
    urow = jnp.dot(uall[...], sel[...], preferred_element_type=F32)

    with jax.named_scope("ph_d_wait"):
        remote(dt.at[1], drecv, ds, dr, xpeer).wait_recv()
    score = jnp.sum((dt[0] + drecv[...]) * urow, axis=0, keepdims=True)
    for row in range(nrow):
        sbuf[pl.ds(row, 1), :] = score[:, row * 128:(row + 1) * 128]

    def s_send(q):
        dev = {"emb": lax.rem(e + q // 4, 2), "col": lax.rem(c + (q // 2) % 2, 2), "row": lax.rem(r + q % 2, 2)}
        return remote(sbuf, srecv.at[q - 1], bs, br, dev)

    for q in range(7, 0, -1):
        s_send(q).start()
    with jax.named_scope("ph_s_wait"):
        remote(srecv, srecv, bs, br, sib).wait_recv()
    for q in range(4):
        mine = sbuf[...] if q == 0 else srecv[q - 1]
        x = mine + srecv[q + 3]
        hq = lax.rem(c + q // 2, 2) * 2 + lax.rem(r + q % 2, 2)
        ls = jnp.maximum(-x, 0.0) + jnp.log1p(jnp.exp(-jnp.abs(x)))
        loss_ref[pl.ds(pl.multiple_of(hq * (nhome // 128), 8), nhome // 128), :] = ls

    with jax.named_scope("ph_drain"):
        half2(0, half).wait_send()
        half3(other).wait_send()
        rounded(it2, own, 5).wait_send()
        rounded(it1, own, 8).wait_send()
        for copy in (rc_i, rc_u, rc_du, rc_di, rc_up, rc_u3, rc_uf, remote(dt.at[1], drecv, ds, dr, xpeer),
                     remote(srecv, srecv, bs, br, sib)):
            copy.wait_send()


def store_kernel(*refs):
    srcs, dsts, sem = refs[0:3], refs[3:6], refs[6]
    copies = [pltpu.make_async_copy(a, b, sem.at[k]) for k, (a, b) in enumerate(zip(srcs, dsts))]
    for copy in copies:
        copy.start()
    for copy in copies:
        copy.wait()


def solution(mesh):
    def local_fn(mask_blk, user_sh, item_sh, triples):
        n_usr, n_itm = mask_blk.shape
        dim = user_sh.shape[1]
        n_trip = triples.shape[0]
        nch = n_itm // CH
        half = n_itm // 2
        tri = triples.T
        vm = pltpu.VMEM
        dma = pltpu.SemaphoreType.DMA
        nhome = n_trip // 4
        hrow = nhome // 4
        scratch = [
            vm((NSLOT, n_usr, MC), jnp.int32), vm((n_usr, n_itm + 256), BF16), vm((n_usr, 128), F32),
            vm((n_itm // MC, MC), F32), vm((n_itm // MC, MC), F32), vm((1, n_usr), F32), vm((1, n_usr), F32),
            vm((n_usr, 128), F32), vm((n_itm // MC, MC), F32),
            vm((dim, n_itm), BF16), vm((dim, n_itm), BF16), vm((dim, n_itm), BF16), vm((dim, n_usr), BF16),
            vm((dim, n_itm), F32), vm((dim, n_itm), F32), vm((dim, n_itm), F32), vm((dim, half), F32),
            vm((2 * dim, n_usr), F32), vm((2 * dim, n_usr), F32), vm((dim, n_usr), F32), vm((dim, n_usr), F32),
            vm((dim, 2 * n_usr), BF16), vm((2 * n_usr, nhome), BF16),
            vm((n_itm + 8, dim), F32),
            vm((3, n_trip), jnp.int32), vm((8, 1, 2 * nhome), jnp.int32),
            *[pltpu.SMEM((1, 2 * nhome), jnp.int32)] * 8,
            vm((128, dim), F32), vm((2, dim, nhome), F32), vm((dim, nhome), F32),
            vm((nhome // 128, 128), F32), vm((7, nhome // 128, 128), F32),
            dma((NSLOT,)), dma((3,)), dma((9,)), dma((9,)),
            dma(()), dma((n_itm // WIDE,)), dma(()), dma(()),
            dma(()), dma(()), dma(()), dma(()), pltpu.SemaphoreType.REGULAR,
        ]
        hbm_spec = pl.BlockSpec(memory_space=pltpu.HBM)
        vmem_spec = pl.BlockSpec(memory_space=pltpu.VMEM)
        ou, oi, loss = pl.pallas_call(
            functools.partial(kernel, n_usr, n_itm, dim, n_trip),
            out_shape=(jax.ShapeDtypeStruct((dim, n_usr // 2), BF16),
                       jax.ShapeDtypeStruct((dim, half), BF16),
                       jax.ShapeDtypeStruct((n_trip // 128, 128), F32)),
            in_specs=[hbm_spec] * 4,
            out_specs=(vmem_spec,) * 3,
            scratch_shapes=scratch,
            compiler_params=pltpu.CompilerParams(collective_id=0, has_side_effects=True,
                                                 vmem_limit_bytes=50 * 1024 * 1024),
            name="gcn",
        )(mask_blk, *[pltpu.with_memory_space_constraint(v, pltpu.HBM) for v in (user_sh.T, item_sh.T, tri)])
        ou, oi, loss = pl.pallas_call(
            store_kernel,
            out_shape=tuple(jax.ShapeDtypeStruct(v.shape, v.dtype) for v in (ou, oi, loss)),
            in_specs=[vmem_spec] * 3,
            out_specs=(pl.BlockSpec(memory_space=pl.ANY),) * 3,
            scratch_shapes=[dma((3,))],
            compiler_params=pltpu.CompilerParams(vmem_limit_bytes=4 * 1024 * 1024),
            name="store",
        )(ou, oi, loss)
        return ou.T, oi.T, loss.reshape(n_trip)

    return jax.shard_map(
        local_fn, mesh=mesh,
        in_specs=(P("row", "col"), P(("row", "col"), "emb"), P(("col", "row"), "emb"), P()),
        out_specs=(P(("row", "col"), "emb"), P(("col", "row"), "emb"), P()),
        check_vma=False)
```
